32 devices in a mesh: row: 16 (over z, x, core), head: 2 (over y).
Axes of the slice: x: 2, y: 2, z: 4, core: 2. Of those that a mesh axis runs over, the one named last changes fastest.
Arguments:
- sequence_matrix: float32 [32, 512, 256], P('row', 'head'), may hold values from -6 to 6
- pair_representation: float32 [512, 512, 128], P('row', 'head'), may hold values from -6 to 6
- alignment_row_mask: int32 [32], P('row'), may hold values 0 or 1
- residue_mask: int32 [512], replicated, may hold values 0 or 1
- attention_scale_vector: float32 [256], replicated, may hold values from 0.1 to 1.9
- asking_factor_matrix: float32 [256, 256], replicated, may hold values from -0.375 to 0.375
- lookup_factor_matrix: float32 [256, 256], replicated, may hold values from -0.375 to 0.375
- content_factor_matrix: float32 [256, 256], replicated, may hold values from -0.375 to 0.375
- sigmoid_factor_matrix: float32 [256, 256], replicated, may hold values from -0.375 to 0.375
- final_factor_matrix: float32 [256, 256], replicated, may hold values from -0.375 to 0.375
- pair_norm_gain: float32 [128], replicated, may hold values from 0.1 to 1.9
- bias_weight: float32 [128, 8], replicated, may hold values from -20 to 20
- tensor_scale_vector: float32 [256], replicated, may hold values from 0.1 to 1.9
- first_factor_matrix: float32 [256, 32], replicated, may hold values from -0.375 to 0.375
- second_factor_matrix: float32 [256, 32], replicated, may hold values from -0.375 to 0.375
- outer_weight: float32 [1024, 128], replicated, may hold values from -1 to 1
Outputs:
- msa_out: float32 [32, 512, 256], P('row', 'head')
- pair_out: float32 [512, 512, 128], P('row', 'head')
The draws below stay inside these ranges and needn't reach their ends.
All inputs are finite; a program needn't handle non-finite values. No bound on the sum of `alignment_row_mask` on one device may be relied on, other than what follows from the above.
Results may differ from the reference program's by a relative error of at most 0.0003.
Values sent between devices are 32-bit elements; how exact they have to be, the bound alone decides.
A program may use at most 128 MiB of HBM per device.

```python
import math
import jax
import jax.numpy as jnp
from jax import lax

FEATURE_DEPTH = 256
C_Z = 128
ATTENTION_GROUPS = 8
TENSOR_FACTOR = 32
CROP_LENGTH = 512
SEQUENCE_TOTAL = 32
N_ROW = 16


def draw_bias_weight(key, part):
    normal_draw = jnp.clip(jax.random.normal(key, (C_Z, ATTENTION_GROUPS), jnp.float32), -4.0, 4.0)
    return normal_draw / math.sqrt(C_Z)


def touch_ends(drawn, own_key, least, high):
    spot = [jax.random.randint(jax.random.fold_in(own_key, axis), (), 0, length) for axis, length in enumerate(drawn.shape)]
    longest = drawn.shape.index(max(drawn.shape))
    beside = spot[:longest] + [(spot[longest] + 1) % drawn.shape[longest]] + spot[longest + 1:]
    return drawn.at[tuple(spot)].set(least).at[tuple(beside)].set(high)


def levels(stream_key, shape, pieces, smallest, top_value):
    def one(axis_at, blocks):
        steps = jax.random.uniform(jax.random.fold_in(jax.random.fold_in(stream_key, 6), axis_at), (blocks,), jnp.float32, smallest / len(pieces), top_value / len(pieces))
        return jnp.repeat(jnp.exp(steps), shape[axis_at] // blocks).reshape((-1,) + (1,) * (len(shape) - axis_at - 1))

    gain = one(*pieces[0])
    for cut in pieces[1:]:
        gain = gain * one(*cut)
    return gain


def noise(stream_key, dims, scale, bound, shards=(), held_as=jnp.bfloat16):
    factor_of = levels(stream_key, dims, shards, -0.22, 0.18) if shards else 1.0
    entries = jax.random.normal(stream_key, dims, jnp.float32) * scale * factor_of
    return jnp.minimum(jnp.maximum(entries, -bound), bound).astype(held_as)


def setup_inputs(seed: int = 0) -> dict:
    seeds = jax.random.split(jax.random.key(seed), 17)
    sequence_matrix = noise(seeds[0], (SEQUENCE_TOTAL, CROP_LENGTH, FEATURE_DEPTH), 1.0, 6.0, ((0, 16), (1, 2)), jnp.float32)
    pair_representation = noise(seeds[1], (CROP_LENGTH, CROP_LENGTH, C_Z), 1.0, 6.0, ((0, 16), (1, 2)), jnp.float32)
    alignment_row_mask = touch_ends((jax.random.randint(seeds[2], (SEQUENCE_TOTAL,), 0, 4) < 3).astype(jnp.int32), jax.random.fold_in(seeds[2], 1), 0, 1)
    residue_mask = touch_ends((jax.random.randint(seeds[3], (CROP_LENGTH,), 0, 8) < 7).astype(jnp.int32), jax.random.fold_in(seeds[3], 1), 0, 1)
    attention_scale_vector = jnp.clip(1.0 + 0.18 * jax.random.normal(seeds[4], (FEATURE_DEPTH,), jnp.float32), 0.1, 1.9)
    asking_factor_matrix = noise(seeds[5], (FEATURE_DEPTH, FEATURE_DEPTH), FEATURE_DEPTH ** -0.5, 0.375, (), jnp.float32)
    lookup_factor_matrix = noise(seeds[6], (FEATURE_DEPTH, FEATURE_DEPTH), FEATURE_DEPTH ** -0.5, 0.375, (), jnp.float32)
    content_factor_matrix = noise(seeds[7], (FEATURE_DEPTH, FEATURE_DEPTH), FEATURE_DEPTH ** -0.5, 0.375, (), jnp.float32)
    sigmoid_factor_matrix = noise(seeds[8], (FEATURE_DEPTH, FEATURE_DEPTH), FEATURE_DEPTH ** -0.5, 0.375, (), jnp.float32)
    final_factor_matrix = noise(seeds[9], (FEATURE_DEPTH, FEATURE_DEPTH), FEATURE_DEPTH ** -0.5, 0.375, (), jnp.float32)
    pair_norm_gain = jnp.clip(1.0 + 0.18 * jax.random.normal(seeds[10], (C_Z,), jnp.float32), 0.1, 1.9)
    bias_weight = draw_bias_weight(jax.random.fold_in(seeds[16], 71), 0)
    tensor_scale_vector = jnp.clip(1.0 + 0.18 * jax.random.normal(seeds[12], (FEATURE_DEPTH,), jnp.float32), 0.1, 1.9)
    first_factor_matrix = noise(seeds[13], (FEATURE_DEPTH, TENSOR_FACTOR), FEATURE_DEPTH ** -0.5, 0.375, (), jnp.float32)
    second_factor_matrix = noise(seeds[14], (FEATURE_DEPTH, TENSOR_FACTOR), FEATURE_DEPTH ** -0.5, 0.375, (), jnp.float32)
    outer_weight = noise(seeds[15], (TENSOR_FACTOR * TENSOR_FACTOR, C_Z), TENSOR_FACTOR ** -0.5, 1.0, (), jnp.float32)
    return dict(sequence_matrix=sequence_matrix, pair_representation=pair_representation, alignment_row_mask=alignment_row_mask, residue_mask=residue_mask, attention_scale_vector=attention_scale_vector, asking_factor_matrix=asking_factor_matrix, lookup_factor_matrix=lookup_factor_matrix, content_factor_matrix=content_factor_matrix, sigmoid_factor_matrix=sigmoid_factor_matrix, final_factor_matrix=final_factor_matrix, pair_norm_gain=pair_norm_gain, bias_weight=bias_weight, tensor_scale_vector=tensor_scale_vector, first_factor_matrix=first_factor_matrix, second_factor_matrix=second_factor_matrix, outer_weight=outer_weight)


exact_arithmetic = lax.Precision.HIGHEST

def apply_layer_norm(values, gains):
    center = values - lax.optimization_barrier(jnp.mean(values, axis=-1, keepdims=True))
    spread = lax.optimization_barrier(jnp.mean(center * center, axis=-1, keepdims=True))
    return center * lax.rsqrt(spread + 1e-05) * gains

def reference(sequence_matrix, pair_representation, alignment_row_mask, residue_mask, attention_scale_vector, asking_factor_matrix, lookup_factor_matrix, content_factor_matrix, sigmoid_factor_matrix, final_factor_matrix, pair_norm_gain, bias_weight, tensor_scale_vector, first_factor_matrix, second_factor_matrix, outer_weight):
    split_groups = FEATURE_DEPTH // ATTENTION_GROUPS
    pair_norm = apply_layer_norm(pair_representation, pair_norm_gain)
    bias_all = jnp.einsum('ijc,ch->hij', pair_norm, bias_weight, precision=exact_arithmetic)
    key_bias = (residue_mask.astype(jnp.float32) - 1.0) * 1000000000.0
    stacked_blocks = jnp.stack([asking_factor_matrix, lookup_factor_matrix, content_factor_matrix, sigmoid_factor_matrix], axis=1)
    inv_root = 1.0 / math.sqrt(split_groups)

    def attend_rows(sequence_features):
        normalized_rows = apply_layer_norm(sequence_features, attention_scale_vector)
        projected_rows = jnp.einsum('ic,cfe->ife', normalized_rows, stacked_blocks, precision=exact_arithmetic).reshape(CROP_LENGTH, 4, ATTENTION_GROUPS, split_groups)
        logits = jnp.einsum('ihd,jhd->hij', projected_rows[:, 0], projected_rows[:, 1], precision=exact_arithmetic) * inv_root + bias_all + key_bias
        largest = lax.optimization_barrier(jnp.max(logits, axis=-1, keepdims=True))
        exponent = jnp.exp(logits - largest)
        weights = exponent / lax.optimization_barrier(jnp.sum(exponent, axis=-1, keepdims=True))
        attended = jnp.einsum('hij,jhd->ihd', weights, projected_rows[:, 2], precision=exact_arithmetic)
        sigmoid_scaled = attended * jax.nn.sigmoid(projected_rows[:, 3])
        return sequence_features + jnp.dot(sigmoid_scaled.reshape(CROP_LENGTH, FEATURE_DEPTH), final_factor_matrix, precision=exact_arithmetic)
    alignment_updated = lax.map(attend_rows, sequence_matrix)
    outer_product_norm = apply_layer_norm(alignment_updated, tensor_scale_vector)
    res_live = residue_mask.astype(jnp.float32)
    live = alignment_row_mask.astype(jnp.float32)[:, None] * res_live[None, :]
    left_side = jnp.einsum('sic,co->sio', outer_product_norm, first_factor_matrix, precision=exact_arithmetic) * live[..., None]
    right = jnp.einsum('sic,co->sio', outer_product_norm, second_factor_matrix, precision=exact_arithmetic) * live[..., None]
    count = jnp.sum(alignment_row_mask.astype(jnp.float32))
    row_block_slice = CROP_LENGTH // N_ROW
    left_side_blocks = left_side.reshape(SEQUENCE_TOTAL, N_ROW, row_block_slice, TENSOR_FACTOR).transpose(1, 0, 2, 3)
    live_blocks = res_live.reshape(N_ROW, row_block_slice)

    def outer_block(inputs):
        left_part, live_part = inputs
        outer = jnp.einsum('sic,sjd->ijcd', left_part, right, precision=exact_arithmetic).reshape(row_block_slice, CROP_LENGTH, TENSOR_FACTOR * TENSOR_FACTOR)
        pair_update = jnp.einsum('ijk,kz->ijz', outer, outer_weight, precision=exact_arithmetic)
        norm_function = count * live_part[:, None] * res_live[None, :] + 0.001
        return pair_update / norm_function[..., None]
    pair_updates = lax.map(outer_block, (left_side_blocks, live_blocks)).reshape(CROP_LENGTH, CROP_LENGTH, C_Z)
    return (alignment_updated, pair_representation + pair_updates)
```

```python
import functools
import math

import jax
import jax.numpy as jnp
from jax import lax
from jax.experimental import pallas as pl
from jax.experimental.pallas import tpu as pltpu
from jax.sharding import PartitionSpec as P


HIGH = lax.Precision.HIGHEST


def apply_layer_norm(values, gains):
    center = values - jnp.mean(values, axis=-1, keepdims=True)
    spread = jnp.mean(center * center, axis=-1, keepdims=True)
    return center * lax.rsqrt(spread + 1e-05) * gains


def split(x):
    hi = x.astype(jnp.bfloat16)
    lo = (x - hi.astype(jnp.float32)).astype(jnp.bfloat16)
    return hi, lo


def mm(a, b, dims=(((1,), (0,)), ((), ()))):
    return lax.dot_general(a, b, dims, preferred_element_type=jnp.float32)


def split_outside(x):
    hi = lax.reduce_precision(x, 8, 7)
    return hi.astype(jnp.bfloat16), lax.reduce_precision(x - hi, 8, 7).astype(jnp.bfloat16)


NT = (((1,), (1,)), ((), ()))


def bias_kernel(pair_ref, gain_ref, weight_ref, out_ref):
    rows, cols, width = pair_ref.shape
    w_hi, w_lo = split(weight_ref[...])
    heads = w_hi.shape[0]
    w_both = jnp.concatenate([w_hi, w_lo], axis=0)
    for r in range(rows):
        x = apply_layer_norm(pair_ref[r], gain_ref[...])
        x_hi, x_lo = split(x)
        both = mm(w_both, x_hi, NT)
        out_ref[r] = both[:heads] + both[heads:] + mm(w_hi, x_lo, NT)


def pair_bias(pair, gain, weight):
    rows, cols, width = pair.shape
    heads = weight.shape[1]
    step = 4
    return pl.pallas_call(
        bias_kernel,
        grid=(rows // step,),
        in_specs=[
            pl.BlockSpec((step, cols, width), lambda i: (i, 0, 0)),
            pl.BlockSpec((1, width), lambda i: (0, 0)),
            pl.BlockSpec((heads, width), lambda i: (0, 0)),
        ],
        out_specs=pl.BlockSpec((step, heads, cols), lambda i: (i, 0, 0)),
        out_shape=jax.ShapeDtypeStruct((rows, heads, cols), jnp.float32),
        cost_estimate=pl.CostEstimate(flops=10**9, bytes_accessed=5 * 10**6, transcendentals=0),
    )(pair, gain[None, :], weight.T)


def attend_kernel(x_ref, gain_ref, w_ref, bias_ref, key_ref, out_ref, q_ref, k_ref, v_ref):
    blocks, heads, depth, keys = bias_ref.shape
    n_rows = x_ref.shape[0]
    width = v_ref.shape[3] // 2
    local = heads * width
    rows = blocks * depth
    step = pl.program_id(0)

    @pl.when(step == 0)
    def _():
        w_hi, w_lo = split(w_ref[...])
        for s in range(n_rows):
            x_hi, x_lo = split(apply_layer_norm(x_ref[s], gain_ref[...]))
            made = mm(x_hi, w_hi) + mm(x_lo, w_hi) + mm(x_hi, w_lo)
            q_hi, q_lo = split(made[:, :local] * (1.0 / math.sqrt(width)))
            k_hi, k_lo = split(made[:, local:2 * local])
            v_hi, v_lo = split(made[:, 2 * local:])
            for h in range(heads):
                at = slice(h * width, (h + 1) * width)
                q_ref[s, h] = jnp.concatenate([q_hi[:, at], q_hi[:, at], q_lo[:, at]], axis=-1)
                k_ref[s, h] = jnp.concatenate([k_hi[:, at], k_lo[:, at], k_hi[:, at]], axis=-1)
                v_ref[s, h] = jnp.concatenate([v_hi[:, at], v_lo[:, at]], axis=-1)

    key_bias = key_ref[...]
    mine = pl.ds(pl.multiple_of(step * rows, rows), rows)
    for s in range(n_rows):
        pieces = []
        for h in range(heads):
            logits = mm(q_ref[s, h, mine, :], k_ref[s, h], NT)
            logits = logits + bias_ref[:, h].reshape(rows, keys) + key_bias
            largest = jnp.max(logits, axis=-1, keepdims=True)
            e = jnp.exp(logits - largest)
            total = jnp.sum(e, axis=-1, keepdims=True)
            e_hi, e_lo = split(e)
            v = v_ref[s, h]
            both = mm(e_hi, v)
            got = both[:, :width] + both[:, width:] + mm(e_lo, v[:, :width])
            pieces.append(got / total)
        out_ref[s] = jnp.concatenate(pieces, axis=-1)


def attend(x, gain, weight, bias, key_bias):
    n_rows, residues, features = x.shape
    groups, heads, depth, keys = bias.shape
    local = weight.shape[1] // 3
    width = local // heads
    blocks = max(1, 128 // depth)
    rows = blocks * depth
    return pl.pallas_call(
        attend_kernel,
        grid=(groups // blocks,),
        in_specs=[
            pl.BlockSpec(x.shape, lambda i: (0, 0, 0)),
            pl.BlockSpec((1, features), lambda i: (0, 0)),
            pl.BlockSpec(weight.shape, lambda i: (0, 0)),
            pl.BlockSpec((blocks, heads, depth, keys), lambda i: (i, 0, 0, 0)),
            pl.BlockSpec((1, keys), lambda i: (0, 0)),
        ],
        out_specs=pl.BlockSpec((n_rows, rows, local), lambda i: (0, i, 0)),
        out_shape=jax.ShapeDtypeStruct((n_rows, residues, local), jnp.float32),
        scratch_shapes=[
            pltpu.VMEM((n_rows, heads, residues, 3 * width), jnp.bfloat16),
            pltpu.VMEM((n_rows, heads, residues, 3 * width), jnp.bfloat16),
            pltpu.VMEM((n_rows, heads, residues, 2 * width), jnp.bfloat16),
        ],
        cost_estimate=pl.CostEstimate(flops=4 * 10**9, bytes_accessed=6 * 10**6, transcendentals=2 * 10**6),
    )(x, gain[None, :], weight, bias, key_bias)


def outer_kernel(scale_ref, left_ref, weight_ref, right_ref, live_ref, pair_ref, out_ref,
                 r_hi, r_lo, t_hi, t_lo):
    step, cols, depth = pair_ref.shape
    rows_all = r_hi.shape[1]
    n_rows = left_ref.shape[0] // step
    width = rows_all // n_rows
    me = pl.program_id(0)

    @pl.when(me == 0)
    def _():
        hi, lo = split(right_ref[...].T)
        r_hi[...] = hi
        r_lo[...] = lo

    left = left_ref[...]
    group = 2
    for d0 in range(0, width, group):
        t = mm(left, weight_ref[:, d0 * depth:(d0 + group) * depth])
        hi, lo = split(t)
        for g in range(group):
            d = d0 + g
            for i in range(step):
                src = (slice(i * n_rows, (i + 1) * n_rows), slice(g * depth, (g + 1) * depth))
                dst = (slice(d * n_rows, (d + 1) * n_rows), slice(i * depth, (i + 1) * depth))
                t_hi[dst] = hi[src]
                t_lo[dst] = lo[src]
    update = mm(r_hi[...], t_hi[...]) + mm(r_lo[...], t_hi[...]) + mm(r_hi[...], t_lo[...])
    for i in range(step):
        norm = scale_ref[me * step + i] * live_ref[...] + 0.001
        out_ref[i] = pair_ref[i] + update[:, i * depth:(i + 1) * depth] / norm


def outer_mean(scale, left, weight, right, live, pair):
    rows, cols, depth = pair.shape
    total = right.shape[0]
    n_rows = left.shape[0] // rows
    packed = left.shape[1]
    step = 4
    return pl.pallas_call(
        outer_kernel,
        grid=(rows // step,),
        in_specs=[
            pl.BlockSpec(memory_space=pltpu.SMEM),
            pl.BlockSpec((step * n_rows, packed), lambda i: (i, 0)),
            pl.BlockSpec(weight.shape, lambda i: (0, 0)),
            pl.BlockSpec(right.shape, lambda i: (0, 0)),
            pl.BlockSpec((cols, 1), lambda i: (0, 0)),
            pl.BlockSpec((step, cols, depth), lambda i: (i, 0, 0)),
        ],
        out_specs=pl.BlockSpec((step, cols, depth), lambda i: (i, 0, 0)),
        out_shape=jax.ShapeDtypeStruct(pair.shape, jnp.float32),
        scratch_shapes=[
            pltpu.VMEM((cols, total), jnp.bfloat16),
            pltpu.VMEM((cols, total), jnp.bfloat16),
            pltpu.VMEM((total, step * depth), jnp.bfloat16),
            pltpu.VMEM((total, step * depth), jnp.bfloat16),
        ],
        cost_estimate=pl.CostEstimate(flops=9 * 10**9, bytes_accessed=10**7, transcendentals=0),
    )(scale, left, weight, right, live, pair)


def gather_kernel(n, block_ref, out_ref, own_sem, send_sem, recv_sem):
    me = lax.axis_index("row")
    core = me % 2
    x = (me // 2) % 2
    nz = n // 4
    z = me // 4

    def place(zz, xx, cc):
        return (zz * 2 + xx) * 2 + cc

    barrier = pltpu.get_barrier_semaphore()
    up_ok, down_ok = z + 1 < nz, z >= 1

    def greet(target):
        pl.semaphore_signal(barrier, inc=1, device_id={"row": target},
                            device_id_type=pl.DeviceIdType.MESH)

    greet(place(z, x, 1 - core))
    greet(place(z, 1 - x, core))
    pl.when(up_ok)(lambda: greet(place(z + 1, x, core)))
    pl.when(down_ok)(lambda: greet(place(z - 1, x, core)))
    peers = 2 + jnp.where(up_ok, 1, 0) + jnp.where(down_ok, 1, 0)
    pl.semaphore_wait(barrier, peers)

    own = pltpu.make_async_copy(block_ref, out_ref.at[me], own_sem)
    own.start()

    def sends(d, other):
        found = []
        first = core == 0
        if other == 0:
            cross = (z >= 0) if d == 0 else jnp.logical_not(first)
            run = z >= 0
        else:
            cross = None
            run = first
        if d <= 0:
            found.append((jnp.logical_and(run, up_ok), 0, lambda: place(z + 1, x, core)))
        if d >= 0:
            found.append((jnp.logical_and(run, down_ok), 1, lambda: place(z - 1, x, core)))
        if cross is not None:
            found.append((cross, 2, lambda: place(z, 1 - x, core)))
        found.append((z >= 0, 3, lambda: place(z, x, 1 - core)))
        return found

    def copy(source, kind, target, mine):
        return pltpu.make_async_remote_copy(
            src_ref=block_ref if mine else out_ref.at[source],
            dst_ref=out_ref.at[source],
            send_sem=send_sem.at[kind, source],
            recv_sem=recv_sem.at[source],
            device_id={"row": target},
            device_id_type=pl.DeviceIdType.MESH,
        )

    hops = [(0, 0), (0, 1)]
    for far in range(1, nz):
        hops += [(-far, 0), (far, 0), (-far, 1), (far, 1)]

    def each(action):
        for d, other in hops:
            source = place(z + d, (x + other) % 2, core)
            mine = d == 0 and other == 0
            there = jnp.logical_and(z + d >= 0, z + d < nz)

            @pl.when(there)
            def _(d=d, other=other, source=source, mine=mine):
                action(d, other, source, mine)

    def forward(d, other, source, mine):
        if not mine:
            copy(source, 3, place(z, x, 1 - core), False).wait_recv()
        for ok, kind, target in sends(d, other):
            pl.when(ok)(lambda kind=kind, target=target: copy(source, kind, target(), mine).start())

    def finish(d, other, source, mine):
        for ok, kind, target in sends(d, other):
            pl.when(ok)(lambda kind=kind, target=target: copy(source, kind, target(), mine).wait_send())

    each(forward)
    for k in range(n // 2):
        copy(2 * k + 1 - core, 3, place(z, x, 1 - core), False).wait_recv()
    each(finish)
    own.wait()


def gather_rows(block, n, ident):
    return pl.pallas_call(
        functools.partial(gather_kernel, n),
        out_shape=jax.ShapeDtypeStruct((n,) + block.shape, block.dtype),
        in_specs=[pl.BlockSpec(memory_space=pltpu.VMEM)],
        out_specs=pl.BlockSpec(memory_space=pl.ANY),
        scratch_shapes=[
            pltpu.SemaphoreType.DMA,
            pltpu.SemaphoreType.DMA((4, n)),
            pltpu.SemaphoreType.DMA((n,)),
        ],
        compiler_params=pltpu.CompilerParams(collective_id=ident, has_side_effects=True),
    )(block)


def around(n):
    return [[(src, (src + k) % n) for src in range(n)] for k in range(n)]


def gather_heads(block, n, index, axis):
    size = block.shape[axis]
    shape = list(block.shape)
    shape[axis] = size * n
    whole = jnp.zeros(shape, block.dtype)
    for k in range(n):
        part = block if k == 0 else lax.ppermute(block, "head", around(n)[k])
        whole = lax.dynamic_update_slice_in_dim(whole, part, ((index - k) % n) * size, axis)
    return whole


def exchange_heads(block, n, index, split_axis, concat_axis):
    size = block.shape[split_axis] // n
    shape = list(block.shape)
    shape[split_axis] = size
    length = shape[concat_axis]
    shape[concat_axis] = length * n
    whole = jnp.zeros(shape, block.dtype)
    for k in range(n):
        part = lax.dynamic_slice_in_dim(block, ((index + k) % n) * size, size, split_axis)
        if k:
            part = lax.ppermute(part, "head", around(n)[k])
        whole = lax.dynamic_update_slice_in_dim(whole, part, ((index - k) % n) * length, concat_axis)
    return whole


def body(
    sequence_matrix,
    pair_representation,
    alignment_row_mask,
    residue_mask,
    attention_scale_vector,
    asking_factor_matrix,
    lookup_factor_matrix,
    content_factor_matrix,
    sigmoid_factor_matrix,
    final_factor_matrix,
    pair_norm_gain,
    bias_weight,
    tensor_scale_vector,
    first_factor_matrix,
    second_factor_matrix,
    outer_weight,
):
    head_count = lax.axis_size("head")
    head_index = lax.axis_index("head")
    row_index = lax.axis_index("row")
    row_count = lax.axis_size("row")
    n_rows, col_count, width = sequence_matrix.shape
    residues = col_count * head_count
    pair_rows = pair_representation.shape[0]
    pair_depth = pair_representation.shape[2]
    heads_all = bias_weight.shape[1]
    head_width = width // heads_all
    local_heads = heads_all // head_count
    local_width = local_heads * head_width
    opm_width = first_factor_matrix.shape[1]

    sequence_all = gather_heads(sequence_matrix, head_count, head_index, 1)

    bias_all = pair_bias(pair_representation, pair_norm_gain, bias_weight)
    bias_part = exchange_heads(
        bias_all.transpose(1, 0, 2), head_count, head_index, 0, 2
    )
    bias = gather_rows(bias_part, row_count, 0)
    key_bias = ((residue_mask.astype(jnp.float32) - 1.0) * 1000000000.0)[None, :]

    weights = jnp.concatenate(
        [
            lax.dynamic_slice_in_dim(w, head_index * local_width, local_width, 1)
            for w in (asking_factor_matrix, lookup_factor_matrix, content_factor_matrix)
        ],
        axis=1,
    )
    attended = attend(sequence_all, attention_scale_vector, weights, bias, key_bias)
    norm_mine = apply_layer_norm(sequence_matrix, attention_scale_vector)
    gate = jax.nn.sigmoid(
        jnp.einsum("sic,ce->sie", norm_mine, sigmoid_factor_matrix, precision=HIGH)
    )
    returned_values = exchange_heads(attended, head_count, head_index, 1, 2) * gate
    alignment_updated = sequence_matrix + jnp.einsum(
        "jna,ab->jnb", returned_values, final_factor_matrix, precision=HIGH
    )

    outer_product_norm = apply_layer_norm(alignment_updated, tensor_scale_vector)
    live_cols = lax.dynamic_slice_in_dim(residue_mask, head_index * col_count, col_count).astype(
        jnp.float32
    )
    row_live = alignment_row_mask.astype(jnp.float32)
    live = row_live[:, None] * live_cols[None, :]
    left_side = (
        jnp.einsum("sic,co->soi", outer_product_norm, first_factor_matrix, precision=HIGH)
        * live[:, None, :]
    )
    right = (
        jnp.einsum("sic,co->soi", outer_product_norm, second_factor_matrix, precision=HIGH)
        * live[:, None, :]
    )
    left_all = gather_heads(left_side, head_count, head_index, 1)
    carried = jnp.broadcast_to(row_live[:, None, None], (n_rows, 8, col_count))
    sides = gather_rows(jnp.concatenate([left_all, right, carried], axis=1), row_count, 1)
    sides = sides.reshape(row_count * n_rows, -1, col_count)
    left_width = head_count * opm_width
    first_row = row_index * pair_rows
    left_mine = lax.dynamic_slice(
        sides,
        (0, (first_row // col_count) * opm_width, first_row % col_count),
        (row_count * n_rows, opm_width, pair_rows),
    )
    right_all = sides[:, left_width:]
    total_rows = row_count * n_rows
    count = jnp.sum(right_all[:, opm_width, 0])
    right_rows = right_all[:, :opm_width].transpose(1, 0, 2).reshape(
        opm_width * total_rows, col_count
    )
    left_rows = left_mine.transpose(2, 0, 1).reshape(pair_rows * total_rows, opm_width)
    l_hi, l_lo = split_outside(left_rows)
    w_hi, w_lo = split_outside(outer_weight.reshape(opm_width, opm_width * pair_depth))
    rows_live = lax.dynamic_slice_in_dim(residue_mask, row_index * pair_rows, pair_rows).astype(
        jnp.float32
    )
    pair_out = outer_mean(
        count * rows_live,
        jnp.concatenate([l_hi, l_hi, l_lo], axis=1),
        jnp.concatenate([w_hi, w_lo, w_hi], axis=0),
        right_rows,
        live_cols[:, None],
        pair_representation,
    )
    return alignment_updated, pair_out


def ln(values, gains):
    return apply_layer_norm(values, gains)


def front_kernel(
    x_hbm, pair_hbm, row_mask, key_ref, gain_ref, wq_hbm, wk_hbm, wv_hbm, wg_hbm, wo_hbm,
    pair_gain, bias_w, tensor_gain, left_w, right_w,
    msa_hbm, left_in, right_all,
    x_ref, pair_ref, wq_ref, wk_ref, wv_ref, wg_ref, wo_ref, msa_ref, wpair_ref, group_ref,
    bias_ref, xn_ref, q_ref, k_ref, v_ref, gate_ref, att_out, att_in, right_loc, left_loc, left_own,
    load_sem, pair_sem, out_sem, s1_send, s1_recv, n_send, n_recv, z_send, z_recv, x_send, x_recv,
    a_send, a_recv, rz_send, rz_recv, rx_send, rx_recv, rc_send, rc_recv,
    l1_send, l1_recv, l2_send, l2_recv, self_sem,
):
    nz, _, chunks, _, n_y, group_heads, sub, cols = bias_ref.shape
    n_rows, _, feat = x_ref.shape
    heads = bias_w.shape[0]
    keys = n_y * cols
    width = v_ref.shape[3] // 2
    group_width = group_heads * width
    local_width = 2 * group_width
    per_half = nz // n_y
    plane = cols // per_half
    pair_width = pair_ref.shape[2]
    opm = left_w.shape[0]

    me, y = lax.axis_index("row"), lax.axis_index("head")
    c, x, z = me % 2, (me // 2) % 2, me // 4
    half = z // per_half

    def place(zz, xx, cc):
        return (zz * 2 + xx) * 2 + cc

    def across(d):
        out, bit = z, 1
        while bit <= d:
            if d & bit:
                out = out + bit * (1 - 2 * ((out // bit) % 2))
            bit *= 2
        return out

    def remote(src, dst, send, recv, row, head):
        return pltpu.make_async_remote_copy(
            src_ref=src, dst_ref=dst, send_sem=send, recv_sem=recv,
            device_id={"row": row, "head": head}, device_id_type=pl.DeviceIdType.MESH,
        )

    def arrived(dst, send, recv):
        remote(dst, dst, send, recv, place(z, x, 1 - c), y).wait_recv()

    pending = []

    def go(copy):
        copy.start()
        pending.append(copy)

    loads = {}
    for at, (src, dst) in enumerate(
        [(x_hbm, x_ref), (wq_hbm, wq_ref), (wk_hbm, wk_ref), (wv_hbm, wv_ref), (wg_hbm, wg_ref), (wo_hbm, wo_ref)]
    ):
        loads[at] = pltpu.make_async_copy(src, dst, load_sem.at[at])
    pair_loads = [
        pltpu.make_async_copy(
            pair_hbm.at[pl.ds(k * sub, sub)], pair_ref.at[pl.ds(k * sub, sub)], pair_sem.at[k]
        )
        for k in range(chunks)
    ]
    loads[0].start()
    for copy in pair_loads:
        copy.start()
    for at in range(1, 6):
        loads[at].start()

    barrier = pltpu.get_barrier_semaphore()
    peers = []
    for dx in range(2):
        for dc in range(2):
            for dy in range(n_y):
                if dx or dc or dy:
                    peers.append((place(z, (x + dx) % 2, (c + dc) % 2), (y + dy) % n_y))
    for d in range(1, nz):
        peers.append((place(across(d), x, c), y))
    for row, head in peers:
        pl.semaphore_signal(barrier, inc=1, device_id={"row": row, "head": head},
                            device_id_type=pl.DeviceIdType.MESH)

    loads[0].wait()
    for s in range(n_rows):
        xn_ref[y, c, s] = ln(x_ref[s], gain_ref[...])

    w_hi, w_lo = split(bias_w[...])
    spread = sub * heads
    at_row = lax.broadcasted_iota(jnp.int32, (heads, sub, pair_width), 1).reshape(spread, pair_width)
    zero = jnp.zeros((spread, pair_width), jnp.float32)

    def rows_of(part):
        part = part.astype(jnp.float32)
        return jnp.broadcast_to(part[:, None, :], (heads, sub, pair_width)).reshape(spread, pair_width)

    rep_hi, rep_lo = rows_of(w_hi), rows_of(w_lo)
    for t in range(sub // 2):
        first, second = at_row == 2 * t, at_row == 2 * t + 1
        both = [
            jnp.concatenate([jnp.where(first, rep, zero), jnp.where(second, rep, zero)], axis=1)
            for rep in (rep_hi, rep_lo)
        ]
        wpair_ref[t] = jnp.concatenate(both, axis=0).astype(jnp.bfloat16)

    def bias_chunk(k):
        pair_loads[k].wait()
        total = None
        for t in range(sub // 2):
            at = k * sub + 2 * t
            pieces = [split(ln(pair_ref[at + e], pair_gain[...])) for e in range(2)]
            hi = jnp.concatenate([pieces[0][0], pieces[1][0]], axis=1)
            lo = jnp.concatenate([pieces[0][1], pieces[1][1]], axis=1)
            both = mm(wpair_ref[t], hi, NT)
            part = both[:spread] + both[spread:] + mm(wpair_ref[t, :spread], lo, NT)
            total = part if total is None else total + part
        group_ref[k] = total.reshape(2 * n_y, group_heads, sub, cols)
        bias_ref[z, x, k, c, y] = group_ref[k, y * 2 + c]

    labels = [(dy, dc) for dy in range(n_y) for dc in range(2) if dy or dc]

    def stage_one(k):
        for at, (dy, dc) in enumerate(labels):
            ty, tc = (y + dy) % n_y, (c + dc) % 2
            go(remote(group_ref.at[k, ty * 2 + tc], bias_ref.at[z, x, k, c, y],
                      s1_send.at[k, at], s1_recv.at[k, at], place(z, x, tc), ty))

    def stage_two(k):
        for at, (dy, dc) in enumerate(labels):
            sy, sc = (y + n_y - dy) % n_y, (c + dc) % 2
            arrived(bias_ref.at[z, x, k, sc, sy], s1_send.at[k, at], s1_recv.at[k, at])
        own = bias_ref.at[z, x, k]
        go(remote(own, own, x_send.at[0, k], x_recv.at[0, k], place(z, 1 - x, c), y))
        for d in range(1, nz):
            go(remote(own, own, z_send.at[d, k], z_recv.at[d, k], place(across(d), x, c), y))

    def pass_across(d):
        zz = across(d)
        for k in range(chunks):
            block = bias_ref.at[zz, x, k]
            arrived(block, z_send.at[d, k], z_recv.at[d, k])
            go(remote(block, block, x_send.at[d, k], x_recv.at[d, k], place(z, 1 - x, c), y))

    bias_chunk(0)
    pl.semaphore_wait(barrier, len(peers))
    own_x = xn_ref.at[y, c]
    for dy in range(1, n_y):
        go(remote(own_x, own_x, n_send.at[dy], n_recv.at[dy], place(z, x, c), (y + dy) % n_y))
    go(remote(own_x, own_x, n_send.at[0], n_recv.at[0], place(z, x, 1 - c), y))
    stage_one(0)
    for k in range(1, chunks):
        bias_chunk(k)
        stage_one(k)
        stage_two(k - 1)

    loads[4].wait()
    g_hi, g_lo = split(wg_ref[...])
    for s in range(n_rows):
        hi, lo = split(xn_ref[y, c, s])
        gate_ref[s] = jax.nn.sigmoid(mm(hi, g_hi) + mm(lo, g_hi) + mm(hi, g_lo))

    stage_two(chunks - 1)
    for dy in range(1, n_y):
        sy = (y + n_y - dy) % n_y
        block = xn_ref.at[sy, c]
        arrived(block, n_send.at[dy], n_recv.at[dy])
        go(remote(block, block, n_send.at[n_y + dy], n_recv.at[n_y + dy], place(z, x, 1 - c), y))
    if nz > 1:
        pass_across(1)

    for at in (1, 2, 3):
        loads[at].wait()
    mine = pl.ds(pl.multiple_of(y * local_width, local_width), local_width)
    picked = []
    for ref in (wq_ref, wk_ref, wv_ref):
        whole = ref[:, mine]
        picked.append(jnp.where(c == 0, whole[:, :group_width], whole[:, group_width:]))
    wa_hi, wa_lo = split(jnp.concatenate(picked, axis=1))

    def project(yy, cc):
        spot = pl.ds(pl.multiple_of(yy * cols, cols), cols)
        for s in range(n_rows):
            hi, lo = split(xn_ref[yy, cc, s])
            made = mm(hi, wa_hi) + mm(lo, wa_hi) + mm(hi, wa_lo)
            q_hi, q_lo = split(made[:, :group_width] * (1.0 / math.sqrt(width)))
            k_hi, k_lo = split(made[:, group_width:2 * group_width])
            v_hi, v_lo = split(made[:, 2 * group_width:])
            for h in range(group_heads):
                at = slice(h * width, (h + 1) * width)
                to = cc * n_rows + s
                q_ref[to, h, spot, :] = jnp.concatenate([q_hi[:, at], q_hi[:, at], q_lo[:, at]], axis=-1)
                k_ref[to, h, spot, :] = jnp.concatenate([k_hi[:, at], k_lo[:, at], k_hi[:, at]], axis=-1)
                v_ref[to, h, spot, :] = jnp.concatenate([v_hi[:, at], v_lo[:, at]], axis=-1)

    project(y, c)
    arrived(xn_ref.at[y, 1 - c], n_send.at[0], n_recv.at[0])
    project(y, 1 - c)
    for dy in range(1, n_y):
        sy = (y + n_y - dy) % n_y
        project(sy, c)
        arrived(xn_ref.at[sy, 1 - c], n_send.at[n_y + dy], n_recv.at[n_y + dy])
        project(sy, 1 - c)

    key_bias = (key_ref[...].astype(jnp.float32) - 1.0) * 1000000000.0

    def attended_copy(d, ct):
        zz = across(d)
        return remote(att_out.at[d, ct], att_in.at[y * 2 + c, zz % per_half],
                      a_send.at[d, ct], a_recv.at[y * 2 + c, zz % per_half],
                      place(z, x, ct), zz // per_half)

    def is_mine(d, ct):
        return jnp.logical_and(across(d) // per_half == y, ct == c)

    def attend_plane(d):
        zz = across(d)
        for k in range(chunks):
            arrived(bias_ref.at[zz, 1 - x, k], x_send.at[d, k], x_recv.at[d, k])
        queries = pl.ds(pl.multiple_of(zz * plane, plane), plane)

        def unit(ct, carry):
            pieces = []
            for s in range(n_rows):
                row = ct * n_rows + s
                for h in range(group_heads):
                    logits = mm(q_ref[row, h, queries, :], k_ref[row, h], NT)
                    tiles = [
                        jnp.concatenate(
                            [bias_ref[zz, xx, :, cc, yy, h].reshape(chunks * sub, cols) for yy in range(n_y)],
                            axis=1,
                        )
                        for xx in range(2)
                        for cc in range(2)
                    ]
                    logits = logits + jnp.concatenate(tiles, axis=0) + key_bias
                    largest = jnp.max(logits, axis=-1, keepdims=True)
                    e = jnp.exp(logits - largest)
                    total = jnp.sum(e, axis=-1, keepdims=True)
                    e_hi, e_lo = split(e)
                    v = v_ref[row, h]
                    both = mm(e_hi, v)
                    got = both[:, :width] + both[:, width:] + mm(e_lo, v[:, :width])
                    pieces.append(got / total)
            value = jnp.concatenate(pieces, axis=-1)
            att_out[d, ct] = value

            @pl.when(is_mine(d, ct))
            def _():
                att_in[y * 2 + c, zz % per_half] = value

            @pl.when(jnp.logical_not(is_mine(d, ct)))
            def _():
                attended_copy(d, ct).start()

            return carry

        lax.fori_loop(0, 2, unit, 0)

    for d in range(nz):
        attend_plane(d)
        if 2 + d < nz:
            pass_across(2 + d)

    for dy, dc in labels:
        sy, sc = (y + n_y - dy) % n_y, (c + dc) % 2
        for p in range(per_half):
            arrived(att_in.at[sy * 2 + sc, p], a_send.at[0, 0], a_recv.at[sy * 2 + sc, p])

    loads[5].wait()
    o_hi, o_lo = split(wo_ref[...])
    wide = n_rows * opm
    left_hi, left_lo = split(left_w[...])
    left_both = jnp.concatenate([left_hi, left_lo], axis=0)
    right_hi, right_lo = split(right_w[...])
    right_both = jnp.concatenate([right_hi, right_lo], axis=0)
    lefts = []
    count = jnp.zeros((sub, cols), jnp.float32)
    for s in range(n_rows):
        at = slice(s * group_width, (s + 1) * group_width)
        whole = jnp.concatenate(
            [
                jnp.concatenate([att_in[g, p][:, at] for p in range(per_half)], axis=0)
                for g in range(2 * n_y)
            ],
            axis=1,
        ) * gate_ref[s]
        hi, lo = split(whole)
        out = x_ref[s] + (mm(hi, o_hi) + mm(lo, o_hi) + mm(hi, o_lo))
        msa_ref[s] = out
        t_hi, t_lo = split(ln(out, tensor_gain[...]))
        live = row_mask[s].astype(jnp.float32)
        both = mm(right_both, t_hi, NT)
        right_loc[s * opm:(s + 1) * opm, :] = (both[:opm] + both[opm:] + mm(right_hi, t_lo, NT)) * live
        both = mm(t_hi, left_both, NT)
        lefts.append((both[:, :opm] + both[:, opm:] + mm(t_lo, left_hi, NT)) * live)
        count = count + live
    right_loc[wide:, :] = count

    keep_right = pltpu.make_async_copy(right_loc, right_all.at[me], self_sem.at[0])
    keep_right.start()
    go(remote(right_loc, right_all.at[me], rc_send.at[0, 0], rc_recv.at[0, 0], place(z, x, 1 - c), y))
    go(remote(right_loc, right_all.at[me], rx_send.at[0], rx_recv.at[0], place(z, 1 - x, c), y))
    for d in range(1, nz):
        go(remote(right_loc, right_all.at[me], rz_send.at[d], rz_recv.at[d], place(across(d), x, c), y))

    left = jnp.concatenate(lefts, axis=1)
    blocks = per_half * 4
    tall = left.shape[0] // blocks // 2
    left = left.reshape(blocks, 2, tall, wide)
    left_loc[...] = jnp.concatenate([left[:, 0], left[:, 1]], axis=2)

    def left_copy(p):
        return remote(left_loc.at[pl.ds(p * 4, 4)], left_own.at[z], l1_send.at[p], l1_recv.at[z],
                      place(y * per_half + p, x, c), y)

    for p in range(per_half):
        here = y * per_half + p == z

        @pl.when(here)
        def _(p=p):
            left_own[z] = left_loc[p * 4:(p + 1) * 4]

        pl.when(jnp.logical_not(here))(lambda p=p: left_copy(p).start())

    keep_msa = pltpu.make_async_copy(msa_ref, msa_hbm, out_sem)
    keep_msa.start()

    for d in range(1, nz):
        block = right_all.at[place(across(d), x, c)]
        arrived(block, rz_send.at[d], rz_recv.at[d])
        go(remote(block, block, rx_send.at[d], rx_recv.at[d], place(z, 1 - x, c), y))
        go(remote(block, block, rc_send.at[d, 0], rc_recv.at[d, 0], place(z, x, 1 - c), y))

    owner = half == y

    def final_copy(at, dx, dc, dy):
        tx, tc, ty = (x + dx) % 2, (c + dc) % 2, (y + dy) % n_y
        return remote(left_own.at[:, tx * 2 + tc], left_in.at[:, x * 2 + c], l2_send.at[at],
                      l2_recv.at[x * 2 + c], place(z, tx, tc), ty)

    finals = [(dx, dc, dy) for dx in range(2) for dc in range(2) for dy in range(n_y) if dx or dc or dy]

    @pl.when(owner)
    def _():
        for d in range(1, nz):
            zz = across(d)
            arrived(left_own.at[zz], l1_send.at[0], l1_recv.at[zz])
        for at, (dx, dc, dy) in enumerate(finals):
            final_copy(at, dx, dc, dy).start()
        pltpu.make_async_copy(left_own.at[:, x * 2 + c], left_in.at[:, x * 2 + c], self_sem.at[1]).start()

    for d in range(nz):
        block = right_all.at[place(across(d), 1 - x, c)]
        arrived(block, rx_send.at[d], rx_recv.at[d])
        go(remote(block, block, rc_send.at[d, 1], rc_recv.at[d, 1], place(z, x, 1 - c), y))

    for xx in range(2):
        for cc in range(2):
            mine_too = jnp.logical_and(owner, jnp.logical_and(xx == x, cc == c))

            @pl.when(jnp.logical_not(mine_too))
            def _(xx=xx, cc=cc):
                arrived(left_in.at[:, xx * 2 + cc], l2_send.at[0], l2_recv.at[xx * 2 + cc])

    for d in range(nz):
        for far in range(2):
            block = right_all.at[place(across(d), (x + far) % 2, 1 - c)]
            arrived(block, rc_send.at[d, far], rc_recv.at[d, far])

    for copy in pending:
        copy.wait_send()
    for d in range(nz):
        for ct in range(2):
            pl.when(jnp.logical_not(is_mine(d, ct)))(lambda d=d, ct=ct: attended_copy(d, ct).wait_send())
    for p in range(per_half):
        pl.when(y * per_half + p != z)(lambda p=p: left_copy(p).wait_send())

    @pl.when(owner)
    def _():
        for at, (dx, dc, dy) in enumerate(finals):
            final_copy(at, dx, dc, dy).wait_send()
        pltpu.make_async_copy(left_own.at[:, x * 2 + c], left_in.at[:, x * 2 + c], self_sem.at[1]).wait()

    keep_right.wait()
    keep_msa.wait()


def front(n_row, n_y, x, pair, row_mask, residue_mask, gain, wq, wk, wv, wg, wo,
          pair_gain, bias_w, tensor_gain, left_w, right_w):
    n_rows, cols, feat = x.shape
    pair_rows, _, pair_width = pair.shape
    heads = bias_w.shape[1]
    width = feat // heads
    group_heads = heads // n_y // 2
    nz, sub = n_row // 4, 8
    chunks = pair_rows // sub
    keys = n_y * cols
    per_half = nz // n_y
    plane = cols // per_half
    opm = left_w.shape[1]
    wide = n_rows * opm
    f32, b16 = jnp.float32, jnp.bfloat16
    any_spec, vmem = pl.BlockSpec(memory_space=pl.ANY), pl.BlockSpec(memory_space=pltpu.VMEM)
    dma = pltpu.SemaphoreType.DMA
    labels = 2 * n_y - 1
    return pl.pallas_call(
        front_kernel,
        out_shape=(
            jax.ShapeDtypeStruct(x.shape, f32),
            jax.ShapeDtypeStruct((nz, 4, pair_rows // 2, 2 * wide), f32),
            jax.ShapeDtypeStruct((n_row, wide + sub, cols), f32),
        ),
        in_specs=[any_spec, any_spec, pl.BlockSpec(memory_space=pltpu.SMEM), vmem, vmem]
        + [any_spec] * 5 + [vmem] * 5,
        out_specs=(any_spec, any_spec, any_spec),
        scratch_shapes=[
            pltpu.VMEM(x.shape, f32),
            pltpu.VMEM(pair.shape, f32),
        ]
        + [pltpu.VMEM((feat, feat), f32)] * 5
        + [
            pltpu.VMEM(x.shape, f32),
            pltpu.VMEM((sub // 2, 2 * sub * heads, 2 * pair_width), b16),
            pltpu.VMEM((chunks, 2 * n_y, group_heads, sub, cols), f32),
            pltpu.VMEM((nz, 2, chunks, 2, n_y, group_heads, sub, cols), f32),
            pltpu.VMEM((n_y, 2, n_rows, cols, feat), f32),
            pltpu.VMEM((2 * n_rows, group_heads, keys, 3 * width), b16),
            pltpu.VMEM((2 * n_rows, group_heads, keys, 3 * width), b16),
            pltpu.VMEM((2 * n_rows, group_heads, keys, 2 * width), b16),
            pltpu.VMEM(x.shape, f32),
            pltpu.VMEM((nz, 2, plane, n_rows * group_heads * width), f32),
            pltpu.VMEM((2 * n_y, per_half, plane, n_rows * group_heads * width), f32),
            pltpu.VMEM((wide + sub, cols), f32),
            pltpu.VMEM((4 * per_half, pair_rows // 2, 2 * wide), f32),
            pltpu.VMEM((nz, 4, pair_rows // 2, 2 * wide), f32),
            dma((6,)), dma((chunks,)), dma,
            dma((chunks, labels)), dma((chunks, labels)),
            dma((2 * n_y,)), dma((2 * n_y,)),
            dma((nz, chunks)), dma((nz, chunks)),
            dma((nz, chunks)), dma((nz, chunks)),
            dma((nz, 2)), dma((2 * n_y, per_half)),
            dma((nz,)), dma((nz,)), dma((nz,)), dma((nz,)),
            dma((nz, 2)), dma((nz, 2)),
            dma((per_half,)), dma((nz,)),
            dma((4 * n_y - 1,)), dma((4,)), dma((2,)),
        ],
        compiler_params=pltpu.CompilerParams(collective_id=0, has_side_effects=True),
    )(x, pair, row_mask, residue_mask[None, :], gain[None, :], wq, wk, wv, wg, wo,
      pair_gain[None, :], bias_w.T, tensor_gain[None, :], left_w.T, right_w.T)


def back_kernel(mask_ref, key_ref, left_ref, right_ref, weight_ref, msa_ref, pair_ref,
                msa_out, out_ref, rows_ref, w_ref, rt_ref, r_hi, r_lo, scale_ref, t_hi, t_lo):
    step, cols, depth = pair_ref.shape
    sources, tall, packed = left_ref.shape
    total = rt_ref.shape[0]
    wide = packed // 2
    width = weight_ref.shape[0] // (w_ref.shape[1] // depth)
    n_rows = wide // width
    n_all = sources * n_rows
    at = pl.program_id(0)
    steps = pl.num_programs(0)

    msa_out[...] = msa_ref[...]

    @pl.when(at == 0)
    def _():
        for i in range(2 * tall):
            block = left_ref[:, i % tall, :]
            base = (i // tall) * wide
            rows = jnp.concatenate(
                [block[:, base + s * width:base + (s + 1) * width] for s in range(n_rows)], axis=0
            )
            hi, lo = split(rows)
            rows_ref[i * n_all:(i + 1) * n_all, :] = jnp.concatenate([hi, hi, lo], axis=1)
        for d in range(width):
            hi, lo = split(weight_ref[pl.ds(d, width, stride=width), :])
            w_ref[:, d * depth:(d + 1) * depth] = jnp.concatenate([hi, lo, hi], axis=0)
            for s in range(n_rows):
                spot = (d * n_rows + s) * sources
                rt_ref[spot:spot + sources, :] = right_ref[:, s * width + d, :]
        hi, lo = split(rt_ref[...].T)
        r_hi[...] = hi
        r_lo[...] = lo
        count = jnp.sum(right_ref[:, wide:, :depth], axis=0)
        own = pl.ds(pl.multiple_of(lax.axis_index("head") * cols, cols), cols)
        live = jnp.broadcast_to(key_ref[:, own].astype(jnp.float32), (depth, cols)).T
        scale_ref[...] = live * (1.0 / (count[0:1, :] + 0.001))

    left = rows_ref[pl.ds(pl.multiple_of(at * step * n_all, step * n_all), step * n_all), :]
    group = 2
    for d0 in range(0, width, group):
        t = mm(left, w_ref[:, d0 * depth:(d0 + group) * depth])
        hi, lo = split(t)
        for g in range(group):
            d = d0 + g
            for i in range(step):
                src = (slice(i * n_all, (i + 1) * n_all), slice(g * depth, (g + 1) * depth))
                dst = (slice(d * n_all, (d + 1) * n_all), slice(i * depth, (i + 1) * depth))
                t_hi[dst] = hi[src]
                t_lo[dst] = lo[src]
    update = mm(r_hi[...], t_hi[...]) + mm(r_lo[...], t_hi[...]) + mm(r_hi[...], t_lo[...])
    first = (lax.axis_index("row") * steps + at) * step
    for i in range(step):
        scale = scale_ref[...] * mask_ref[first + i].astype(jnp.float32)
        out_ref[i] = pair_ref[i] + update[:, i * depth:(i + 1) * depth] * scale


def back(residue_mask, left_in, right_all, weight, msa, pair):
    rows, cols, depth = pair.shape
    sources, _, _ = right_all.shape
    tall, packed = left_in.shape[2:]
    left_in = left_in.reshape(sources, tall, packed)
    wide = packed // 2
    n_rows, _, feat = msa.shape
    width = wide // n_rows
    total = sources * wide
    n_all = sources * n_rows
    step = 4
    steps = rows // step
    whole = lambda a: pl.BlockSpec(a.shape, lambda i: (0,) * a.ndim)
    msa_spec = pl.BlockSpec((n_rows, cols // steps, feat), lambda i: (0, i, 0))
    pair_spec = pl.BlockSpec((step, cols, depth), lambda i: (i, 0, 0))
    keys = residue_mask[None, :]
    b16 = jnp.bfloat16
    return pl.pallas_call(
        back_kernel,
        grid=(steps,),
        in_specs=[pl.BlockSpec(memory_space=pltpu.SMEM), whole(keys), whole(left_in), whole(right_all),
                  whole(weight), msa_spec, pair_spec],
        out_specs=(msa_spec, pair_spec),
        out_shape=(jax.ShapeDtypeStruct(msa.shape, jnp.float32), jax.ShapeDtypeStruct(pair.shape, jnp.float32)),
        scratch_shapes=[
            pltpu.VMEM((rows * n_all, 3 * width), b16),
            pltpu.VMEM((3 * width, width * depth), b16),
            pltpu.VMEM((total, cols), jnp.float32),
            pltpu.VMEM((cols, total), b16),
            pltpu.VMEM((cols, total), b16),
            pltpu.VMEM((cols, depth), jnp.float32),
            pltpu.VMEM((total, step * depth), b16),
            pltpu.VMEM((total, step * depth), b16),
        ],
        cost_estimate=pl.CostEstimate(flops=9 * 10**9, bytes_accessed=10**7, transcendentals=0),
    )(residue_mask, keys, left_in, right_all, weight, msa, pair)


def fused_body(
    sequence_matrix, pair_representation, alignment_row_mask, residue_mask, attention_scale_vector,
    asking_factor_matrix, lookup_factor_matrix, content_factor_matrix, sigmoid_factor_matrix,
    final_factor_matrix, pair_norm_gain, bias_weight, tensor_scale_vector, first_factor_matrix,
    second_factor_matrix, outer_weight,
):
    msa, left_in, right_all = front(
        lax.axis_size("row"), lax.axis_size("head"), sequence_matrix, pair_representation,
        alignment_row_mask, residue_mask, attention_scale_vector, asking_factor_matrix,
        lookup_factor_matrix, content_factor_matrix, sigmoid_factor_matrix, final_factor_matrix,
        pair_norm_gain, bias_weight, tensor_scale_vector, first_factor_matrix, second_factor_matrix,
    )
    return back(residue_mask, left_in, right_all, outer_weight, msa, pair_representation)


def fits(n_row, n_y, sequence_matrix, pair_representation, bias_weight, first_factor_matrix):
    rows, residues, feat = sequence_matrix.shape
    heads, opm = bias_weight.shape[1], first_factor_matrix.shape[1]
    n_rows, cols, pair_rows, nz = rows // n_row, residues // n_y, residues // n_row, n_row // 4
    if n_row % 4 or nz & (nz - 1) or nz % n_y or heads % (2 * n_y):
        return False
    group_width = heads // n_y // 2 * (feat // heads)
    return (
        n_rows * group_width == 128 and group_width == 64 and 2 * n_rows * opm == 128
        and cols % 128 == 0 and pair_rows % 16 == 0 and pair_representation.shape[2] == 128
        and n_row % 8 == 0
    )


def solution(mesh):
    placed = (P("row", "head", None), P("row", "head", None), P("row")) + (P(),) * 13
    n_row, n_y = mesh.shape["row"], mesh.shape["head"]

    def step(*args):
        chosen = fused_body if fits(n_row, n_y, args[0], args[1], args[11], args[13]) else body
        return jax.shard_map(
            chosen,
            mesh=mesh,
            in_specs=placed,
            out_specs=(P("row", "head", None), P("row", "head", None)),
            check_vma=False,
        )(*args)

    return step
```

```python
import functools
import math

import jax
import jax.numpy as jnp
from jax import lax
from jax.experimental import pallas as pl
from jax.experimental.pallas import tpu as pltpu
from jax.sharding import PartitionSpec as P


HIGH = lax.Precision.HIGHEST


def apply_layer_norm(values, gains):
    center = values - jnp.mean(values, axis=-1, keepdims=True)
    spread = jnp.mean(center * center, axis=-1, keepdims=True)
    return center * lax.rsqrt(spread + 1e-05) * gains


def split(x):
    hi = x.astype(jnp.bfloat16)
    lo = (x - hi.astype(jnp.float32)).astype(jnp.bfloat16)
    return hi, lo


def mm(a, b, dims=(((1,), (0,)), ((), ()))):
    return lax.dot_general(a, b, dims, preferred_element_type=jnp.float32)


def split_outside(x):
    hi = lax.reduce_precision(x, 8, 7)
    return hi.astype(jnp.bfloat16), lax.reduce_precision(x - hi, 8, 7).astype(jnp.bfloat16)


NT = (((1,), (1,)), ((), ()))


def bias_kernel(pair_ref, gain_ref, weight_ref, out_ref):
    rows, cols, width = pair_ref.shape
    w_hi, w_lo = split(weight_ref[...])
    heads = w_hi.shape[0]
    w_both = jnp.concatenate([w_hi, w_lo], axis=0)
    for r in range(rows):
        x = apply_layer_norm(pair_ref[r], gain_ref[...])
        x_hi, x_lo = split(x)
        both = mm(w_both, x_hi, NT)
        out_ref[r] = both[:heads] + both[heads:] + mm(w_hi, x_lo, NT)


def pair_bias(pair, gain, weight):
    rows, cols, width = pair.shape
    heads = weight.shape[1]
    step = 4
    return pl.pallas_call(
        bias_kernel,
        grid=(rows // step,),
        in_specs=[
            pl.BlockSpec((step, cols, width), lambda i: (i, 0, 0)),
            pl.BlockSpec((1, width), lambda i: (0, 0)),
            pl.BlockSpec((heads, width), lambda i: (0, 0)),
        ],
        out_specs=pl.BlockSpec((step, heads, cols), lambda i: (i, 0, 0)),
        out_shape=jax.ShapeDtypeStruct((rows, heads, cols), jnp.float32),
        cost_estimate=pl.CostEstimate(flops=10**9, bytes_accessed=5 * 10**6, transcendentals=0),
    )(pair, gain[None, :], weight.T)


def attend_kernel(x_ref, gain_ref, w_ref, bias_ref, key_ref, out_ref, q_ref, k_ref, v_ref):
    blocks, heads, depth, keys = bias_ref.shape
    n_rows = x_ref.shape[0]
    width = v_ref.shape[3] // 2
    local = heads * width
    rows = blocks * depth
    step = pl.program_id(0)

    @pl.when(step == 0)
    def _():
        w_hi, w_lo = split(w_ref[...])
        for s in range(n_rows):
            x_hi, x_lo = split(apply_layer_norm(x_ref[s], gain_ref[...]))
            made = mm(x_hi, w_hi) + mm(x_lo, w_hi) + mm(x_hi, w_lo)
            q_hi, q_lo = split(made[:, :local] * (1.0 / math.sqrt(width)))
            k_hi, k_lo = split(made[:, local:2 * local])
            v_hi, v_lo = split(made[:, 2 * local:])
            for h in range(heads):
                at = slice(h * width, (h + 1) * width)
                q_ref[s, h] = jnp.concatenate([q_hi[:, at], q_hi[:, at], q_lo[:, at]], axis=-1)
                k_ref[s, h] = jnp.concatenate([k_hi[:, at], k_lo[:, at], k_hi[:, at]], axis=-1)
                v_ref[s, h] = jnp.concatenate([v_hi[:, at], v_lo[:, at]], axis=-1)

    key_bias = key_ref[...]
    mine = pl.ds(pl.multiple_of(step * rows, rows), rows)
    for s in range(n_rows):
        pieces = []
        for h in range(heads):
            logits = mm(q_ref[s, h, mine, :], k_ref[s, h], NT)
            logits = logits + bias_ref[:, h].reshape(rows, keys) + key_bias
            largest = jnp.max(logits, axis=-1, keepdims=True)
            e = jnp.exp(logits - largest)
            total = jnp.sum(e, axis=-1, keepdims=True)
            e_hi, e_lo = split(e)
            v = v_ref[s, h]
            both = mm(e_hi, v)
            got = both[:, :width] + both[:, width:] + mm(e_lo, v[:, :width])
            pieces.append(got / total)
        out_ref[s] = jnp.concatenate(pieces, axis=-1)


def attend(x, gain, weight, bias, key_bias):
    n_rows, residues, features = x.shape
    groups, heads, depth, keys = bias.shape
    local = weight.shape[1] // 3
    width = local // heads
    blocks = max(1, 128 // depth)
    rows = blocks * depth
    return pl.pallas_call(
        attend_kernel,
        grid=(groups // blocks,),
        in_specs=[
            pl.BlockSpec(x.shape, lambda i: (0, 0, 0)),
            pl.BlockSpec((1, features), lambda i: (0, 0)),
            pl.BlockSpec(weight.shape, lambda i: (0, 0)),
            pl.BlockSpec((blocks, heads, depth, keys), lambda i: (i, 0, 0, 0)),
            pl.BlockSpec((1, keys), lambda i: (0, 0)),
        ],
        out_specs=pl.BlockSpec((n_rows, rows, local), lambda i: (0, i, 0)),
        out_shape=jax.ShapeDtypeStruct((n_rows, residues, local), jnp.float32),
        scratch_shapes=[
            pltpu.VMEM((n_rows, heads, residues, 3 * width), jnp.bfloat16),
            pltpu.VMEM((n_rows, heads, residues, 3 * width), jnp.bfloat16),
            pltpu.VMEM((n_rows, heads, residues, 2 * width), jnp.bfloat16),
        ],
        cost_estimate=pl.CostEstimate(flops=4 * 10**9, bytes_accessed=6 * 10**6, transcendentals=2 * 10**6),
    )(x, gain[None, :], weight, bias, key_bias)


def outer_kernel(scale_ref, left_ref, weight_ref, right_ref, live_ref, pair_ref, out_ref,
                 r_hi, r_lo, t_hi, t_lo):
    step, cols, depth = pair_ref.shape
    rows_all = r_hi.shape[1]
    n_rows = left_ref.shape[0] // step
    width = rows_all // n_rows
    me = pl.program_id(0)

    @pl.when(me == 0)
    def _():
        hi, lo = split(right_ref[...].T)
        r_hi[...] = hi
        r_lo[...] = lo

    left = left_ref[...]
    group = 2
    for d0 in range(0, width, group):
        t = mm(left, weight_ref[:, d0 * depth:(d0 + group) * depth])
        hi, lo = split(t)
        for g in range(group):
            d = d0 + g
            for i in range(step):
                src = (slice(i * n_rows, (i + 1) * n_rows), slice(g * depth, (g + 1) * depth))
                dst = (slice(d * n_rows, (d + 1) * n_rows), slice(i * depth, (i + 1) * depth))
                t_hi[dst] = hi[src]
                t_lo[dst] = lo[src]
    update = mm(r_hi[...], t_hi[...]) + mm(r_lo[...], t_hi[...]) + mm(r_hi[...], t_lo[...])
    for i in range(step):
        norm = scale_ref[me * step + i] * live_ref[...] + 0.001
        out_ref[i] = pair_ref[i] + update[:, i * depth:(i + 1) * depth] / norm


def outer_mean(scale, left, weight, right, live, pair):
    rows, cols, depth = pair.shape
    total = right.shape[0]
    n_rows = left.shape[0] // rows
    packed = left.shape[1]
    step = 4
    return pl.pallas_call(
        outer_kernel,
        grid=(rows // step,),
        in_specs=[
            pl.BlockSpec(memory_space=pltpu.SMEM),
            pl.BlockSpec((step * n_rows, packed), lambda i: (i, 0)),
            pl.BlockSpec(weight.shape, lambda i: (0, 0)),
            pl.BlockSpec(right.shape, lambda i: (0, 0)),
            pl.BlockSpec((cols, 1), lambda i: (0, 0)),
            pl.BlockSpec((step, cols, depth), lambda i: (i, 0, 0)),
        ],
        out_specs=pl.BlockSpec((step, cols, depth), lambda i: (i, 0, 0)),
        out_shape=jax.ShapeDtypeStruct(pair.shape, jnp.float32),
        scratch_shapes=[
            pltpu.VMEM((cols, total), jnp.bfloat16),
            pltpu.VMEM((cols, total), jnp.bfloat16),
            pltpu.VMEM((total, step * depth), jnp.bfloat16),
            pltpu.VMEM((total, step * depth), jnp.bfloat16),
        ],
        cost_estimate=pl.CostEstimate(flops=9 * 10**9, bytes_accessed=10**7, transcendentals=0),
    )(scale, left, weight, right, live, pair)


def gather_kernel(n, block_ref, out_ref, own_sem, send_sem, recv_sem):
    me = lax.axis_index("row")
    core = me % 2
    x = (me // 2) % 2
    nz = n // 4
    z = me // 4

    def place(zz, xx, cc):
        return (zz * 2 + xx) * 2 + cc

    barrier = pltpu.get_barrier_semaphore()
    up_ok, down_ok = z + 1 < nz, z >= 1

    def greet(target):
        pl.semaphore_signal(barrier, inc=1, device_id={"row": target},
                            device_id_type=pl.DeviceIdType.MESH)

    greet(place(z, x, 1 - core))
    greet(place(z, 1 - x, core))
    pl.when(up_ok)(lambda: greet(place(z + 1, x, core)))
    pl.when(down_ok)(lambda: greet(place(z - 1, x, core)))
    peers = 2 + jnp.where(up_ok, 1, 0) + jnp.where(down_ok, 1, 0)
    pl.semaphore_wait(barrier, peers)

    own = pltpu.make_async_copy(block_ref, out_ref.at[me], own_sem)
    own.start()

    def sends(d, other):
        found = []
        first = core == 0
        if other == 0:
            cross = (z >= 0) if d == 0 else jnp.logical_not(first)
            run = z >= 0
        else:
            cross = None
            run = first
        if d <= 0:
            found.append((jnp.logical_and(run, up_ok), 0, lambda: place(z + 1, x, core)))
        if d >= 0:
            found.append((jnp.logical_and(run, down_ok), 1, lambda: place(z - 1, x, core)))
        if cross is not None:
            found.append((cross, 2, lambda: place(z, 1 - x, core)))
        found.append((z >= 0, 3, lambda: place(z, x, 1 - core)))
        return found

    def copy(source, kind, target, mine):
        return pltpu.make_async_remote_copy(
            src_ref=block_ref if mine else out_ref.at[source],
            dst_ref=out_ref.at[source],
            send_sem=send_sem.at[kind, source],
            recv_sem=recv_sem.at[source],
            device_id={"row": target},
            device_id_type=pl.DeviceIdType.MESH,
        )

    hops = [(0, 0), (0, 1)]
    for far in range(1, nz):
        hops += [(-far, 0), (far, 0), (-far, 1), (far, 1)]

    def each(action):
        for d, other in hops:
            source = place(z + d, (x + other) % 2, core)
            mine = d == 0 and other == 0
            there = jnp.logical_and(z + d >= 0, z + d < nz)

            @pl.when(there)
            def _(d=d, other=other, source=source, mine=mine):
                action(d, other, source, mine)

    def forward(d, other, source, mine):
        if not mine:
            copy(source, 3, place(z, x, 1 - core), False).wait_recv()
        for ok, kind, target in sends(d, other):
            pl.when(ok)(lambda kind=kind, target=target: copy(source, kind, target(), mine).start())

    def finish(d, other, source, mine):
        for ok, kind, target in sends(d, other):
            pl.when(ok)(lambda kind=kind, target=target: copy(source, kind, target(), mine).wait_send())

    each(forward)
    for k in range(n // 2):
        copy(2 * k + 1 - core, 3, place(z, x, 1 - core), False).wait_recv()
    each(finish)
    own.wait()


def gather_rows(block, n, ident):
    return pl.pallas_call(
        functools.partial(gather_kernel, n),
        out_shape=jax.ShapeDtypeStruct((n,) + block.shape, block.dtype),
        in_specs=[pl.BlockSpec(memory_space=pltpu.VMEM)],
        out_specs=pl.BlockSpec(memory_space=pl.ANY),
        scratch_shapes=[
            pltpu.SemaphoreType.DMA,
            pltpu.SemaphoreType.DMA((4, n)),
            pltpu.SemaphoreType.DMA((n,)),
        ],
        compiler_params=pltpu.CompilerParams(collective_id=ident, has_side_effects=True),
    )(block)


def around(n):
    return [[(src, (src + k) % n) for src in range(n)] for k in range(n)]


def gather_heads(block, n, index, axis):
    size = block.shape[axis]
    shape = list(block.shape)
    shape[axis] = size * n
    whole = jnp.zeros(shape, block.dtype)
    for k in range(n):
        part = block if k == 0 else lax.ppermute(block, "head", around(n)[k])
        whole = lax.dynamic_update_slice_in_dim(whole, part, ((index - k) % n) * size, axis)
    return whole


def exchange_heads(block, n, index, split_axis, concat_axis):
    size = block.shape[split_axis] // n
    shape = list(block.shape)
    shape[split_axis] = size
    length = shape[concat_axis]
    shape[concat_axis] = length * n
    whole = jnp.zeros(shape, block.dtype)
    for k in range(n):
        part = lax.dynamic_slice_in_dim(block, ((index + k) % n) * size, size, split_axis)
        if k:
            part = lax.ppermute(part, "head", around(n)[k])
        whole = lax.dynamic_update_slice_in_dim(whole, part, ((index - k) % n) * length, concat_axis)
    return whole


def body(
    sequence_matrix,
    pair_representation,
    alignment_row_mask,
    residue_mask,
    attention_scale_vector,
    asking_factor_matrix,
    lookup_factor_matrix,
    content_factor_matrix,
    sigmoid_factor_matrix,
    final_factor_matrix,
    pair_norm_gain,
    bias_weight,
    tensor_scale_vector,
    first_factor_matrix,
    second_factor_matrix,
    outer_weight,
):
    head_count = lax.axis_size("head")
    head_index = lax.axis_index("head")
    row_index = lax.axis_index("row")
    row_count = lax.axis_size("row")
    n_rows, col_count, width = sequence_matrix.shape
    residues = col_count * head_count
    pair_rows = pair_representation.shape[0]
    pair_depth = pair_representation.shape[2]
    heads_all = bias_weight.shape[1]
    head_width = width // heads_all
    local_heads = heads_all // head_count
    local_width = local_heads * head_width
    opm_width = first_factor_matrix.shape[1]

    sequence_all = gather_heads(sequence_matrix, head_count, head_index, 1)

    bias_all = pair_bias(pair_representation, pair_norm_gain, bias_weight)
    bias_part = exchange_heads(
        bias_all.transpose(1, 0, 2), head_count, head_index, 0, 2
    )
    bias = gather_rows(bias_part, row_count, 0)
    key_bias = ((residue_mask.astype(jnp.float32) - 1.0) * 1000000000.0)[None, :]

    weights = jnp.concatenate(
        [
            lax.dynamic_slice_in_dim(w, head_index * local_width, local_width, 1)
            for w in (asking_factor_matrix, lookup_factor_matrix, content_factor_matrix)
        ],
        axis=1,
    )
    attended = attend(sequence_all, attention_scale_vector, weights, bias, key_bias)
    norm_mine = apply_layer_norm(sequence_matrix, attention_scale_vector)
    gate = jax.nn.sigmoid(
        jnp.einsum("sic,ce->sie", norm_mine, sigmoid_factor_matrix, precision=HIGH)
    )
    returned_values = exchange_heads(attended, head_count, head_index, 1, 2) * gate
    alignment_updated = sequence_matrix + jnp.einsum(
        "jna,ab->jnb", returned_values, final_factor_matrix, precision=HIGH
    )

    outer_product_norm = apply_layer_norm(alignment_updated, tensor_scale_vector)
    live_cols = lax.dynamic_slice_in_dim(residue_mask, head_index * col_count, col_count).astype(
        jnp.float32
    )
    row_live = alignment_row_mask.astype(jnp.float32)
    live = row_live[:, None] * live_cols[None, :]
    left_side = (
        jnp.einsum("sic,co->soi", outer_product_norm, first_factor_matrix, precision=HIGH)
        * live[:, None, :]
    )
    right = (
        jnp.einsum("sic,co->soi", outer_product_norm, second_factor_matrix, precision=HIGH)
        * live[:, None, :]
    )
    left_all = gather_heads(left_side, head_count, head_index, 1)
    carried = jnp.broadcast_to(row_live[:, None, None], (n_rows, 8, col_count))
    sides = gather_rows(jnp.concatenate([left_all, right, carried], axis=1), row_count, 1)
    sides = sides.reshape(row_count * n_rows, -1, col_count)
    left_width = head_count * opm_width
    first_row = row_index * pair_rows
    left_mine = lax.dynamic_slice(
        sides,
        (0, (first_row // col_count) * opm_width, first_row % col_count),
        (row_count * n_rows, opm_width, pair_rows),
    )
    right_all = sides[:, left_width:]
    total_rows = row_count * n_rows
    count = jnp.sum(right_all[:, opm_width, 0])
    right_rows = right_all[:, :opm_width].transpose(1, 0, 2).reshape(
        opm_width * total_rows, col_count
    )
    left_rows = left_mine.transpose(2, 0, 1).reshape(pair_rows * total_rows, opm_width)
    l_hi, l_lo = split_outside(left_rows)
    w_hi, w_lo = split_outside(outer_weight.reshape(opm_width, opm_width * pair_depth))
    rows_live = lax.dynamic_slice_in_dim(residue_mask, row_index * pair_rows, pair_rows).astype(
        jnp.float32
    )
    pair_out = outer_mean(
        count * rows_live,
        jnp.concatenate([l_hi, l_hi, l_lo], axis=1),
        jnp.concatenate([w_hi, w_lo, w_hi], axis=0),
        right_rows,
        live_cols[:, None],
        pair_representation,
    )
    return alignment_updated, pair_out


def ln(values, gains):
    return apply_layer_norm(values, gains)


def front_kernel(
    x_hbm, pair_hbm, row_mask, key_ref, gain_ref, wq_hbm, wk_hbm, wv_hbm, wg_hbm, wo_hbm,
    pair_gain, bias_w, tensor_gain, left_w, right_w,
    msa_hbm, left_in, right_all,
    x_ref, pair_ref, wq_ref, wk_ref, wv_ref, wg_ref, wo_ref, msa_ref, wpair_ref, group_ref,
    bias_ref, xn_ref, q_ref, k_ref, v_ref, gate_ref, att_out, att_in, right_buf, left_loc, left_own,
    load_sem, pair_sem, out_sem, s1_send, s1_recv, n_send, n_recv, z_send, z_recv, x_send, x_recv,
    a_send, a_recv, rz_send, rz_recv, rx_send, rx_recv, rc_send, rc_recv,
    l1_send, l1_recv, l2_send, l2_recv, self_sem, keep_sem,
):
    nz, _, chunks, _, n_y, group_heads, sub, cols = bias_ref.shape
    n_rows, _, feat = x_ref.shape
    heads = bias_w.shape[0]
    keys = n_y * cols
    width = v_ref.shape[3] // 2
    group_width = group_heads * width
    local_width = 2 * group_width
    per_half = nz // n_y
    plane = cols // per_half
    pair_width = pair_ref.shape[2]
    opm = left_w.shape[0]

    me, y = lax.axis_index("row"), lax.axis_index("head")
    c, x, z = me % 2, (me // 2) % 2, me // 4
    half = z // per_half

    def place(zz, xx, cc):
        return (zz * 2 + xx) * 2 + cc

    def across(d):
        out, bit = z, 1
        while bit <= d:
            if d & bit:
                out = out + bit * (1 - 2 * ((out // bit) % 2))
            bit *= 2
        return out

    def plane_at(p):
        if p < 2:
            return across(p)
        return jnp.where(z < nz // 2, p, nz - 1 - p)

    def remote(src, dst, send, recv, row, head):
        return pltpu.make_async_remote_copy(
            src_ref=src, dst_ref=dst, send_sem=send, recv_sem=recv,
            device_id={"row": row, "head": head}, device_id_type=pl.DeviceIdType.MESH,
        )

    def arrived(dst, send, recv):
        remote(dst, dst, send, recv, place(z, x, 1 - c), y).wait_recv()

    pending = []

    def go(copy):
        copy.start()
        pending.append(copy)

    loads = {}
    for at, (src, dst) in enumerate(
        [(x_hbm, x_ref), (wq_hbm, wq_ref), (wk_hbm, wk_ref), (wv_hbm, wv_ref), (wg_hbm, wg_ref), (wo_hbm, wo_ref)]
    ):
        loads[at] = pltpu.make_async_copy(src, dst, load_sem.at[at])
    pair_loads = [
        pltpu.make_async_copy(
            pair_hbm.at[pl.ds(k * sub, sub)], pair_ref.at[pl.ds(k * sub, sub)], pair_sem.at[k]
        )
        for k in range(chunks)
    ]
    loads[0].start()
    for copy in pair_loads:
        copy.start()
    for at in range(1, 6):
        loads[at].start()

    barrier = pltpu.get_barrier_semaphore()
    peers = []
    for dx in range(2):
        for dc in range(2):
            for dy in range(n_y):
                if dx or dc or dy:
                    peers.append((place(z, (x + dx) % 2, (c + dc) % 2), (y + dy) % n_y))
    for d in range(1, nz):
        peers.append((place(across(d), x, c), y))
    for row, head in peers:
        pl.semaphore_signal(barrier, inc=1, device_id={"row": row, "head": head},
                            device_id_type=pl.DeviceIdType.MESH)

    w_hi, w_lo = split(bias_w[...])
    spread = sub * heads
    at_row = lax.broadcasted_iota(jnp.int32, (heads, sub, pair_width), 1).reshape(spread, pair_width)
    zero = jnp.zeros((spread, pair_width), jnp.float32)

    def rows_of(part):
        part = part.astype(jnp.float32)
        return jnp.broadcast_to(part[:, None, :], (heads, sub, pair_width)).reshape(spread, pair_width)

    rep_hi, rep_lo = rows_of(w_hi), rows_of(w_lo)
    for t in range(sub // 2):
        first, second = at_row == 2 * t, at_row == 2 * t + 1
        both = [
            jnp.concatenate([jnp.where(first, rep, zero), jnp.where(second, rep, zero)], axis=1)
            for rep in (rep_hi, rep_lo)
        ]
        wpair_ref[t] = jnp.concatenate(both, axis=0).astype(jnp.bfloat16)

    def bias_chunk(k):
        pair_loads[k].wait()
        total = None
        for t in range(sub // 2):
            at = k * sub + 2 * t
            pieces = [split(ln(pair_ref[at + e], pair_gain[...])) for e in range(2)]
            hi = jnp.concatenate([pieces[0][0], pieces[1][0]], axis=1)
            lo = jnp.concatenate([pieces[0][1], pieces[1][1]], axis=1)
            both = mm(wpair_ref[t], hi, NT)
            part = both[:spread] + both[spread:] + mm(wpair_ref[t, :spread], lo, NT)
            total = part if total is None else total + part
        group_ref[k] = total.reshape(2 * n_y, group_heads, sub, cols)
        bias_ref[z, x, k, c, y] = group_ref[k, y * 2 + c]

    labels = [(dy, dc) for dy in range(n_y) for dc in range(2) if dy or dc]

    def stage_one(k):
        for at, (dy, dc) in enumerate(labels):
            ty, tc = (y + dy) % n_y, (c + dc) % 2
            go(remote(group_ref.at[k, ty * 2 + tc], bias_ref.at[z, x, k, c, y],
                      s1_send.at[k, at], s1_recv.at[k, at], place(z, x, tc), ty))

    def stage_two(k):
        for at, (dy, dc) in enumerate(labels):
            sy, sc = (y + n_y - dy) % n_y, (c + dc) % 2
            arrived(bias_ref.at[z, x, k, sc, sy], s1_send.at[k, at], s1_recv.at[k, at])
        own = bias_ref.at[z, x, k]
        go(remote(own, own, x_send.at[z, k], x_recv.at[z, k], place(z, 1 - x, c), y))
        for up in range(2):
            relay(up, z, k)

    def relay_copy(up, zz, k):
        block = bias_ref.at[zz, x, k]
        return remote(block, block, z_send.at[up, zz, k], z_recv.at[zz, k],
                      place(z + 1 if up else z - 1, x, c), y)

    def can_relay(up):
        return z + 1 < nz if up else z >= 1

    def relay(up, zz, k):
        pl.when(can_relay(up))(lambda: relay_copy(up, zz, k).start())

    def source(up, j):
        return (z - j, z >= j) if up else (z + j, z + j < nz)

    def pass_on(j, k):
        for up in range(2):
            zz, there = source(up, j)

            @pl.when(there)
            def _(up=up, zz=zz):
                block = bias_ref.at[zz, x, k]
                arrived(block, z_send.at[0, 0, k], z_recv.at[zz, k])
                if j + 1 < nz:
                    relay(up, zz, k)
                remote(block, block, x_send.at[zz, k], x_recv.at[zz, k], place(z, 1 - x, c), y).start()

    bias_chunk(0)
    pl.semaphore_wait(barrier, len(peers))
    stage_one(0)
    for k in range(1, chunks):
        bias_chunk(k)
        stage_one(k)
        if k >= 2:
            stage_two(k - 2)

    loads[0].wait()
    for s in range(n_rows):
        xn_ref[y, c, s] = ln(x_ref[s], gain_ref[...])
        own_x = xn_ref.at[y, c, s]
        for dy in range(1, n_y):
            go(remote(own_x, own_x, n_send.at[dy, s], n_recv.at[dy, s], place(z, x, c), (y + dy) % n_y))
        go(remote(own_x, own_x, n_send.at[0, s], n_recv.at[0, s], place(z, x, 1 - c), y))
    stage_two(chunks - 2)

    for at in (1, 2, 3):
        loads[at].wait()
    mine = pl.ds(pl.multiple_of(y * local_width, local_width), local_width)
    picked = []
    for ref in (wq_ref, wk_ref, wv_ref):
        whole = ref[:, mine]
        picked.append(jnp.where(c == 0, whole[:, :group_width], whole[:, group_width:]))
    wa_hi, wa_lo = split(jnp.concatenate(picked, axis=1))

    def project(yy, cc, rows=range(n_rows)):
        spot = pl.ds(pl.multiple_of(yy * cols, cols), cols)
        for s in rows:
            hi, lo = split(xn_ref[yy, cc, s])
            made = mm(hi, wa_hi) + mm(lo, wa_hi) + mm(hi, wa_lo)
            q_hi, q_lo = split(made[:, :group_width] * (1.0 / math.sqrt(width)))
            k_hi, k_lo = split(made[:, group_width:2 * group_width])
            v_hi, v_lo = split(made[:, 2 * group_width:])
            for h in range(group_heads):
                at = slice(h * width, (h + 1) * width)
                to = cc * n_rows + s
                q_ref[to, h, spot, :] = jnp.concatenate([q_hi[:, at], q_hi[:, at], q_lo[:, at]], axis=-1)
                k_ref[to, h, spot, :] = jnp.concatenate([k_hi[:, at], k_lo[:, at], k_hi[:, at]], axis=-1)
                v_ref[to, h, spot, :] = jnp.concatenate([v_hi[:, at], v_lo[:, at]], axis=-1)

    project(y, c)
    stage_two(chunks - 1)
    loads[4].wait()
    g_hi, g_lo = split(wg_ref[...])
    for s in range(n_rows):
        hi, lo = split(xn_ref[y, c, s])
        gate_ref[s] = jax.nn.sigmoid(mm(hi, g_hi) + mm(lo, g_hi) + mm(hi, g_lo))
    for s in range(n_rows):
        arrived(xn_ref.at[y, 1 - c, s], n_send.at[0, s], n_recv.at[0, s])
    project(y, 1 - c)

    tasks = [(j, k) for j in range(1, nz) for k in range(chunks)]
    early = tasks[:chunks]
    late = tasks[chunks:2 * chunks]
    rest = tasks[2 * chunks:]
    for j, k in early:
        pass_on(j, k)
    for dy in range(1, n_y):
        sy = (y + n_y - dy) % n_y
        for s in range(n_rows):
            block = xn_ref.at[sy, c, s]
            arrived(block, n_send.at[dy, s], n_recv.at[dy, s])
            go(remote(block, block, n_send.at[n_y + dy, s], n_recv.at[n_y + dy, s], place(z, x, 1 - c), y))
            project(sy, c, [s])
            share = len(late) // (n_rows * (n_y - 1))
            for j, k in late[:share] if s + 1 < n_rows or dy + 1 < n_y else late:
                pass_on(j, k)
            late = late[share:]
    for dy in range(1, n_y):
        sy = (y + n_y - dy) % n_y
        for s in range(n_rows):
            arrived(xn_ref.at[sy, 1 - c, s], n_send.at[n_y + dy, s], n_recv.at[n_y + dy, s])
        project(sy, 1 - c)

    key_bias = (key_ref[...].astype(jnp.float32) - 1.0) * 1000000000.0

    def attended_copy(d, ct):
        zz = plane_at(d)
        return remote(att_out.at[d, ct], att_in.at[y * 2 + c, zz % per_half],
                      a_send.at[d, ct], a_recv.at[y * 2 + c, zz % per_half],
                      place(z, x, ct), zz // per_half)

    def is_mine(d, ct):
        return jnp.logical_and(plane_at(d) // per_half == y, ct == c)

    def attend_plane(d):
        zz = plane_at(d)
        for k in range(chunks):
            arrived(bias_ref.at[zz, 1 - x, k], x_send.at[0, k], x_recv.at[zz, k])
        queries = pl.ds(pl.multiple_of(zz * plane, plane), plane)

        def unit(ct, carry):
            pieces = []
            for s in range(n_rows):
                row = ct * n_rows + s
                for h in range(group_heads):
                    logits = mm(q_ref[row, h, queries, :], k_ref[row, h], NT)
                    tiles = [
                        jnp.concatenate(
                            [bias_ref[zz, xx, :, cc, yy, h].reshape(chunks * sub, cols) for yy in range(n_y)],
                            axis=1,
                        )
                        for xx in range(2)
                        for cc in range(2)
                    ]
                    logits = logits + jnp.concatenate(tiles, axis=0) + key_bias
                    largest = jnp.max(logits, axis=-1, keepdims=True)
                    e = jnp.exp(logits - largest)
                    total = jnp.sum(e, axis=-1, keepdims=True)
                    e_hi, e_lo = split(e)
                    v = v_ref[row, h]
                    both = mm(e_hi, v)
                    got = both[:, :width] + both[:, width:] + mm(e_lo, v[:, :width])
                    pieces.append(got / total)
            value = jnp.concatenate(pieces, axis=-1)
            att_out[d, ct] = value

            @pl.when(is_mine(d, ct))
            def _():
                att_in[y * 2 + c, zz % per_half] = value

            @pl.when(jnp.logical_not(is_mine(d, ct)))
            def _():
                attended_copy(d, ct).start()

            return carry

        lax.fori_loop(0, 2, unit, 0)

    for d in range(nz):
        attend_plane(d)
        share = -(-len(rest) // 2) if d == 0 else len(rest)
        for j, k in rest[:share]:
            pass_on(j, k)
        rest = rest[share:]

    for dy, dc in labels:
        sy, sc = (y + n_y - dy) % n_y, (c + dc) % 2
        for p in range(per_half):
            arrived(att_in.at[sy * 2 + sc, p], a_send.at[0, 0], a_recv.at[sy * 2 + sc, p])

    loads[5].wait()
    o_hi, o_lo = split(wo_ref[...])
    wide = n_rows * opm
    left_hi, left_lo = split(left_w[...])
    left_both = jnp.concatenate([left_hi, left_lo], axis=0)
    right_hi, right_lo = split(right_w[...])
    right_both = jnp.concatenate([right_hi, right_lo], axis=0)
    lefts = []
    count = jnp.zeros((sub, cols), jnp.float32)
    for s in range(n_rows):
        at = slice(s * group_width, (s + 1) * group_width)
        whole = jnp.concatenate(
            [
                jnp.concatenate([att_in[g, p][:, at] for p in range(per_half)], axis=0)
                for g in range(2 * n_y)
            ],
            axis=1,
        ) * gate_ref[s]
        hi, lo = split(whole)
        out = x_ref[s] + (mm(hi, o_hi) + mm(lo, o_hi) + mm(hi, o_lo))
        msa_ref[s] = out
        t_hi, t_lo = split(ln(out, tensor_gain[...]))
        live = row_mask[s].astype(jnp.float32)
        both = mm(right_both, t_hi, NT)
        right_buf[z, x, s * opm:(s + 1) * opm, :] = (both[:opm] + both[opm:] + mm(right_hi, t_lo, NT)) * live
        both = mm(t_hi, left_both, NT)
        lefts.append((both[:, :opm] + both[:, opm:] + mm(t_lo, left_hi, NT)) * live)
        count = count + live
    right_buf[z, x, wide:, :] = count

    left = jnp.concatenate(lefts, axis=1)
    blocks = per_half * 4
    tall = left.shape[0] // blocks // 2
    left = left.reshape(blocks, 2, tall, wide)
    left_loc[...] = jnp.concatenate([left[:, 0], left[:, 1]], axis=2)

    def left_copy(p):
        return remote(left_loc.at[pl.ds(p * 4, 4)], left_own.at[z], l1_send.at[p], l1_recv.at[z],
                      place(y * per_half + p, x, c), y)

    for p in range(per_half):
        here = y * per_half + p == z

        @pl.when(here)
        def _(p=p):
            left_own[z] = left_loc[p * 4:(p + 1) * 4]

        pl.when(jnp.logical_not(here))(lambda p=p: left_copy(p).start())

    def keep(zz, far, index):
        xx = x if far == 0 else 1 - x
        block, to = right_buf.at[zz, xx], right_all.at[place(zz, xx, c)]
        own = pltpu.make_async_copy(block, to, keep_sem.at[zz, far])
        other = remote(block, to, rc_send.at[zz, far], rc_recv.at[zz, far], place(z, x, 1 - c), y)
        return own, other

    def right_relay(up, zz):
        block = right_buf.at[zz, x]
        return remote(block, block, rz_send.at[up, zz], rz_recv.at[zz], place(z + 1 if up else z - 1, x, c), y)

    def right_cross(zz):
        block = right_buf.at[zz, x]
        return remote(block, block, rx_send.at[zz], rx_recv.at[zz], place(z, 1 - x, c), y)

    for up in range(2):
        pl.when(can_relay(up))(lambda up=up: right_relay(up, z).start())
    right_cross(z).start()
    for copy in keep(z, 0, 0):
        copy.start()
    keep_msa = pltpu.make_async_copy(msa_ref, msa_hbm, out_sem)
    keep_msa.start()

    def right_pass(j):
        for up in range(2):
            zz, there = source(up, j)

            @pl.when(there)
            def _(up=up, zz=zz):
                arrived(right_buf.at[zz, x], rz_send.at[0, 0], rz_recv.at[zz])
                if j + 1 < nz:
                    pl.when(can_relay(up))(lambda: right_relay(up, zz).start())
                right_cross(zz).start()
                for copy in keep(zz, 0, j):
                    copy.start()

    right_pass(1)
    owner = half == y

    def final_copy(at, dx, dc, dy):
        tx, tc, ty = (x + dx) % 2, (c + dc) % 2, (y + dy) % n_y
        return remote(left_own.at[:, tx * 2 + tc], left_in.at[:, x * 2 + c], l2_send.at[at],
                      l2_recv.at[x * 2 + c], place(z, tx, tc), ty)

    finals = [(dx, dc, dy) for dx in range(2) for dc in range(2) for dy in range(n_y) if dx or dc or dy]

    @pl.when(owner)
    def _():
        for d in range(1, nz):
            zz = across(d)
            arrived(left_own.at[zz], l1_send.at[0], l1_recv.at[zz])
        for at, (dx, dc, dy) in enumerate(finals):
            final_copy(at, dx, dc, dy).start()
        pltpu.make_async_copy(left_own.at[:, x * 2 + c], left_in.at[:, x * 2 + c], self_sem.at[1]).start()

    def right_far(zz):
        arrived(right_buf.at[zz, 1 - x], rx_send.at[0], rx_recv.at[zz])
        for copy in keep(zz, 1, 0):
            copy.start()

    for j in range(2, nz):
        right_far(plane_at(j - 2))
        right_pass(j)
    for j in range(nz - 2, nz):
        right_far(plane_at(j))

    for xx in range(2):
        for cc in range(2):
            mine_too = jnp.logical_and(owner, jnp.logical_and(xx == x, cc == c))

            @pl.when(jnp.logical_not(mine_too))
            def _(xx=xx, cc=cc):
                arrived(left_in.at[:, xx * 2 + cc], l2_send.at[0], l2_recv.at[xx * 2 + cc])

    for zz in range(nz):
        for far in range(2):
            block = right_all.at[place(zz, x if far == 0 else 1 - x, 1 - c)]
            arrived(block, rc_send.at[zz, far], rc_recv.at[zz, far])

    for copy in pending:
        copy.wait_send()
    for zz in range(nz):
        for k in range(chunks):
            block = bias_ref.at[zz, x, k]

            @pl.when(zz != z)
            def _(zz=zz, k=k, block=block):
                remote(block, block, x_send.at[zz, k], x_recv.at[zz, k], place(z, 1 - x, c), y).wait_send()

            for up in range(2):
                goes = jnp.logical_and(can_relay(up), zz <= z if up else zz >= z)
                pl.when(goes)(lambda up=up, zz=zz, k=k: relay_copy(up, zz, k).wait_send())
        for up in range(2):
            goes = jnp.logical_and(can_relay(up), zz <= z if up else zz >= z)
            pl.when(goes)(lambda up=up, zz=zz: right_relay(up, zz).wait_send())
        right_cross(zz).wait_send()
        for far in range(2):
            own, other = keep(zz, far, 0)
            own.wait()
            other.wait_send()
    for d in range(nz):
        for ct in range(2):
            pl.when(jnp.logical_not(is_mine(d, ct)))(lambda d=d, ct=ct: attended_copy(d, ct).wait_send())
    for p in range(per_half):
        pl.when(y * per_half + p != z)(lambda p=p: left_copy(p).wait_send())

    @pl.when(owner)
    def _():
        for at, (dx, dc, dy) in enumerate(finals):
            final_copy(at, dx, dc, dy).wait_send()
        pltpu.make_async_copy(left_own.at[:, x * 2 + c], left_in.at[:, x * 2 + c], self_sem.at[1]).wait()

    keep_msa.wait()


def front(n_row, n_y, x, pair, row_mask, residue_mask, gain, wq, wk, wv, wg, wo,
          pair_gain, bias_w, tensor_gain, left_w, right_w):
    n_rows, cols, feat = x.shape
    pair_rows, _, pair_width = pair.shape
    heads = bias_w.shape[1]
    width = feat // heads
    group_heads = heads // n_y // 2
    nz, sub = n_row // 4, 8
    chunks = pair_rows // sub
    keys = n_y * cols
    per_half = nz // n_y
    plane = cols // per_half
    opm = left_w.shape[1]
    wide = n_rows * opm
    f32, b16 = jnp.float32, jnp.bfloat16
    any_spec, vmem = pl.BlockSpec(memory_space=pl.ANY), pl.BlockSpec(memory_space=pltpu.VMEM)
    dma = pltpu.SemaphoreType.DMA
    labels = 2 * n_y - 1
    return pl.pallas_call(
        front_kernel,
        out_shape=(
            jax.ShapeDtypeStruct(x.shape, f32),
            jax.ShapeDtypeStruct((nz, 4, pair_rows // 2, 2 * wide), f32),
            jax.ShapeDtypeStruct((n_row, wide + sub, cols), f32),
        ),
        in_specs=[any_spec, any_spec, pl.BlockSpec(memory_space=pltpu.SMEM), vmem, vmem]
        + [any_spec] * 5 + [vmem] * 5,
        out_specs=(any_spec, any_spec, any_spec),
        scratch_shapes=[
            pltpu.VMEM(x.shape, f32),
            pltpu.VMEM(pair.shape, f32),
        ]
        + [pltpu.VMEM((feat, feat), f32)] * 5
        + [
            pltpu.VMEM(x.shape, f32),
            pltpu.VMEM((sub // 2, 2 * sub * heads, 2 * pair_width), b16),
            pltpu.VMEM((chunks, 2 * n_y, group_heads, sub, cols), f32),
            pltpu.VMEM((nz, 2, chunks, 2, n_y, group_heads, sub, cols), f32),
            pltpu.VMEM((n_y, 2, n_rows, cols, feat), f32),
            pltpu.VMEM((2 * n_rows, group_heads, keys, 3 * width), b16),
            pltpu.VMEM((2 * n_rows, group_heads, keys, 3 * width), b16),
            pltpu.VMEM((2 * n_rows, group_heads, keys, 2 * width), b16),
            pltpu.VMEM(x.shape, f32),
            pltpu.VMEM((nz, 2, plane, n_rows * group_heads * width), f32),
            pltpu.VMEM((2 * n_y, per_half, plane, n_rows * group_heads * width), f32),
            pltpu.VMEM((nz, 2, wide + sub, cols), f32),
            pltpu.VMEM((4 * per_half, pair_rows // 2, 2 * wide), f32),
            pltpu.VMEM((nz, 4, pair_rows // 2, 2 * wide), f32),
            dma((6,)), dma((chunks,)), dma,
            dma((chunks, labels)), dma((chunks, labels)),
            dma((2 * n_y, n_rows)), dma((2 * n_y, n_rows)),
            dma((2, nz, chunks)), dma((nz, chunks)),
            dma((nz, chunks)), dma((nz, chunks)),
            dma((nz, 2)), dma((2 * n_y, per_half)),
            dma((2, nz)), dma((nz,)), dma((nz,)), dma((nz,)),
            dma((nz, 2)), dma((nz, 2)),
            dma((per_half,)), dma((nz,)),
            dma((4 * n_y - 1,)), dma((4,)), dma((2,)), dma((nz, 2)),
        ],
        compiler_params=pltpu.CompilerParams(collective_id=0, has_side_effects=True),
    )(x, pair, row_mask, residue_mask[None, :], gain[None, :], wq, wk, wv, wg, wo,
      pair_gain[None, :], bias_w.T, tensor_gain[None, :], left_w.T, right_w.T)


def back_kernel(mask_ref, key_ref, left_ref, right_ref, weight_ref, msa_ref, pair_ref,
                msa_out, out_ref, rows_ref, w_ref, rt_ref, r_hi, r_lo, scale_ref, t_hi, t_lo):
    step, cols, depth = pair_ref.shape
    sources, tall, packed = left_ref.shape
    total = rt_ref.shape[0]
    wide = packed // 2
    width = weight_ref.shape[0] // (w_ref.shape[1] // depth)
    n_rows = wide // width
    n_all = sources * n_rows
    at = pl.program_id(0)
    steps = pl.num_programs(0)

    msa_out[...] = msa_ref[...]

    @pl.when(at == 0)
    def _():
        for i in range(2 * tall):
            block = left_ref[:, i % tall, :]
            base = (i // tall) * wide
            rows = jnp.concatenate(
                [block[:, base + s * width:base + (s + 1) * width] for s in range(n_rows)], axis=0
            )
            hi, lo = split(rows)
            rows_ref[i * n_all:(i + 1) * n_all, :] = jnp.concatenate([hi, hi, lo], axis=1)
        for d in range(width):
            hi, lo = split(weight_ref[pl.ds(d, width, stride=width), :])
            w_ref[:, d * depth:(d + 1) * depth] = jnp.concatenate([hi, lo, hi], axis=0)
            for s in range(n_rows):
                spot = (d * n_rows + s) * sources
                rt_ref[spot:spot + sources, :] = right_ref[:, s * width + d, :]
        hi, lo = split(rt_ref[...].T)
        r_hi[...] = hi
        r_lo[...] = lo
        count = jnp.sum(right_ref[:, wide:, :depth], axis=0)
        own = pl.ds(pl.multiple_of(lax.axis_index("head") * cols, cols), cols)
        live = jnp.broadcast_to(key_ref[:, own].astype(jnp.float32), (depth, cols)).T
        scale_ref[...] = live * (1.0 / (count[0:1, :] + 0.001))

    left = rows_ref[pl.ds(pl.multiple_of(at * step * n_all, step * n_all), step * n_all), :]
    group = 2
    for d0 in range(0, width, group):
        t = mm(left, w_ref[:, d0 * depth:(d0 + group) * depth])
        hi, lo = split(t)
        for g in range(group):
            d = d0 + g
            for i in range(step):
                src = (slice(i * n_all, (i + 1) * n_all), slice(g * depth, (g + 1) * depth))
                dst = (slice(d * n_all, (d + 1) * n_all), slice(i * depth, (i + 1) * depth))
                t_hi[dst] = hi[src]
                t_lo[dst] = lo[src]
    update = mm(r_hi[...], t_hi[...]) + mm(r_lo[...], t_hi[...]) + mm(r_hi[...], t_lo[...])
    first = (lax.axis_index("row") * steps + at) * step
    for i in range(step):
        scale = scale_ref[...] * mask_ref[first + i].astype(jnp.float32)
        out_ref[i] = pair_ref[i] + update[:, i * depth:(i + 1) * depth] * scale


def back(residue_mask, left_in, right_all, weight, msa, pair):
    rows, cols, depth = pair.shape
    sources, _, _ = right_all.shape
    tall, packed = left_in.shape[2:]
    left_in = left_in.reshape(sources, tall, packed)
    wide = packed // 2
    n_rows, _, feat = msa.shape
    width = wide // n_rows
    total = sources * wide
    n_all = sources * n_rows
    step = 4
    steps = rows // step
    whole = lambda a: pl.BlockSpec(a.shape, lambda i: (0,) * a.ndim)
    msa_spec = pl.BlockSpec((n_rows, cols // steps, feat), lambda i: (0, i, 0))
    pair_spec = pl.BlockSpec((step, cols, depth), lambda i: (i, 0, 0))
    keys = residue_mask[None, :]
    b16 = jnp.bfloat16
    return pl.pallas_call(
        back_kernel,
        grid=(steps,),
        in_specs=[pl.BlockSpec(memory_space=pltpu.SMEM), whole(keys), whole(left_in), whole(right_all),
                  whole(weight), msa_spec, pair_spec],
        out_specs=(msa_spec, pair_spec),
        out_shape=(jax.ShapeDtypeStruct(msa.shape, jnp.float32), jax.ShapeDtypeStruct(pair.shape, jnp.float32)),
        scratch_shapes=[
            pltpu.VMEM((rows * n_all, 3 * width), b16),
            pltpu.VMEM((3 * width, width * depth), b16),
            pltpu.VMEM((total, cols), jnp.float32),
            pltpu.VMEM((cols, total), b16),
            pltpu.VMEM((cols, total), b16),
            pltpu.VMEM((cols, depth), jnp.float32),
            pltpu.VMEM((total, step * depth), b16),
            pltpu.VMEM((total, step * depth), b16),
        ],
        cost_estimate=pl.CostEstimate(flops=9 * 10**9, bytes_accessed=10**7, transcendentals=0),
    )(residue_mask, keys, left_in, right_all, weight, msa, pair)


def fused_body(
    sequence_matrix, pair_representation, alignment_row_mask, residue_mask, attention_scale_vector,
    asking_factor_matrix, lookup_factor_matrix, content_factor_matrix, sigmoid_factor_matrix,
    final_factor_matrix, pair_norm_gain, bias_weight, tensor_scale_vector, first_factor_matrix,
    second_factor_matrix, outer_weight,
):
    msa, left_in, right_all = front(
        lax.axis_size("row"), lax.axis_size("head"), sequence_matrix, pair_representation,
        alignment_row_mask, residue_mask, attention_scale_vector, asking_factor_matrix,
        lookup_factor_matrix, content_factor_matrix, sigmoid_factor_matrix, final_factor_matrix,
        pair_norm_gain, bias_weight, tensor_scale_vector, first_factor_matrix, second_factor_matrix,
    )
    return back(residue_mask, left_in, right_all, outer_weight, msa, pair_representation)


def fits(n_row, n_y, sequence_matrix, pair_representation, bias_weight, first_factor_matrix):
    rows, residues, feat = sequence_matrix.shape
    heads, opm = bias_weight.shape[1], first_factor_matrix.shape[1]
    n_rows, cols, pair_rows, nz = rows // n_row, residues // n_y, residues // n_row, n_row // 4
    if n_row % 4 or nz & (nz - 1) or nz % n_y or heads % (2 * n_y):
        return False
    group_width = heads // n_y // 2 * (feat // heads)
    return (
        n_rows * group_width == 128 and group_width == 64 and 2 * n_rows * opm == 128
        and cols % 128 == 0 and pair_rows % 16 == 0 and pair_representation.shape[2] == 128
        and n_row % 8 == 0
    )


def solution(mesh):
    placed = (P("row", "head", None), P("row", "head", None), P("row")) + (P(),) * 13
    n_row, n_y = mesh.shape["row"], mesh.shape["head"]

    def step(*args):
        chosen = fused_body if fits(n_row, n_y, args[0], args[1], args[11], args[13]) else body
        return jax.shard_map(
            chosen,
            mesh=mesh,
            in_specs=placed,
            out_specs=(P("row", "head", None), P("row", "head", None)),
            check_vma=False,
        )(*args)

    return step
```

```python
import functools
import math

import jax
import jax.numpy as jnp
from jax import lax
from jax.experimental import pallas as pl
from jax.experimental.pallas import tpu as pltpu
from jax.sharding import PartitionSpec as P


HIGH = lax.Precision.HIGHEST
VMEM_GRANT = 40 * 2**20


def apply_layer_norm(values, gains):
    center = values - jnp.mean(values, axis=-1, keepdims=True)
    spread = jnp.mean(center * center, axis=-1, keepdims=True)
    return center * lax.rsqrt(spread + 1e-05) * gains


def split(x):
    hi = x.astype(jnp.bfloat16)
    lo = (x - hi.astype(jnp.float32)).astype(jnp.bfloat16)
    return hi, lo


def mm(a, b, dims=(((1,), (0,)), ((), ()))):
    return lax.dot_general(a, b, dims, preferred_element_type=jnp.float32)


def split_outside(x):
    hi = lax.reduce_precision(x, 8, 7)
    return hi.astype(jnp.bfloat16), lax.reduce_precision(x - hi, 8, 7).astype(jnp.bfloat16)


NT = (((1,), (1,)), ((), ()))


def bias_kernel(pair_ref, gain_ref, weight_ref, out_ref):
    rows, cols, width = pair_ref.shape
    w_hi, w_lo = split(weight_ref[...])
    heads = w_hi.shape[0]
    w_both = jnp.concatenate([w_hi, w_lo], axis=0)
    for r in range(rows):
        x = apply_layer_norm(pair_ref[r], gain_ref[...])
        x_hi, x_lo = split(x)
        both = mm(w_both, x_hi, NT)
        out_ref[r] = both[:heads] + both[heads:] + mm(w_hi, x_lo, NT)


def pair_bias(pair, gain, weight):
    rows, cols, width = pair.shape
    heads = weight.shape[1]
    step = 4
    return pl.pallas_call(
        bias_kernel,
        grid=(rows // step,),
        in_specs=[
            pl.BlockSpec((step, cols, width), lambda i: (i, 0, 0)),
            pl.BlockSpec((1, width), lambda i: (0, 0)),
            pl.BlockSpec((heads, width), lambda i: (0, 0)),
        ],
        out_specs=pl.BlockSpec((step, heads, cols), lambda i: (i, 0, 0)),
        out_shape=jax.ShapeDtypeStruct((rows, heads, cols), jnp.float32),
        cost_estimate=pl.CostEstimate(flops=10**9, bytes_accessed=5 * 10**6, transcendentals=0),
    )(pair, gain[None, :], weight.T)


def attend_kernel(x_ref, gain_ref, w_ref, bias_ref, key_ref, out_ref, q_ref, k_ref, v_ref):
    blocks, heads, depth, keys = bias_ref.shape
    n_rows = x_ref.shape[0]
    width = v_ref.shape[3] // 2
    local = heads * width
    rows = blocks * depth
    step = pl.program_id(0)

    @pl.when(step == 0)
    def _():
        w_hi, w_lo = split(w_ref[...])
        for s in range(n_rows):
            x_hi, x_lo = split(apply_layer_norm(x_ref[s], gain_ref[...]))
            made = mm(x_hi, w_hi) + mm(x_lo, w_hi) + mm(x_hi, w_lo)
            q_hi, q_lo = split(made[:, :local] * (1.0 / math.sqrt(width)))
            k_hi, k_lo = split(made[:, local:2 * local])
            v_hi, v_lo = split(made[:, 2 * local:])
            for h in range(heads):
                at = slice(h * width, (h + 1) * width)
                q_ref[s, h] = jnp.concatenate([q_hi[:, at], q_hi[:, at], q_lo[:, at]], axis=-1)
                k_ref[s, h] = jnp.concatenate([k_hi[:, at], k_lo[:, at], k_hi[:, at]], axis=-1)
                v_ref[s, h] = jnp.concatenate([v_hi[:, at], v_lo[:, at]], axis=-1)

    key_bias = key_ref[...]
    mine = pl.ds(pl.multiple_of(step * rows, rows), rows)
    for s in range(n_rows):
        pieces = []
        for h in range(heads):
            logits = mm(q_ref[s, h, mine, :], k_ref[s, h], NT)
            logits = logits + bias_ref[:, h].reshape(rows, keys) + key_bias
            largest = jnp.max(logits, axis=-1, keepdims=True)
            e = jnp.exp(logits - largest)
            total = jnp.sum(e, axis=-1, keepdims=True)
            e_hi, e_lo = split(e)
            v = v_ref[s, h]
            both = mm(e_hi, v)
            got = both[:, :width] + both[:, width:] + mm(e_lo, v[:, :width])
            pieces.append(got / total)
        out_ref[s] = jnp.concatenate(pieces, axis=-1)


def attend(x, gain, weight, bias, key_bias):
    n_rows, residues, features = x.shape
    groups, heads, depth, keys = bias.shape
    local = weight.shape[1] // 3
    width = local // heads
    blocks = max(1, 128 // depth)
    rows = blocks * depth
    return pl.pallas_call(
        attend_kernel,
        grid=(groups // blocks,),
        in_specs=[
            pl.BlockSpec(x.shape, lambda i: (0, 0, 0)),
            pl.BlockSpec((1, features), lambda i: (0, 0)),
            pl.BlockSpec(weight.shape, lambda i: (0, 0)),
            pl.BlockSpec((blocks, heads, depth, keys), lambda i: (i, 0, 0, 0)),
            pl.BlockSpec((1, keys), lambda i: (0, 0)),
        ],
        out_specs=pl.BlockSpec((n_rows, rows, local), lambda i: (0, i, 0)),
        out_shape=jax.ShapeDtypeStruct((n_rows, residues, local), jnp.float32),
        scratch_shapes=[
            pltpu.VMEM((n_rows, heads, residues, 3 * width), jnp.bfloat16),
            pltpu.VMEM((n_rows, heads, residues, 3 * width), jnp.bfloat16),
            pltpu.VMEM((n_rows, heads, residues, 2 * width), jnp.bfloat16),
        ],
        cost_estimate=pl.CostEstimate(flops=4 * 10**9, bytes_accessed=6 * 10**6, transcendentals=2 * 10**6),
    )(x, gain[None, :], weight, bias, key_bias)


def outer_kernel(scale_ref, left_ref, weight_ref, right_ref, live_ref, pair_ref, out_ref,
                 r_hi, r_lo, t_hi, t_lo):
    step, cols, depth = pair_ref.shape
    rows_all = r_hi.shape[1]
    n_rows = left_ref.shape[0] // step
    width = rows_all // n_rows
    me = pl.program_id(0)

    @pl.when(me == 0)
    def _():
        hi, lo = split(right_ref[...].T)
        r_hi[...] = hi
        r_lo[...] = lo

    left = left_ref[...]
    group = 2
    for d0 in range(0, width, group):
        t = mm(left, weight_ref[:, d0 * depth:(d0 + group) * depth])
        hi, lo = split(t)
        for g in range(group):
            d = d0 + g
            for i in range(step):
                src = (slice(i * n_rows, (i + 1) * n_rows), slice(g * depth, (g + 1) * depth))
                dst = (slice(d * n_rows, (d + 1) * n_rows), slice(i * depth, (i + 1) * depth))
                t_hi[dst] = hi[src]
                t_lo[dst] = lo[src]
    update = mm(r_hi[...], t_hi[...]) + mm(r_lo[...], t_hi[...]) + mm(r_hi[...], t_lo[...])
    for i in range(step):
        norm = scale_ref[me * step + i] * live_ref[...] + 0.001
        out_ref[i] = pair_ref[i] + update[:, i * depth:(i + 1) * depth] / norm


def outer_mean(scale, left, weight, right, live, pair):
    rows, cols, depth = pair.shape
    total = right.shape[0]
    n_rows = left.shape[0] // rows
    packed = left.shape[1]
    step = 4
    return pl.pallas_call(
        outer_kernel,
        grid=(rows // step,),
        in_specs=[
            pl.BlockSpec(memory_space=pltpu.SMEM),
            pl.BlockSpec((step * n_rows, packed), lambda i: (i, 0)),
            pl.BlockSpec(weight.shape, lambda i: (0, 0)),
            pl.BlockSpec(right.shape, lambda i: (0, 0)),
            pl.BlockSpec((cols, 1), lambda i: (0, 0)),
            pl.BlockSpec((step, cols, depth), lambda i: (i, 0, 0)),
        ],
        out_specs=pl.BlockSpec((step, cols, depth), lambda i: (i, 0, 0)),
        out_shape=jax.ShapeDtypeStruct(pair.shape, jnp.float32),
        scratch_shapes=[
            pltpu.VMEM((cols, total), jnp.bfloat16),
            pltpu.VMEM((cols, total), jnp.bfloat16),
            pltpu.VMEM((total, step * depth), jnp.bfloat16),
            pltpu.VMEM((total, step * depth), jnp.bfloat16),
        ],
        cost_estimate=pl.CostEstimate(flops=9 * 10**9, bytes_accessed=10**7, transcendentals=0),
    )(scale, left, weight, right, live, pair)


def gather_kernel(n, block_ref, out_ref, own_sem, send_sem, recv_sem):
    me = lax.axis_index("row")
    core = me % 2
    x = (me // 2) % 2
    nz = n // 4
    z = me // 4

    def place(zz, xx, cc):
        return (zz * 2 + xx) * 2 + cc

    barrier = pltpu.get_barrier_semaphore()
    up_ok, down_ok = z + 1 < nz, z >= 1

    def greet(target):
        pl.semaphore_signal(barrier, inc=1, device_id={"row": target},
                            device_id_type=pl.DeviceIdType.MESH)

    greet(place(z, x, 1 - core))
    greet(place(z, 1 - x, core))
    pl.when(up_ok)(lambda: greet(place(z + 1, x, core)))
    pl.when(down_ok)(lambda: greet(place(z - 1, x, core)))
    peers = 2 + jnp.where(up_ok, 1, 0) + jnp.where(down_ok, 1, 0)
    pl.semaphore_wait(barrier, peers)

    own = pltpu.make_async_copy(block_ref, out_ref.at[me], own_sem)
    own.start()

    def sends(d, other):
        found = []
        first = core == 0
        if other == 0:
            cross = (z >= 0) if d == 0 else jnp.logical_not(first)
            run = z >= 0
        else:
            cross = None
            run = first
        if d <= 0:
            found.append((jnp.logical_and(run, up_ok), 0, lambda: place(z + 1, x, core)))
        if d >= 0:
            found.append((jnp.logical_and(run, down_ok), 1, lambda: place(z - 1, x, core)))
        if cross is not None:
            found.append((cross, 2, lambda: place(z, 1 - x, core)))
        found.append((z >= 0, 3, lambda: place(z, x, 1 - core)))
        return found

    def copy(source, kind, target, mine):
        return pltpu.make_async_remote_copy(
            src_ref=block_ref if mine else out_ref.at[source],
            dst_ref=out_ref.at[source],
            send_sem=send_sem.at[kind, source],
            recv_sem=recv_sem.at[source],
            device_id={"row": target},
            device_id_type=pl.DeviceIdType.MESH,
        )

    hops = [(0, 0), (0, 1)]
    for far in range(1, nz):
        hops += [(-far, 0), (far, 0), (-far, 1), (far, 1)]

    def each(action):
        for d, other in hops:
            source = place(z + d, (x + other) % 2, core)
            mine = d == 0 and other == 0
            there = jnp.logical_and(z + d >= 0, z + d < nz)

            @pl.when(there)
            def _(d=d, other=other, source=source, mine=mine):
                action(d, other, source, mine)

    def forward(d, other, source, mine):
        if not mine:
            copy(source, 3, place(z, x, 1 - core), False).wait_recv()
        for ok, kind, target in sends(d, other):
            pl.when(ok)(lambda kind=kind, target=target: copy(source, kind, target(), mine).start())

    def finish(d, other, source, mine):
        for ok, kind, target in sends(d, other):
            pl.when(ok)(lambda kind=kind, target=target: copy(source, kind, target(), mine).wait_send())

    each(forward)
    for k in range(n // 2):
        copy(2 * k + 1 - core, 3, place(z, x, 1 - core), False).wait_recv()
    each(finish)
    own.wait()


def gather_rows(block, n, ident):
    return pl.pallas_call(
        functools.partial(gather_kernel, n),
        out_shape=jax.ShapeDtypeStruct((n,) + block.shape, block.dtype),
        in_specs=[pl.BlockSpec(memory_space=pltpu.VMEM)],
        out_specs=pl.BlockSpec(memory_space=pl.ANY),
        scratch_shapes=[
            pltpu.SemaphoreType.DMA,
            pltpu.SemaphoreType.DMA((4, n)),
            pltpu.SemaphoreType.DMA((n,)),
        ],
        compiler_params=pltpu.CompilerParams(collective_id=ident, has_side_effects=True),
    )(block)


def around(n):
    return [[(src, (src + k) % n) for src in range(n)] for k in range(n)]


def gather_heads(block, n, index, axis):
    size = block.shape[axis]
    shape = list(block.shape)
    shape[axis] = size * n
    whole = jnp.zeros(shape, block.dtype)
    for k in range(n):
        part = block if k == 0 else lax.ppermute(block, "head", around(n)[k])
        whole = lax.dynamic_update_slice_in_dim(whole, part, ((index - k) % n) * size, axis)
    return whole


def exchange_heads(block, n, index, split_axis, concat_axis):
    size = block.shape[split_axis] // n
    shape = list(block.shape)
    shape[split_axis] = size
    length = shape[concat_axis]
    shape[concat_axis] = length * n
    whole = jnp.zeros(shape, block.dtype)
    for k in range(n):
        part = lax.dynamic_slice_in_dim(block, ((index + k) % n) * size, size, split_axis)
        if k:
            part = lax.ppermute(part, "head", around(n)[k])
        whole = lax.dynamic_update_slice_in_dim(whole, part, ((index - k) % n) * length, concat_axis)
    return whole


def body(
    sequence_matrix,
    pair_representation,
    alignment_row_mask,
    residue_mask,
    attention_scale_vector,
    asking_factor_matrix,
    lookup_factor_matrix,
    content_factor_matrix,
    sigmoid_factor_matrix,
    final_factor_matrix,
    pair_norm_gain,
    bias_weight,
    tensor_scale_vector,
    first_factor_matrix,
    second_factor_matrix,
    outer_weight,
):
    head_count = lax.axis_size("head")
    head_index = lax.axis_index("head")
    row_index = lax.axis_index("row")
    row_count = lax.axis_size("row")
    n_rows, col_count, width = sequence_matrix.shape
    residues = col_count * head_count
    pair_rows = pair_representation.shape[0]
    pair_depth = pair_representation.shape[2]
    heads_all = bias_weight.shape[1]
    head_width = width // heads_all
    local_heads = heads_all // head_count
    local_width = local_heads * head_width
    opm_width = first_factor_matrix.shape[1]

    sequence_all = gather_heads(sequence_matrix, head_count, head_index, 1)

    bias_all = pair_bias(pair_representation, pair_norm_gain, bias_weight)
    bias_part = exchange_heads(
        bias_all.transpose(1, 0, 2), head_count, head_index, 0, 2
    )
    bias = gather_rows(bias_part, row_count, 0)
    key_bias = ((residue_mask.astype(jnp.float32) - 1.0) * 1000000000.0)[None, :]

    weights = jnp.concatenate(
        [
            lax.dynamic_slice_in_dim(w, head_index * local_width, local_width, 1)
            for w in (asking_factor_matrix, lookup_factor_matrix, content_factor_matrix)
        ],
        axis=1,
    )
    attended = attend(sequence_all, attention_scale_vector, weights, bias, key_bias)
    norm_mine = apply_layer_norm(sequence_matrix, attention_scale_vector)
    gate = jax.nn.sigmoid(
        jnp.einsum("sic,ce->sie", norm_mine, sigmoid_factor_matrix, precision=HIGH)
    )
    returned_values = exchange_heads(attended, head_count, head_index, 1, 2) * gate
    alignment_updated = sequence_matrix + jnp.einsum(
        "jna,ab->jnb", returned_values, final_factor_matrix, precision=HIGH
    )

    outer_product_norm = apply_layer_norm(alignment_updated, tensor_scale_vector)
    live_cols = lax.dynamic_slice_in_dim(residue_mask, head_index * col_count, col_count).astype(
        jnp.float32
    )
    row_live = alignment_row_mask.astype(jnp.float32)
    live = row_live[:, None] * live_cols[None, :]
    left_side = (
        jnp.einsum("sic,co->soi", outer_product_norm, first_factor_matrix, precision=HIGH)
        * live[:, None, :]
    )
    right = (
        jnp.einsum("sic,co->soi", outer_product_norm, second_factor_matrix, precision=HIGH)
        * live[:, None, :]
    )
    left_all = gather_heads(left_side, head_count, head_index, 1)
    carried = jnp.broadcast_to(row_live[:, None, None], (n_rows, 8, col_count))
    sides = gather_rows(jnp.concatenate([left_all, right, carried], axis=1), row_count, 1)
    sides = sides.reshape(row_count * n_rows, -1, col_count)
    left_width = head_count * opm_width
    first_row = row_index * pair_rows
    left_mine = lax.dynamic_slice(
        sides,
        (0, (first_row // col_count) * opm_width, first_row % col_count),
        (row_count * n_rows, opm_width, pair_rows),
    )
    right_all = sides[:, left_width:]
    total_rows = row_count * n_rows
    count = jnp.sum(right_all[:, opm_width, 0])
    right_rows = right_all[:, :opm_width].transpose(1, 0, 2).reshape(
        opm_width * total_rows, col_count
    )
    left_rows = left_mine.transpose(2, 0, 1).reshape(pair_rows * total_rows, opm_width)
    l_hi, l_lo = split_outside(left_rows)
    w_hi, w_lo = split_outside(outer_weight.reshape(opm_width, opm_width * pair_depth))
    rows_live = lax.dynamic_slice_in_dim(residue_mask, row_index * pair_rows, pair_rows).astype(
        jnp.float32
    )
    pair_out = outer_mean(
        count * rows_live,
        jnp.concatenate([l_hi, l_hi, l_lo], axis=1),
        jnp.concatenate([w_hi, w_lo, w_hi], axis=0),
        right_rows,
        live_cols[:, None],
        pair_representation,
    )
    return alignment_updated, pair_out


def ln(values, gains):
    return apply_layer_norm(values, gains)


def front_kernel(
    x_hbm, pair_hbm, row_mask, key_ref, gain_ref, wq_hbm, wk_hbm, wv_hbm, wg_hbm, wo_hbm,
    pair_gain, bias_w, tensor_gain, left_w, right_w, weight_hbm, mask_ref,
    msa_ref, acc_ref,
    x_ref, pair_ref, wq_ref, wk_ref, wv_ref, wg_ref, wo_ref, wpair_ref, group_ref,
    bias_ref, xn_ref, q_ref, k_ref, v_ref, gate_ref, att_out, att_in, right_buf, left_loc, left_own,
    left_in, weight_ref, w_ref, rows_ref, rt_ref, r_hi, r_lo, t_hi, t_lo, live_ref,
    load_sem, pair_sem, s1_send, s1_recv, n_send, n_recv, z_send, z_recv, x_send, x_recv,
    a_send, a_recv, rz_send, rz_recv, rx_send, rx_recv, rc_send, rc_recv,
    l1_send, l1_recv, l2_send, l2_recv,
):
    nz, _, chunks, _, n_y, group_heads, sub, cols = bias_ref.shape
    n_rows, _, feat = x_ref.shape
    heads = bias_w.shape[0]
    keys = n_y * cols
    width = v_ref.shape[3] // 2
    group_width = group_heads * width
    local_width = 2 * group_width
    per_half = nz // n_y
    plane = cols // per_half
    pair_width = pair_ref.shape[2]
    opm = left_w.shape[0]

    me, y = lax.axis_index("row"), lax.axis_index("head")
    c, x, z = me % 2, (me // 2) % 2, me // 4
    half = z // per_half

    def place(zz, xx, cc):
        return (zz * 2 + xx) * 2 + cc

    def across(d):
        out, bit = z, 1
        while bit <= d:
            if d & bit:
                out = out + bit * (1 - 2 * ((out // bit) % 2))
            bit *= 2
        return out

    def plane_at(p):
        if p < 2:
            return across(p)
        return jnp.where(z < nz // 2, p, nz - 1 - p)

    def remote(src, dst, send, recv, row, head):
        return pltpu.make_async_remote_copy(
            src_ref=src, dst_ref=dst, send_sem=send, recv_sem=recv,
            device_id={"row": row, "head": head}, device_id_type=pl.DeviceIdType.MESH,
        )

    def arrived(dst, send, recv):
        remote(dst, dst, send, recv, place(z, x, 1 - c), y).wait_recv()

    pending = []

    def go(copy):
        copy.start()
        pending.append(copy)

    loads = {}
    for at, (src, dst) in enumerate(
        [(x_hbm, x_ref), (wq_hbm, wq_ref), (wk_hbm, wk_ref), (wv_hbm, wv_ref), (wg_hbm, wg_ref), (wo_hbm, wo_ref),
         (weight_hbm, weight_ref)]
    ):
        loads[at] = pltpu.make_async_copy(src, dst, load_sem.at[at])
    pair_loads = [
        pltpu.make_async_copy(
            pair_hbm.at[pl.ds(k * sub, sub)], pair_ref.at[pl.ds(k * sub, sub)], pair_sem.at[k]
        )
        for k in range(chunks)
    ]
    loads[0].start()
    for copy in pair_loads:
        copy.start()
    for at in range(1, 7):
        loads[at].start()

    barrier = pltpu.get_barrier_semaphore()
    peers = []
    for dx in range(2):
        for dc in range(2):
            for dy in range(n_y):
                if dx or dc or dy:
                    peers.append((place(z, (x + dx) % 2, (c + dc) % 2), (y + dy) % n_y))
    for d in range(1, nz):
        peers.append((place(across(d), x, c), y))
    for row, head in peers:
        pl.semaphore_signal(barrier, inc=1, device_id={"row": row, "head": head},
                            device_id_type=pl.DeviceIdType.MESH)

    w_hi, w_lo = split(bias_w[...])
    spread = sub * heads
    at_row = lax.broadcasted_iota(jnp.int32, (heads, sub, pair_width), 1).reshape(spread, pair_width)
    zero = jnp.zeros((spread, pair_width), jnp.float32)

    def rows_of(part):
        part = part.astype(jnp.float32)
        return jnp.broadcast_to(part[:, None, :], (heads, sub, pair_width)).reshape(spread, pair_width)

    rep_hi, rep_lo = rows_of(w_hi), rows_of(w_lo)
    for t in range(sub // 2):
        first, second = at_row == 2 * t, at_row == 2 * t + 1
        both = [
            jnp.concatenate([jnp.where(first, rep, zero), jnp.where(second, rep, zero)], axis=1)
            for rep in (rep_hi, rep_lo)
        ]
        wpair_ref[t] = jnp.concatenate(both, axis=0).astype(jnp.bfloat16)

    def bias_chunk(k):
        pair_loads[k].wait()
        total = None
        for t in range(sub // 2):
            at = k * sub + 2 * t
            pieces = [split(ln(pair_ref[at + e], pair_gain[...])) for e in range(2)]
            hi = jnp.concatenate([pieces[0][0], pieces[1][0]], axis=1)
            lo = jnp.concatenate([pieces[0][1], pieces[1][1]], axis=1)
            both = mm(wpair_ref[t], hi, NT)
            part = both[:spread] + both[spread:] + mm(wpair_ref[t, :spread], lo, NT)
            total = part if total is None else total + part
        group_ref[k] = total.reshape(2 * n_y, group_heads, sub, cols)
        bias_ref[z, x, k, c, y] = group_ref[k, y * 2 + c]

    labels = [(dy, dc) for dy in range(n_y) for dc in range(2) if dy or dc]

    def stage_one(k):
        for at, (dy, dc) in enumerate(labels):
            ty, tc = (y + dy) % n_y, (c + dc) % 2
            go(remote(group_ref.at[k, ty * 2 + tc], bias_ref.at[z, x, k, c, y],
                      s1_send.at[k, at], s1_recv.at[k, at], place(z, x, tc), ty))

    def stage_two(k):
        for at, (dy, dc) in enumerate(labels):
            sy, sc = (y + n_y - dy) % n_y, (c + dc) % 2
            arrived(bias_ref.at[z, x, k, sc, sy], s1_send.at[k, at], s1_recv.at[k, at])
        own = bias_ref.at[z, x, k]
        go(remote(own, own, x_send.at[z, k], x_recv.at[z, k], place(z, 1 - x, c), y))
        for up in range(2):
            relay(up, z, k)

    def relay_copy(up, zz, k):
        block = bias_ref.at[zz, x, k]
        return remote(block, block, z_send.at[up, zz, k], z_recv.at[zz, k],
                      place(z + 1 if up else z - 1, x, c), y)

    def can_relay(up):
        return z + 1 < nz if up else z >= 1

    def relay(up, zz, k):
        pl.when(can_relay(up))(lambda: relay_copy(up, zz, k).start())

    def source(up, j):
        return (z - j, z >= j) if up else (z + j, z + j < nz)

    def pass_on(j, k):
        for up in range(2):
            zz, there = source(up, j)

            @pl.when(there)
            def _(up=up, zz=zz):
                block = bias_ref.at[zz, x, k]
                arrived(block, z_send.at[0, 0, k], z_recv.at[zz, k])
                if j + 1 < nz:
                    relay(up, zz, k)
                remote(block, block, x_send.at[zz, k], x_recv.at[zz, k], place(z, 1 - x, c), y).start()

    bias_chunk(0)
    pl.semaphore_wait(barrier, len(peers))
    stage_one(0)
    for k in range(1, chunks):
        bias_chunk(k)
        stage_one(k)
        if k >= 2:
            stage_two(k - 2)

    loads[0].wait()
    for s in range(n_rows):
        xn_ref[y, c, s] = ln(x_ref[s], gain_ref[...])
        own_x = xn_ref.at[y, c, s]
        for dy in range(1, n_y):
            go(remote(own_x, own_x, n_send.at[dy, s], n_recv.at[dy, s], place(z, x, c), (y + dy) % n_y))
        go(remote(own_x, own_x, n_send.at[0, s], n_recv.at[0, s], place(z, x, 1 - c), y))
    stage_two(chunks - 2)

    for at in (1, 2, 3):
        loads[at].wait()
    mine = pl.ds(pl.multiple_of(y * local_width, local_width), local_width)
    picked = []
    for ref in (wq_ref, wk_ref, wv_ref):
        whole = ref[:, mine]
        picked.append(jnp.where(c == 0, whole[:, :group_width], whole[:, group_width:]))
    wa_hi, wa_lo = split(jnp.concatenate(picked, axis=1))

    def project(yy, cc, rows=range(n_rows)):
        spot = pl.ds(pl.multiple_of(yy * cols, cols), cols)
        for s in rows:
            hi, lo = split(xn_ref[yy, cc, s])
            made = mm(hi, wa_hi) + mm(lo, wa_hi) + mm(hi, wa_lo)
            q_hi, q_lo = split(made[:, :group_width] * (1.0 / math.sqrt(width)))
            k_hi, k_lo = split(made[:, group_width:2 * group_width])
            v_hi, v_lo = split(made[:, 2 * group_width:])
            for h in range(group_heads):
                at = slice(h * width, (h + 1) * width)
                to = cc * n_rows + s
                q_ref[to, h, spot, :] = jnp.concatenate([q_hi[:, at], q_hi[:, at], q_lo[:, at]], axis=-1)
                k_ref[to, h, spot, :] = jnp.concatenate([k_hi[:, at], k_lo[:, at], k_hi[:, at]], axis=-1)
                v_ref[to, h, spot, :] = jnp.concatenate([v_hi[:, at], v_lo[:, at]], axis=-1)

    project(y, c)
    stage_two(chunks - 1)
    loads[4].wait()
    g_hi, g_lo = split(wg_ref[...])
    for s in range(n_rows):
        hi, lo = split(xn_ref[y, c, s])
        gate_ref[s] = jax.nn.sigmoid(mm(hi, g_hi) + mm(lo, g_hi) + mm(hi, g_lo))
    for s in range(n_rows):
        arrived(xn_ref.at[y, 1 - c, s], n_send.at[0, s], n_recv.at[0, s])
    project(y, 1 - c)

    acc_ref[...] = jnp.zeros_like(acc_ref)
    loads[6].wait()
    for d in range(opm):
        hi, lo = split(weight_ref[pl.ds(d, opm, stride=opm), :])
        w_ref[:, d * pair_width:(d + 1) * pair_width] = jnp.concatenate([hi, lo, hi], axis=0)
    own = pl.ds(pl.multiple_of(y * cols, cols), cols)
    live_ref[...] = jnp.broadcast_to(key_ref[:, own].astype(jnp.float32), (pair_width, cols)).T

    tasks = [(j, k) for j in range(1, nz) for k in range(chunks)]
    early = tasks[:chunks]
    late = tasks[chunks:2 * chunks]
    rest = tasks[2 * chunks:]
    for j, k in early:
        pass_on(j, k)
    for dy in range(1, n_y):
        sy = (y + n_y - dy) % n_y
        for s in range(n_rows):
            block = xn_ref.at[sy, c, s]
            arrived(block, n_send.at[dy, s], n_recv.at[dy, s])
            go(remote(block, block, n_send.at[n_y + dy, s], n_recv.at[n_y + dy, s], place(z, x, 1 - c), y))
            project(sy, c, [s])
            share = len(late) // (n_rows * (n_y - 1))
            for j, k in late[:share] if s + 1 < n_rows or dy + 1 < n_y else late:
                pass_on(j, k)
            late = late[share:]
    for dy in range(1, n_y):
        sy = (y + n_y - dy) % n_y
        for s in range(n_rows):
            arrived(xn_ref.at[sy, 1 - c, s], n_send.at[n_y + dy, s], n_recv.at[n_y + dy, s])
        project(sy, 1 - c)

    key_bias = (key_ref[...].astype(jnp.float32) - 1.0) * 1000000000.0

    def attended_copy(d, ct):
        zz = plane_at(d)
        return remote(att_out.at[d, ct], att_in.at[y * 2 + c, zz % per_half],
                      a_send.at[d, ct], a_recv.at[y * 2 + c, zz % per_half],
                      place(z, x, ct), zz // per_half)

    def is_mine(d, ct):
        return jnp.logical_and(plane_at(d) // per_half == y, ct == c)

    def attend_plane(d):
        zz = plane_at(d)
        for k in range(chunks):
            arrived(bias_ref.at[zz, 1 - x, k], x_send.at[0, k], x_recv.at[zz, k])
        queries = pl.ds(pl.multiple_of(zz * plane, plane), plane)

        def unit(ct, carry):
            pieces = []
            for s in range(n_rows):
                row = ct * n_rows + s
                for h in range(group_heads):
                    logits = mm(q_ref[row, h, queries, :], k_ref[row, h], NT)
                    tiles = [
                        jnp.concatenate(
                            [bias_ref[zz, xx, :, cc, yy, h].reshape(chunks * sub, cols) for yy in range(n_y)],
                            axis=1,
                        )
                        for xx in range(2)
                        for cc in range(2)
                    ]
                    logits = logits + jnp.concatenate(tiles, axis=0) + key_bias
                    largest = jnp.max(logits, axis=-1, keepdims=True)
                    e = jnp.exp(logits - largest)
                    total = jnp.sum(e, axis=-1, keepdims=True)
                    e_hi, e_lo = split(e)
                    v = v_ref[row, h]
                    both = mm(e_hi, v)
                    got = both[:, :width] + both[:, width:] + mm(e_lo, v[:, :width])
                    pieces.append(got / total)
            value = jnp.concatenate(pieces, axis=-1)
            att_out[d, ct] = value

            @pl.when(is_mine(d, ct))
            def _():
                att_in[y * 2 + c, zz % per_half] = value

            @pl.when(jnp.logical_not(is_mine(d, ct)))
            def _():
                attended_copy(d, ct).start()

            return carry

        lax.fori_loop(0, 2, unit, 0)

    for d in range(nz):
        attend_plane(d)
        share = -(-len(rest) // 2) if d == 0 else len(rest)
        for j, k in rest[:share]:
            pass_on(j, k)
        rest = rest[share:]

    for dy, dc in labels:
        sy, sc = (y + n_y - dy) % n_y, (c + dc) % 2
        for p in range(per_half):
            arrived(att_in.at[sy * 2 + sc, p], a_send.at[0, 0], a_recv.at[sy * 2 + sc, p])

    loads[5].wait()
    o_hi, o_lo = split(wo_ref[...])
    wide = n_rows * opm
    left_hi, left_lo = split(left_w[...])
    left_both = jnp.concatenate([left_hi, left_lo], axis=0)
    right_hi, right_lo = split(right_w[...])
    right_both = jnp.concatenate([right_hi, right_lo], axis=0)
    lefts = []
    count = jnp.zeros((sub, cols), jnp.float32)
    for s in range(n_rows):
        at = slice(s * group_width, (s + 1) * group_width)
        whole = jnp.concatenate(
            [
                jnp.concatenate([att_in[g, p][:, at] for p in range(per_half)], axis=0)
                for g in range(2 * n_y)
            ],
            axis=1,
        ) * gate_ref[s]
        hi, lo = split(whole)
        out = x_ref[s] + (mm(hi, o_hi) + mm(lo, o_hi) + mm(hi, o_lo))
        msa_ref[s] = out
        f_hi, f_lo = split(ln(out, tensor_gain[...]))
        live = row_mask[s].astype(jnp.float32)
        both = mm(right_both, f_hi, NT)
        right_buf[z, x * 2 + c, s * opm:(s + 1) * opm, :] = (both[:opm] + both[opm:] + mm(right_hi, f_lo, NT)) * live
        both = mm(f_hi, left_both, NT)
        lefts.append((both[:, :opm] + both[:, opm:] + mm(f_lo, left_hi, NT)) * live)
        count = count + live
    right_buf[z, x * 2 + c, wide:, :] = count

    left = jnp.concatenate(lefts, axis=1)
    blocks = per_half * 4
    tall = left.shape[0] // blocks // 2
    left = left.reshape(blocks, 2, tall, wide)
    left_loc[...] = jnp.concatenate([left[:, 0], left[:, 1]], axis=2)

    def left_copy(p):
        return remote(left_loc.at[pl.ds(p * 4, 4)], left_own.at[z], l1_send.at[p], l1_recv.at[z],
                      place(y * per_half + p, x, c), y)

    for p in range(per_half):
        here = y * per_half + p == z

        @pl.when(here)
        def _(p=p):
            left_own[z] = left_loc[p * 4:(p + 1) * 4]

        pl.when(jnp.logical_not(here))(lambda p=p: left_copy(p).start())

    def right_core(zz, far):
        block = right_buf.at[zz, (x if far == 0 else 1 - x) * 2 + c]
        return remote(block, block, rc_send.at[zz, far], rc_recv.at[zz, far], place(z, x, 1 - c), y)

    def right_relay(up, zz):
        block = right_buf.at[zz, x * 2 + c]
        return remote(block, block, rz_send.at[up, zz], rz_recv.at[zz], place(z + 1 if up else z - 1, x, c), y)

    def right_cross(zz):
        block = right_buf.at[zz, x * 2 + c]
        return remote(block, block, rx_send.at[zz], rx_recv.at[zz], place(z, 1 - x, c), y)

    for up in range(2):
        pl.when(can_relay(up))(lambda up=up: right_relay(up, z).start())
    right_cross(z).start()
    right_core(z, 0).start()

    owner = half == y
    finals = [(dx, dc, dy) for dx in range(2) for dc in range(2) for dy in range(n_y) if dx or dc or dy]

    def final_copy(at, zz):
        dx, dc, dy = finals[at]
        tx, tc, ty = (x + dx) % 2, (c + dc) % 2, (y + dy) % n_y
        return remote(left_own.at[zz, tx * 2 + tc], left_in.at[zz, x * 2 + c], l2_send.at[zz, at],
                      l2_recv.at[zz, x * 2 + c], place(z, tx, tc), ty)

    def left_pass(zz):
        @pl.when(owner)
        def _():
            pl.when(zz != z)(lambda: arrived(left_own.at[zz], l1_send.at[0], l1_recv.at[zz]))
            for at in range(len(finals)):
                final_copy(at, zz).start()
            left_in[zz, x * 2 + c] = left_own[zz, x * 2 + c]

    def left_wait(zz):
        for xx in range(2):
            for cc in range(2):
                mine_too = jnp.logical_and(owner, jnp.logical_and(xx == x, cc == c))

                @pl.when(jnp.logical_not(mine_too))
                def _(xx=xx, cc=cc):
                    arrived(left_in.at[zz, xx * 2 + cc], l2_send.at[0, 0], l2_recv.at[zz, xx * 2 + cc])

    def right_pass(j):
        for up in range(2):
            zz, there = source(up, j)

            @pl.when(there)
            def _(up=up, zz=zz):
                arrived(right_buf.at[zz, x * 2 + c], rz_send.at[0, 0], rz_recv.at[zz])
                pl.when(jnp.logical_and(can_relay(up), j + 1 < nz))(lambda: right_relay(up, zz).start())
                right_cross(zz).start()
                right_core(zz, 0).start()

    def right_far(zz):
        arrived(right_buf.at[zz, (1 - x) * 2 + c], rx_send.at[0], rx_recv.at[zz])
        right_core(zz, 1).start()

    def ordered(p):
        late = jnp.where(z < nz // 2, p, nz - 1 - p)
        return jnp.where(p == 0, z, jnp.where(p == 1, across(1), late))

    left_pass(z)
    tall = pair_ref.shape[0] // 2
    slots = 4 * n_rows

    def outer_plane(p, carry):
        zz = ordered(p)
        pl.when(p + 1 < nz)(lambda: right_pass(p + 1))
        right_far(zz)
        left_wait(zz)
        for i in range(2 * tall):
            block = left_in[zz, :, i % tall, :]
            base = (i // tall) * wide
            rows_ref[i * slots:(i + 1) * slots, :] = jnp.concatenate(
                [block[:, base + s * opm:base + (s + 1) * opm] for s in range(n_rows)], axis=0
            )
        hi, lo = split(rows_ref[...])
        rows = jnp.concatenate([hi, hi, lo], axis=1)
        for d in range(0, opm, 2):
            t = mm(rows, w_ref[:, d * pair_width:(d + 2) * pair_width])
            for i in range(2 * tall):
                piece = t[i * slots:(i + 1) * slots]
                hi, lo = split(jnp.concatenate([piece[:, :pair_width], piece[:, pair_width:]], axis=0))
                spot = (slice(d * slots, (d + 2) * slots), slice(i * pair_width, (i + 1) * pair_width))
                t_hi[spot] = hi
                t_lo[spot] = lo
        pl.when(p + 1 < nz)(lambda: left_pass(ordered(p + 1)))
        for far in range(2):
            block = right_buf.at[zz, (x if far == 0 else 1 - x) * 2 + 1 - c]
            arrived(block, rc_send.at[0, 0], rc_recv.at[zz, far])
        for d in range(opm):
            for s in range(n_rows):
                spot = (d * n_rows + s) * 4
                rt_ref[spot:spot + 4, :] = right_buf[zz, :, s * opm + d, :]
        hi, lo = split(rt_ref[...].T)
        r_hi[...] = hi
        r_lo[...] = lo
        group = 4
        for i in range(0, 2 * tall, group):
            at = slice(i * pair_width, (i + group) * pair_width)
            update = mm(r_hi[...], t_hi[:, at]) + mm(r_lo[...], t_hi[:, at]) + mm(r_hi[...], t_lo[:, at])
            for e in range(group):
                acc_ref[i + e] += update[:, e * pair_width:(e + 1) * pair_width]
        return carry

    lax.fori_loop(0, nz, outer_plane, 0)

    total = jnp.zeros((sub, pair_width), jnp.float32)
    for zz in range(nz):
        for at in range(4):
            total = total + right_buf[zz, at, wide:, :pair_width]
    live_ref[...] = live_ref[...] * (1.0 / (total[0:1, :] + 0.001))
    group = 4
    for i in range(0, 2 * tall, group):
        for e in range(group):
            live = mask_ref[me * 2 * tall + i + e].astype(jnp.float32)
            acc_ref[i + e] = pair_ref[i + e] + acc_ref[i + e] * (live_ref[...] * live)

    for copy in pending:
        copy.wait_send()
    for zz in range(nz):
        for k in range(chunks):
            block = bias_ref.at[zz, x, k]

            @pl.when(zz != z)
            def _(zz=zz, k=k, block=block):
                remote(block, block, x_send.at[zz, k], x_recv.at[zz, k], place(z, 1 - x, c), y).wait_send()

            for up in range(2):
                goes = jnp.logical_and(can_relay(up), zz <= z if up else zz >= z)
                pl.when(goes)(lambda up=up, zz=zz, k=k: relay_copy(up, zz, k).wait_send())
        for up in range(2):
            goes = jnp.logical_and(can_relay(up), zz <= z if up else zz >= z)
            pl.when(goes)(lambda up=up, zz=zz: right_relay(up, zz).wait_send())
        right_cross(zz).wait_send()
        for far in range(2):
            right_core(zz, far).wait_send()
    for d in range(nz):
        for ct in range(2):
            pl.when(jnp.logical_not(is_mine(d, ct)))(lambda d=d, ct=ct: attended_copy(d, ct).wait_send())
    for p in range(per_half):
        pl.when(y * per_half + p != z)(lambda p=p: left_copy(p).wait_send())

    @pl.when(owner)
    def _():
        for zz in range(nz):
            for at in range(len(finals)):
                final_copy(at, zz).wait_send()


def front(n_row, n_y, x, pair, row_mask, residue_mask, gain, wq, wk, wv, wg, wo,
          pair_gain, bias_w, tensor_gain, left_w, right_w, weight):
    n_rows, cols, feat = x.shape
    pair_rows, _, pair_width = pair.shape
    heads = bias_w.shape[1]
    width = feat // heads
    group_heads = heads // n_y // 2
    nz, sub = n_row // 4, 8
    chunks = pair_rows // sub
    keys = n_y * cols
    per_half = nz // n_y
    plane = cols // per_half
    opm = left_w.shape[1]
    wide = n_rows * opm
    f32, b16 = jnp.float32, jnp.bfloat16
    hbm, vmem = pl.BlockSpec(memory_space=pltpu.HBM), pl.BlockSpec(memory_space=pltpu.VMEM)
    dma = pltpu.SemaphoreType.DMA
    labels = 2 * n_y - 1
    return pl.pallas_call(
        front_kernel,
        out_shape=(
            jax.ShapeDtypeStruct(x.shape, f32),
            jax.ShapeDtypeStruct(pair.shape, f32),
        ),
        in_specs=[hbm, hbm, pl.BlockSpec(memory_space=pltpu.SMEM), vmem, vmem]
        + [hbm] * 5 + [vmem] * 5 + [hbm, pl.BlockSpec(memory_space=pltpu.SMEM)],
        out_specs=(vmem, vmem),
        scratch_shapes=[
            pltpu.VMEM(x.shape, f32),
            pltpu.VMEM(pair.shape, f32),
        ]
        + [pltpu.VMEM((feat, feat), f32)] * 5
        + [
            pltpu.VMEM((sub // 2, 2 * sub * heads, 2 * pair_width), b16),
            pltpu.VMEM((chunks, 2 * n_y, group_heads, sub, cols), f32),
            pltpu.VMEM((nz, 2, chunks, 2, n_y, group_heads, sub, cols), f32),
            pltpu.VMEM((n_y, 2, n_rows, cols, feat), f32),
            pltpu.VMEM((2 * n_rows, group_heads, keys, 3 * width), b16),
            pltpu.VMEM((2 * n_rows, group_heads, keys, 3 * width), b16),
            pltpu.VMEM((2 * n_rows, group_heads, keys, 2 * width), b16),
            pltpu.VMEM(x.shape, f32),
            pltpu.VMEM((nz, 2, plane, n_rows * group_heads * width), f32),
            pltpu.VMEM((2 * n_y, per_half, plane, n_rows * group_heads * width), f32),
            pltpu.VMEM((nz, 4, wide + sub, cols), f32),
            pltpu.VMEM((4 * per_half, pair_rows // 2, 2 * wide), f32),
            pltpu.VMEM((nz, 4, pair_rows // 2, 2 * wide), f32),
            pltpu.VMEM((nz, 4, pair_rows // 2, 2 * wide), f32),
            pltpu.VMEM(weight.shape, f32),
            pltpu.VMEM((3 * opm, opm * pair_width), b16),
            pltpu.VMEM((pair_rows * 4 * n_rows, opm), f32),
            pltpu.VMEM((opm * 4 * n_rows, cols), f32),
            pltpu.VMEM((cols, opm * 4 * n_rows), b16),
            pltpu.VMEM((cols, opm * 4 * n_rows), b16),
            pltpu.VMEM((opm * 4 * n_rows, pair_rows * pair_width), b16),
            pltpu.VMEM((opm * 4 * n_rows, pair_rows * pair_width), b16),
            pltpu.VMEM((cols, pair_width), f32),
            dma((7,)), dma((chunks,)),
            dma((chunks, labels)), dma((chunks, labels)),
            dma((2 * n_y, n_rows)), dma((2 * n_y, n_rows)),
            dma((2, nz, chunks)), dma((nz, chunks)),
            dma((nz, chunks)), dma((nz, chunks)),
            dma((nz, 2)), dma((2 * n_y, per_half)),
            dma((2, nz)), dma((nz,)), dma((nz,)), dma((nz,)),
            dma((nz, 2)), dma((nz, 2)),
            dma((per_half,)), dma((nz,)),
            dma((nz, 4 * n_y - 1)), dma((nz, 4)),
        ],
        compiler_params=pltpu.CompilerParams(
            collective_id=0, has_side_effects=True, vmem_limit_bytes=VMEM_GRANT
        ),
    )(*[
        pltpu.with_memory_space_constraint(a, pltpu.HBM)
        for a in (x, pair, row_mask, residue_mask[None, :], gain[None, :], wq, wk, wv, wg, wo,
                  pair_gain[None, :], bias_w.T, tensor_gain[None, :], left_w.T, right_w.T,
                  weight, residue_mask)
    ])


def fused_body(
    sequence_matrix, pair_representation, alignment_row_mask, residue_mask, attention_scale_vector,
    asking_factor_matrix, lookup_factor_matrix, content_factor_matrix, sigmoid_factor_matrix,
    final_factor_matrix, pair_norm_gain, bias_weight, tensor_scale_vector, first_factor_matrix,
    second_factor_matrix, outer_weight,
):
    return front(
        lax.axis_size("row"), lax.axis_size("head"), sequence_matrix, pair_representation,
        alignment_row_mask, residue_mask, attention_scale_vector, asking_factor_matrix,
        lookup_factor_matrix, content_factor_matrix, sigmoid_factor_matrix, final_factor_matrix,
        pair_norm_gain, bias_weight, tensor_scale_vector, first_factor_matrix, second_factor_matrix,
        outer_weight,
    )


def fits(n_row, n_y, sequence_matrix, pair_representation, bias_weight, first_factor_matrix):
    rows, residues, feat = sequence_matrix.shape
    heads, opm = bias_weight.shape[1], first_factor_matrix.shape[1]
    n_rows, cols, pair_rows, nz = rows // n_row, residues // n_y, residues // n_row, n_row // 4
    if n_row % 4 or nz & (nz - 1) or nz % n_y or heads % (2 * n_y):
        return False
    group_width = heads // n_y // 2 * (feat // heads)
    return (
        n_rows * group_width == 128 and group_width == 64 and 2 * n_rows * opm == 128
        and cols % 128 == 0 and pair_rows % 16 == 0 and pair_representation.shape[2] == 128
        and n_row % 8 == 0
    )


def solution(mesh):
    placed = (P("row", "head", None), P("row", "head", None), P("row")) + (P(),) * 13
    n_row, n_y = mesh.shape["row"], mesh.shape["head"]

    def step(*args):
        chosen = fused_body if fits(n_row, n_y, args[0], args[1], args[11], args[13]) else body
        return jax.shard_map(
            chosen,
            mesh=mesh,
            in_specs=placed,
            out_specs=(P("row", "head", None), P("row", "head", None)),
            check_vma=False,
        )(*args)

    return step
```

```python
import functools
import math

import jax
import jax.numpy as jnp
from jax import lax
from jax.experimental import pallas as pl
from jax.experimental.pallas import tpu as pltpu
from jax.sharding import PartitionSpec as P


HIGH = lax.Precision.HIGHEST
VMEM_GRANT = 40 * 2**20
LOG2E = math.log2(math.e)


def apply_layer_norm(values, gains):
    center = values - jnp.mean(values, axis=-1, keepdims=True)
    spread = jnp.mean(center * center, axis=-1, keepdims=True)
    return center * lax.rsqrt(spread + 1e-05) * gains


def split(x):
    hi = x.astype(jnp.bfloat16)
    lo = (x - hi.astype(jnp.float32)).astype(jnp.bfloat16)
    return hi, lo


def mm(a, b, dims=(((1,), (0,)), ((), ()))):
    return lax.dot_general(a, b, dims, preferred_element_type=jnp.float32)


def split_outside(x):
    hi = lax.reduce_precision(x, 8, 7)
    return hi.astype(jnp.bfloat16), lax.reduce_precision(x - hi, 8, 7).astype(jnp.bfloat16)


NT = (((1,), (1,)), ((), ()))


def bias_kernel(pair_ref, gain_ref, weight_ref, out_ref):
    rows, cols, width = pair_ref.shape
    w_hi, w_lo = split(weight_ref[...])
    heads = w_hi.shape[0]
    w_both = jnp.concatenate([w_hi, w_lo], axis=0)
    for r in range(rows):
        x = apply_layer_norm(pair_ref[r], gain_ref[...])
        x_hi, x_lo = split(x)
        both = mm(w_both, x_hi, NT)
        out_ref[r] = both[:heads] + both[heads:] + mm(w_hi, x_lo, NT)


def pair_bias(pair, gain, weight):
    rows, cols, width = pair.shape
    heads = weight.shape[1]
    step = 4
    return pl.pallas_call(
        bias_kernel,
        grid=(rows // step,),
        in_specs=[
            pl.BlockSpec((step, cols, width), lambda i: (i, 0, 0)),
            pl.BlockSpec((1, width), lambda i: (0, 0)),
            pl.BlockSpec((heads, width), lambda i: (0, 0)),
        ],
        out_specs=pl.BlockSpec((step, heads, cols), lambda i: (i, 0, 0)),
        out_shape=jax.ShapeDtypeStruct((rows, heads, cols), jnp.float32),
        cost_estimate=pl.CostEstimate(flops=10**9, bytes_accessed=5 * 10**6, transcendentals=0),
    )(pair, gain[None, :], weight.T)


def attend_kernel(x_ref, gain_ref, w_ref, bias_ref, key_ref, out_ref, q_ref, k_ref, v_ref):
    blocks, heads, depth, keys = bias_ref.shape
    n_rows = x_ref.shape[0]
    width = v_ref.shape[3] // 2
    local = heads * width
    rows = blocks * depth
    step = pl.program_id(0)

    @pl.when(step == 0)
    def _():
        w_hi, w_lo = split(w_ref[...])
        for s in range(n_rows):
            x_hi, x_lo = split(apply_layer_norm(x_ref[s], gain_ref[...]))
            made = mm(x_hi, w_hi) + mm(x_lo, w_hi) + mm(x_hi, w_lo)
            q_hi, q_lo = split(made[:, :local] * (1.0 / math.sqrt(width)))
            k_hi, k_lo = split(made[:, local:2 * local])
            v_hi, v_lo = split(made[:, 2 * local:])
            for h in range(heads):
                at = slice(h * width, (h + 1) * width)
                q_ref[s, h] = jnp.concatenate([q_hi[:, at], q_hi[:, at], q_lo[:, at]], axis=-1)
                k_ref[s, h] = jnp.concatenate([k_hi[:, at], k_lo[:, at], k_hi[:, at]], axis=-1)
                v_ref[s, h] = jnp.concatenate([v_hi[:, at], v_lo[:, at]], axis=-1)

    key_bias = key_ref[...]
    mine = pl.ds(pl.multiple_of(step * rows, rows), rows)
    for s in range(n_rows):
        pieces = []
        for h in range(heads):
            logits = mm(q_ref[s, h, mine, :], k_ref[s, h], NT)
            logits = logits + bias_ref[:, h].reshape(rows, keys) + key_bias
            largest = jnp.max(logits, axis=-1, keepdims=True)
            e = jnp.exp(logits - largest)
            total = jnp.sum(e, axis=-1, keepdims=True)
            e_hi, e_lo = split(e)
            v = v_ref[s, h]
            both = mm(e_hi, v)
            got = both[:, :width] + both[:, width:] + mm(e_lo, v[:, :width])
            pieces.append(got / total)
        out_ref[s] = jnp.concatenate(pieces, axis=-1)


def attend(x, gain, weight, bias, key_bias):
    n_rows, residues, features = x.shape
    groups, heads, depth, keys = bias.shape
    local = weight.shape[1] // 3
    width = local // heads
    blocks = max(1, 128 // depth)
    rows = blocks * depth
    return pl.pallas_call(
        attend_kernel,
        grid=(groups // blocks,),
        in_specs=[
            pl.BlockSpec(x.shape, lambda i: (0, 0, 0)),
            pl.BlockSpec((1, features), lambda i: (0, 0)),
            pl.BlockSpec(weight.shape, lambda i: (0, 0)),
            pl.BlockSpec((blocks, heads, depth, keys), lambda i: (i, 0, 0, 0)),
            pl.BlockSpec((1, keys), lambda i: (0, 0)),
        ],
        out_specs=pl.BlockSpec((n_rows, rows, local), lambda i: (0, i, 0)),
        out_shape=jax.ShapeDtypeStruct((n_rows, residues, local), jnp.float32),
        scratch_shapes=[
            pltpu.VMEM((n_rows, heads, residues, 3 * width), jnp.bfloat16),
            pltpu.VMEM((n_rows, heads, residues, 3 * width), jnp.bfloat16),
            pltpu.VMEM((n_rows, heads, residues, 2 * width), jnp.bfloat16),
        ],
        cost_estimate=pl.CostEstimate(flops=4 * 10**9, bytes_accessed=6 * 10**6, transcendentals=2 * 10**6),
    )(x, gain[None, :], weight, bias, key_bias)


def outer_kernel(scale_ref, left_ref, weight_ref, right_ref, live_ref, pair_ref, out_ref,
                 r_hi, r_lo, t_hi, t_lo):
    step, cols, depth = pair_ref.shape
    rows_all = r_hi.shape[1]
    n_rows = left_ref.shape[0] // step
    width = rows_all // n_rows
    me = pl.program_id(0)

    @pl.when(me == 0)
    def _():
        hi, lo = split(right_ref[...].T)
        r_hi[...] = hi
        r_lo[...] = lo

    left = left_ref[...]
    group = 2
    for d0 in range(0, width, group):
        t = mm(left, weight_ref[:, d0 * depth:(d0 + group) * depth])
        hi, lo = split(t)
        for g in range(group):
            d = d0 + g
            for i in range(step):
                src = (slice(i * n_rows, (i + 1) * n_rows), slice(g * depth, (g + 1) * depth))
                dst = (slice(d * n_rows, (d + 1) * n_rows), slice(i * depth, (i + 1) * depth))
                t_hi[dst] = hi[src]
                t_lo[dst] = lo[src]
    update = mm(r_hi[...], t_hi[...]) + mm(r_lo[...], t_hi[...]) + mm(r_hi[...], t_lo[...])
    for i in range(step):
        norm = scale_ref[me * step + i] * live_ref[...] + 0.001
        out_ref[i] = pair_ref[i] + update[:, i * depth:(i + 1) * depth] / norm


def outer_mean(scale, left, weight, right, live, pair):
    rows, cols, depth = pair.shape
    total = right.shape[0]
    n_rows = left.shape[0] // rows
    packed = left.shape[1]
    step = 4
    return pl.pallas_call(
        outer_kernel,
        grid=(rows // step,),
        in_specs=[
            pl.BlockSpec(memory_space=pltpu.SMEM),
            pl.BlockSpec((step * n_rows, packed), lambda i: (i, 0)),
            pl.BlockSpec(weight.shape, lambda i: (0, 0)),
            pl.BlockSpec(right.shape, lambda i: (0, 0)),
            pl.BlockSpec((cols, 1), lambda i: (0, 0)),
            pl.BlockSpec((step, cols, depth), lambda i: (i, 0, 0)),
        ],
        out_specs=pl.BlockSpec((step, cols, depth), lambda i: (i, 0, 0)),
        out_shape=jax.ShapeDtypeStruct(pair.shape, jnp.float32),
        scratch_shapes=[
            pltpu.VMEM((cols, total), jnp.bfloat16),
            pltpu.VMEM((cols, total), jnp.bfloat16),
            pltpu.VMEM((total, step * depth), jnp.bfloat16),
            pltpu.VMEM((total, step * depth), jnp.bfloat16),
        ],
        cost_estimate=pl.CostEstimate(flops=9 * 10**9, bytes_accessed=10**7, transcendentals=0),
    )(scale, left, weight, right, live, pair)


def gather_kernel(n, block_ref, out_ref, own_sem, send_sem, recv_sem):
    me = lax.axis_index("row")
    core = me % 2
    x = (me // 2) % 2
    nz = n // 4
    z = me // 4

    def place(zz, xx, cc):
        return (zz * 2 + xx) * 2 + cc

    barrier = pltpu.get_barrier_semaphore()
    up_ok, down_ok = z + 1 < nz, z >= 1

    def greet(target):
        pl.semaphore_signal(barrier, inc=1, device_id={"row": target},
                            device_id_type=pl.DeviceIdType.MESH)

    greet(place(z, x, 1 - core))
    greet(place(z, 1 - x, core))
    pl.when(up_ok)(lambda: greet(place(z + 1, x, core)))
    pl.when(down_ok)(lambda: greet(place(z - 1, x, core)))
    peers = 2 + jnp.where(up_ok, 1, 0) + jnp.where(down_ok, 1, 0)
    pl.semaphore_wait(barrier, peers)

    own = pltpu.make_async_copy(block_ref, out_ref.at[me], own_sem)
    own.start()

    def sends(d, other):
        found = []
        first = core == 0
        if other == 0:
            cross = (z >= 0) if d == 0 else jnp.logical_not(first)
            run = z >= 0
        else:
            cross = None
            run = first
        if d <= 0:
            found.append((jnp.logical_and(run, up_ok), 0, lambda: place(z + 1, x, core)))
        if d >= 0:
            found.append((jnp.logical_and(run, down_ok), 1, lambda: place(z - 1, x, core)))
        if cross is not None:
            found.append((cross, 2, lambda: place(z, 1 - x, core)))
        found.append((z >= 0, 3, lambda: place(z, x, 1 - core)))
        return found

    def copy(source, kind, target, mine):
        return pltpu.make_async_remote_copy(
            src_ref=block_ref if mine else out_ref.at[source],
            dst_ref=out_ref.at[source],
            send_sem=send_sem.at[kind, source],
            recv_sem=recv_sem.at[source],
            device_id={"row": target},
            device_id_type=pl.DeviceIdType.MESH,
        )

    hops = [(0, 0), (0, 1)]
    for far in range(1, nz):
        hops += [(-far, 0), (far, 0), (-far, 1), (far, 1)]

    def each(action):
        for d, other in hops:
            source = place(z + d, (x + other) % 2, core)
            mine = d == 0 and other == 0
            there = jnp.logical_and(z + d >= 0, z + d < nz)

            @pl.when(there)
            def _(d=d, other=other, source=source, mine=mine):
                action(d, other, source, mine)

    def forward(d, other, source, mine):
        if not mine:
            copy(source, 3, place(z, x, 1 - core), False).wait_recv()
        for ok, kind, target in sends(d, other):
            pl.when(ok)(lambda kind=kind, target=target: copy(source, kind, target(), mine).start())

    def finish(d, other, source, mine):
        for ok, kind, target in sends(d, other):
            pl.when(ok)(lambda kind=kind, target=target: copy(source, kind, target(), mine).wait_send())

    each(forward)
    for k in range(n // 2):
        copy(2 * k + 1 - core, 3, place(z, x, 1 - core), False).wait_recv()
    each(finish)
    own.wait()


def gather_rows(block, n, ident):
    return pl.pallas_call(
        functools.partial(gather_kernel, n),
        out_shape=jax.ShapeDtypeStruct((n,) + block.shape, block.dtype),
        in_specs=[pl.BlockSpec(memory_space=pltpu.VMEM)],
        out_specs=pl.BlockSpec(memory_space=pl.ANY),
        scratch_shapes=[
            pltpu.SemaphoreType.DMA,
            pltpu.SemaphoreType.DMA((4, n)),
            pltpu.SemaphoreType.DMA((n,)),
        ],
        compiler_params=pltpu.CompilerParams(collective_id=ident, has_side_effects=True),
    )(block)


def around(n):
    return [[(src, (src + k) % n) for src in range(n)] for k in range(n)]


def gather_heads(block, n, index, axis):
    size = block.shape[axis]
    shape = list(block.shape)
    shape[axis] = size * n
    whole = jnp.zeros(shape, block.dtype)
    for k in range(n):
        part = block if k == 0 else lax.ppermute(block, "head", around(n)[k])
        whole = lax.dynamic_update_slice_in_dim(whole, part, ((index - k) % n) * size, axis)
    return whole


def exchange_heads(block, n, index, split_axis, concat_axis):
    size = block.shape[split_axis] // n
    shape = list(block.shape)
    shape[split_axis] = size
    length = shape[concat_axis]
    shape[concat_axis] = length * n
    whole = jnp.zeros(shape, block.dtype)
    for k in range(n):
        part = lax.dynamic_slice_in_dim(block, ((index + k) % n) * size, size, split_axis)
        if k:
            part = lax.ppermute(part, "head", around(n)[k])
        whole = lax.dynamic_update_slice_in_dim(whole, part, ((index - k) % n) * length, concat_axis)
    return whole


def body(
    sequence_matrix,
    pair_representation,
    alignment_row_mask,
    residue_mask,
    attention_scale_vector,
    asking_factor_matrix,
    lookup_factor_matrix,
    content_factor_matrix,
    sigmoid_factor_matrix,
    final_factor_matrix,
    pair_norm_gain,
    bias_weight,
    tensor_scale_vector,
    first_factor_matrix,
    second_factor_matrix,
    outer_weight,
):
    head_count = lax.axis_size("head")
    head_index = lax.axis_index("head")
    row_index = lax.axis_index("row")
    row_count = lax.axis_size("row")
    n_rows, col_count, width = sequence_matrix.shape
    residues = col_count * head_count
    pair_rows = pair_representation.shape[0]
    pair_depth = pair_representation.shape[2]
    heads_all = bias_weight.shape[1]
    head_width = width // heads_all
    local_heads = heads_all // head_count
    local_width = local_heads * head_width
    opm_width = first_factor_matrix.shape[1]

    sequence_all = gather_heads(sequence_matrix, head_count, head_index, 1)

    bias_all = pair_bias(pair_representation, pair_norm_gain, bias_weight)
    bias_part = exchange_heads(
        bias_all.transpose(1, 0, 2), head_count, head_index, 0, 2
    )
    bias = gather_rows(bias_part, row_count, 0)
    key_bias = ((residue_mask.astype(jnp.float32) - 1.0) * 1000000000.0)[None, :]

    weights = jnp.concatenate(
        [
            lax.dynamic_slice_in_dim(w, head_index * local_width, local_width, 1)
            for w in (asking_factor_matrix, lookup_factor_matrix, content_factor_matrix)
        ],
        axis=1,
    )
    attended = attend(sequence_all, attention_scale_vector, weights, bias, key_bias)
    norm_mine = apply_layer_norm(sequence_matrix, attention_scale_vector)
    gate = jax.nn.sigmoid(
        jnp.einsum("sic,ce->sie", norm_mine, sigmoid_factor_matrix, precision=HIGH)
    )
    returned_values = exchange_heads(attended, head_count, head_index, 1, 2) * gate
    alignment_updated = sequence_matrix + jnp.einsum(
        "jna,ab->jnb", returned_values, final_factor_matrix, precision=HIGH
    )

    outer_product_norm = apply_layer_norm(alignment_updated, tensor_scale_vector)
    live_cols = lax.dynamic_slice_in_dim(residue_mask, head_index * col_count, col_count).astype(
        jnp.float32
    )
    row_live = alignment_row_mask.astype(jnp.float32)
    live = row_live[:, None] * live_cols[None, :]
    left_side = (
        jnp.einsum("sic,co->soi", outer_product_norm, first_factor_matrix, precision=HIGH)
        * live[:, None, :]
    )
    right = (
        jnp.einsum("sic,co->soi", outer_product_norm, second_factor_matrix, precision=HIGH)
        * live[:, None, :]
    )
    left_all = gather_heads(left_side, head_count, head_index, 1)
    carried = jnp.broadcast_to(row_live[:, None, None], (n_rows, 8, col_count))
    sides = gather_rows(jnp.concatenate([left_all, right, carried], axis=1), row_count, 1)
    sides = sides.reshape(row_count * n_rows, -1, col_count)
    left_width = head_count * opm_width
    first_row = row_index * pair_rows
    left_mine = lax.dynamic_slice(
        sides,
        (0, (first_row // col_count) * opm_width, first_row % col_count),
        (row_count * n_rows, opm_width, pair_rows),
    )
    right_all = sides[:, left_width:]
    total_rows = row_count * n_rows
    count = jnp.sum(right_all[:, opm_width, 0])
    right_rows = right_all[:, :opm_width].transpose(1, 0, 2).reshape(
        opm_width * total_rows, col_count
    )
    left_rows = left_mine.transpose(2, 0, 1).reshape(pair_rows * total_rows, opm_width)
    l_hi, l_lo = split_outside(left_rows)
    w_hi, w_lo = split_outside(outer_weight.reshape(opm_width, opm_width * pair_depth))
    rows_live = lax.dynamic_slice_in_dim(residue_mask, row_index * pair_rows, pair_rows).astype(
        jnp.float32
    )
    pair_out = outer_mean(
        count * rows_live,
        jnp.concatenate([l_hi, l_hi, l_lo], axis=1),
        jnp.concatenate([w_hi, w_lo, w_hi], axis=0),
        right_rows,
        live_cols[:, None],
        pair_representation,
    )
    return alignment_updated, pair_out


def ln(values, gains):
    return apply_layer_norm(values, gains)


def front_kernel(
    x_hbm, pair_hbm, row_mask_hbm, key_hbm, gain_hbm, wq_hbm, wk_hbm, wv_hbm, wg_hbm, wo_hbm,
    pair_gain_hbm, bias_hbm, tensor_gain_hbm, left_hbm, right_hbm, weight_hbm, mask_hbm,
    msa_ref, acc_ref,
    x_ref, pair_ref, wq_ref, wk_ref, wv_ref, wg_ref, wo_ref, wpair_ref, group_ref,
    bias_ref, xn_ref, q_ref, k_ref, v_ref, absent_ref, logit_ref, e_ref, gate_ref, att_out, att_in, right_buf, left_loc, left_own,
    left_in, row_mask, mask_ref, key_ref, gain_ref, pair_gain, bias_w, tensor_gain, left_w, right_w,
    weight_ref, w_ref, rows_ref, rt_ref, r_hi, r_lo, t_hi_0, t_hi_1, t_lo_0, t_lo_1, live_ref,
    load_sem, pair_sem, s1_send, s1_recv, n_send, n_recv, z_send, z_recv, x_send, x_recv, xl_send, t_send, t_recv,
    a_send, a_recv, rz_send, rz_recv, rx_send, rx_recv, rc_send, rc_recv,
    l1_send, l1_recv, l2_send, l2_recv,
):
    nz, _, chunks, _, n_y, group_heads, sub, cols = bias_ref.shape
    n_rows, _, feat = x_ref.shape
    heads = bias_w.shape[0]
    keys = n_y * cols
    width = k_ref.shape[3] // 4
    group_width = group_heads * width
    local_width = 2 * group_width
    per_half = nz // n_y
    plane = cols // per_half
    pair_width = pair_ref.shape[2]
    opm = left_w.shape[0]

    me, y = lax.axis_index("row"), lax.axis_index("head")
    c, x, z = me % 2, (me // 2) % 2, me // 4
    half = z // per_half

    def place(zz, xx, cc):
        return (zz * 2 + xx) * 2 + cc

    def across(d):
        out, bit = z, 1
        while bit <= d:
            if d & bit:
                out = out + bit * (1 - 2 * ((out // bit) % 2))
            bit *= 2
        return out

    def plane_at(p):
        if p < 2:
            return across(p)
        return jnp.where(z < nz // 2, p, nz - 1 - p)

    def remote(src, dst, send, recv, row, head):
        return pltpu.make_async_remote_copy(
            src_ref=src, dst_ref=dst, send_sem=send, recv_sem=recv,
            device_id={"row": row, "head": head}, device_id_type=pl.DeviceIdType.MESH,
        )

    def arrived(dst, send, recv):
        remote(dst, dst, send, recv, place(z, x, 1 - c), y).wait_recv()

    pending = []

    def go(copy):
        copy.start()
        pending.append(copy)

    loads = {}
    for at, (src, dst) in enumerate(
        [(x_hbm, x_ref), (wq_hbm, wq_ref), (wk_hbm, wk_ref), (wv_hbm, wv_ref), (wg_hbm, wg_ref), (wo_hbm, wo_ref),
         (weight_hbm, weight_ref), (pair_gain_hbm, pair_gain), (bias_hbm, bias_w), (gain_hbm, gain_ref),
         (key_hbm, key_ref), (row_mask_hbm, row_mask), (mask_hbm, mask_ref), (tensor_gain_hbm, tensor_gain),
         (left_hbm, left_w), (right_hbm, right_w)]
    ):
        loads[at] = pltpu.make_async_copy(src, dst, load_sem.at[at])
    pair_loads = [
        pltpu.make_async_copy(
            pair_hbm.at[pl.ds(k * sub, sub)], pair_ref.at[pl.ds(k * sub, sub)], pair_sem.at[k]
        )
        for k in range(chunks)
    ]
    for at in (7, 8):
        loads[at].start()
    for copy in pair_loads:
        copy.start()
    for at in [0, 9, 10] + list(range(1, 7)) + list(range(11, 16)):
        loads[at].start()

    barrier = pltpu.get_barrier_semaphore()
    peers = []
    for dx in range(2):
        for dc in range(2):
            for dy in range(n_y):
                if dx or dc or dy:
                    peers.append((place(z, (x + dx) % 2, (c + dc) % 2), (y + dy) % n_y))
    for d in range(1, nz):
        peers.append((place(across(d), x, c), y))
    for row, head in peers:
        pl.semaphore_signal(barrier, inc=1, device_id={"row": row, "head": head},
                            device_id_type=pl.DeviceIdType.MESH)

    for at in (7, 8):
        loads[at].wait()
    w_hi, w_lo = split(bias_w[...] * LOG2E)
    spread = sub * heads
    at_row = lax.broadcasted_iota(jnp.int32, (heads, sub, pair_width), 1).reshape(spread, pair_width)
    zero = jnp.zeros((spread, pair_width), jnp.float32)

    def rows_of(part):
        part = part.astype(jnp.float32)
        return jnp.broadcast_to(part[:, None, :], (heads, sub, pair_width)).reshape(spread, pair_width)

    rep_hi, rep_lo = rows_of(w_hi), rows_of(w_lo)
    for t in range(sub // 2):
        first, second = at_row == 2 * t, at_row == 2 * t + 1
        both = [
            jnp.concatenate([jnp.where(first, rep, zero), jnp.where(second, rep, zero)], axis=1)
            for rep in (rep_hi, rep_lo)
        ]
        wpair_ref[t] = jnp.concatenate(both, axis=0).astype(jnp.bfloat16)

    def bias_chunk(k):
        pair_loads[k].wait()
        total = None
        for t in range(sub // 2):
            at = k * sub + 2 * t
            pieces = [split(ln(pair_ref[at + e], pair_gain[...])) for e in range(2)]
            hi = jnp.concatenate([pieces[0][0], pieces[1][0]], axis=1)
            lo = jnp.concatenate([pieces[0][1], pieces[1][1]], axis=1)
            both = mm(wpair_ref[t], hi, NT)
            part = both[:spread] + both[spread:] + mm(wpair_ref[t, :spread], lo, NT)
            total = part if total is None else total + part
        group_ref[k] = total.reshape(2 * n_y, group_heads, sub, cols)
        bias_ref[z, x, k, c, y] = group_ref[k, y * 2 + c]

    labels = [(dy, dc) for dy in range(n_y) for dc in range(2) if dy or dc]

    def stage_one(k):
        for at, (dy, dc) in enumerate(labels):
            ty, tc = (y + dy) % n_y, (c + dc) % 2
            go(remote(group_ref.at[k, ty * 2 + tc], bias_ref.at[z, x, k, c, y],
                      s1_send.at[k, at], s1_recv.at[k, at], place(z, x, tc), ty))

    def stage_two(k):
        for at, (dy, dc) in enumerate(labels):
            sy, sc = (y + n_y - dy) % n_y, (c + dc) % 2
            arrived(bias_ref.at[z, x, k, sc, sy], s1_send.at[k, at], s1_recv.at[k, at])
        own = bias_ref.at[z, x, k]
        for up in range(2):
            pl.when(reaches(up, 1))(lambda up=up: relay_copy(up, z, k).start())
        cross_copy(z, k).start()

    def relay_copy(up, zz, k):
        block = bias_ref.at[zz, x] if k is None else bias_ref.at[zz, x, k]
        return remote(block, block, z_send.at[up, zz], z_recv.at[zz, 0 if k is None else k],
                      place(z + 1 if up else z - 1, x, c), y)

    def reaches(up, j):
        return z + j < nz if up else z >= j

    def source(up, j):
        return (z - j, z >= j) if up else (z + j, z + j < nz)

    def pass_on(j, k):
        for up in range(2):
            zz, there = source(up, j)

            @pl.when(there)
            def _(up=up, zz=zz):
                block = bias_ref.at[zz, x, k]
                arrived(block, z_send.at[0, 0], z_recv.at[zz, k])
                if j < nz - 1:
                    pl.when(reaches(up, 1))(lambda: relay_copy(up, zz, k).start())
                cross_copy(zz, k, True).start()
                if k == last_chunk:
                    twin = bias_ref.at[zz, 1 - x, last_chunk, 0]
                    arrived(twin, t_send.at[0, 0], t_recv.at[zz])
                    if j < nz - 1:
                        pl.when(reaches(up, 1))(lambda: twin_copy(up, zz).start())

    last_chunk = chunks - 1

    def cross_copy(zz, k, beyond=False):
        block = bias_ref.at[zz, x, k, 1] if beyond and k == last_chunk else bias_ref.at[zz, x, k]
        return remote(block, block, (xl_send if k == last_chunk else x_send).at[zz], x_recv.at[zz, k],
                      place(z, 1 - x, c), y)

    def twin_copy(up, zz):
        block = bias_ref.at[zz, 1 - x, last_chunk, 0]
        return remote(block, block, t_send.at[up, zz], t_recv.at[zz], place(z + 1 if up else z - 1, x, c), y)

    def start_twins():
        arrived(bias_ref.at[z, 1 - x, last_chunk], xl_send.at[0], x_recv.at[z, last_chunk])
        for up in range(2):
            pl.when(reaches(up, 1))(lambda up=up: twin_copy(up, z).start())

    bias_chunk(0)
    pl.semaphore_wait(barrier, len(peers))
    stage_one(0)
    for k in range(1, chunks):
        bias_chunk(k)
        stage_one(k)
        if k >= 2:
            stage_two(k - 2)

    for at in (0, 9, 10):
        loads[at].wait()
    for s in range(n_rows):
        xn_ref[y, c, s] = ln(x_ref[s], gain_ref[...])
        own_x = xn_ref.at[y, c, s]
        for dy in range(1, n_y):
            go(remote(own_x, own_x, n_send.at[dy, s], n_recv.at[dy, s], place(z, x, c), (y + dy) % n_y))
        go(remote(own_x, own_x, n_send.at[0, s], n_recv.at[0, s], place(z, x, 1 - c), y))
    stage_two(chunks - 2)

    for at in (1, 2, 3):
        loads[at].wait()
    mine = pl.ds(pl.multiple_of(y * local_width, local_width), local_width)
    picked = []
    for ref in (wq_ref, wk_ref, wv_ref):
        whole = ref[:, mine]
        picked.append(jnp.where(c == 0, whole[:, :group_width], whole[:, group_width:]))
    wa_hi, wa_lo = split(jnp.concatenate(picked, axis=1))

    lane = lax.broadcasted_iota(jnp.int32, (cols, width), 1)
    pick = jnp.where(lane < 2, 1.0, 0.0).astype(jnp.bfloat16)
    one, none = jnp.ones((cols, width), jnp.bfloat16), jnp.zeros((cols, width), jnp.bfloat16)
    for yy in range(n_y):
        keep = jnp.broadcast_to(
            key_ref[:, yy * cols:(yy + 1) * cols].astype(jnp.float32), (pair_width, cols)
        ).T[:, :width]
        hi, lo = split((keep - 1.0) * (1000000000.0 * LOG2E))
        absent_ref[yy] = jnp.where(
            lane == 0, hi.astype(jnp.float32), jnp.where(lane == 1, lo.astype(jnp.float32), 0.0)
        ).astype(jnp.bfloat16)

    def project(yy, cc, rows=range(n_rows)):
        spot = pl.ds(pl.multiple_of(yy * cols, cols), cols)
        absent = absent_ref[yy]
        for s in rows:
            hi, lo = split(xn_ref[yy, cc, s])
            made = mm(hi, wa_hi) + mm(lo, wa_hi) + mm(hi, wa_lo)
            q_hi, q_lo = split(made[:, :group_width] * (LOG2E / math.sqrt(width)))
            k_hi, k_lo = split(made[:, group_width:2 * group_width])
            v_hi, v_lo = split(made[:, 2 * group_width:])
            for h in range(group_heads):
                at = slice(h * width, (h + 1) * width)
                to = cc * n_rows + s
                q_ref[to, h, spot, :] = jnp.concatenate([q_hi[:, at], q_hi[:, at], q_lo[:, at], pick], axis=-1)
                k_ref[to, h, spot, :] = jnp.concatenate([k_hi[:, at], k_lo[:, at], k_hi[:, at], absent], axis=-1)
                mine_at, count_at = s * group_heads + h, (s * group_heads + h + 1) % (n_rows * group_heads)
                parts = [none] * (2 * n_rows * group_heads)
                parts[mine_at], parts[count_at], parts[n_rows * group_heads + mine_at] = v_hi[:, at], one, v_lo[:, at]
                v_ref[to, h, spot, :] = jnp.concatenate(parts, axis=-1)

    project(y, c)
    stage_two(chunks - 1)

    def gate_rows(s):
        hi, lo = split(xn_ref[y, c, s])
        gate_ref[s] = jax.nn.sigmoid(mm(hi, g_hi) + mm(lo, g_hi) + mm(hi, g_lo))

    def own_rows(s):
        arrived(xn_ref.at[y, 1 - c, s], n_send.at[0, s], n_recv.at[0, s])
        project(y, 1 - c, [s])

    def spread_weight(d0, d1):
        for d in range(d0, d1):
            hi, lo = split(weight_ref[pl.ds(d, opm, stride=opm), :])
            w_ref[:, d * pair_width:(d + 1) * pair_width] = jnp.concatenate([hi, lo, hi], axis=0)

    def clear(i0, i1):
        acc_ref[i0:i1] = jnp.zeros((i1 - i0, cols, pair_width), jnp.float32)

    loads[4].wait()
    g_hi, g_lo = split(wg_ref[...])
    loads[6].wait()
    pair_rows = pair_ref.shape[0]
    fillers = [functools.partial(gate_rows, s) for s in range(n_rows)]
    fillers += [functools.partial(own_rows, s) for s in range(n_rows)]
    quarter = opm // 4
    fillers += [functools.partial(spread_weight, i * quarter, (i + 1) * quarter) for i in range(4)]
    part = pair_rows // 4
    fillers += [functools.partial(clear, i * part, (i + 1) * part) for i in range(4)]
    tasks = [(j, k) for j in range(1, nz) for k in range(chunks)]

    def advance(n_tasks, n_fillers):
        for _ in range(n_tasks):
            if tasks:
                pass_on(*tasks.pop(0))
            if n_fillers and fillers:
                fillers.pop(0)()

    advance(2, 2)
    start_twins()
    advance(4, 4)
    while fillers:
        fillers.pop(0)()
    for dy in range(1, n_y):
        sy = (y + n_y - dy) % n_y
        for s in range(n_rows):
            block = xn_ref.at[sy, c, s]
            arrived(block, n_send.at[dy, s], n_recv.at[dy, s])
            go(remote(block, block, n_send.at[n_y + dy, s], n_recv.at[n_y + dy, s], place(z, x, 1 - c), y))
            advance(1, 0)
            project(sy, c, [s])
            advance(1 if s + 1 < n_rows else 0, 0)
    for dy in range(1, n_y):
        sy = (y + n_y - dy) % n_y
        for s in range(n_rows):
            arrived(xn_ref.at[sy, 1 - c, s], n_send.at[n_y + dy, s], n_recv.at[n_y + dy, s])
            project(sy, 1 - c, [s])
    advance(max(0, len(tasks) - 2), 0)
    for copy in pending:
        copy.wait_send()
    pending.clear()

    own = pl.ds(pl.multiple_of(y * cols, cols), cols)
    live_ref[...] = jnp.broadcast_to(key_ref[:, own].astype(jnp.float32), (pair_width, cols)).T

    lanes = n_rows * group_width
    block = lax.broadcasted_iota(jnp.int32, (plane, lanes), 1) // width

    def attended_copy(d, ct):
        zz = plane_at(d)
        return remote(att_out.at[d, ct], att_in.at[y * 2 + c, zz % per_half],
                      a_send.at[d, ct], a_recv.at[y * 2 + c, zz % per_half],
                      place(z, x, ct), zz // per_half)

    def is_mine(d, ct):
        return jnp.logical_and(plane_at(d) // per_half == y, ct == c)

    def attend_plane(d):
        zz = plane_at(d)
        for k in range(last_chunk):
            arrived(bias_ref.at[zz, 1 - x, k], x_send.at[0], x_recv.at[zz, k])
        if d:
            arrived(bias_ref.at[zz, 1 - x, last_chunk, 1], xl_send.at[0], x_recv.at[zz, last_chunk])
        queries = pl.ds(pl.multiple_of(zz * plane, plane), plane)

        tiles = [
            jnp.concatenate(
                [
                    jnp.concatenate(
                        [bias_ref[zz, xx, :, cc, yy, h].reshape(chunks * sub, cols) for yy in range(n_y)],
                        axis=1,
                    )
                    for xx in range(2)
                    for cc in range(2)
                ],
                axis=0,
            )
            for h in range(group_heads)
        ]
        units = [(s, h) for s in range(n_rows) for h in range(group_heads)]

        def compare(ct):
            for at, (s, h) in enumerate(units):
                row = ct * n_rows + s
                logit_ref[ct, at] = mm(q_ref[row, h, queries, :], k_ref[row, h], NT) + tiles[h]

        def soften(ct):
            for at in range(len(units)):
                logits = logit_ref[ct, at]
                e_hi, e_lo = split(jnp.exp2(logits - jnp.max(logits, axis=-1, keepdims=True)))
                e_ref[ct, at, :plane] = e_hi
                e_ref[ct, at, plane:] = e_lo

        def gather(ct):
            upper = lower = None
            for at, (s, h) in enumerate(units):
                row = ct * n_rows + s
                both = mm(e_ref[ct, at, :plane], v_ref[row, h])
                whole = both[:, :lanes] + both[:, lanes:] + mm(e_ref[ct, at, plane:], v_ref[row, h, :, :lanes])
                upper = whole if upper is None else jnp.where(block == at, whole, upper)
                lower = whole if lower is None else jnp.where(block == (at + 1) % len(units), whole, lower)
            return upper / pltpu.roll(lower, lanes - width, 1)

        compare(0)
        soften(0)
        compare(1)
        values = [gather(0)]
        soften(1)
        values.append(gather(1))
        for ct in range(2):
            att_out[d, ct] = values[ct]
        for ct in range(2):
            @pl.when(is_mine(d, ct))
            def _(ct=ct):
                att_in[y * 2 + c, zz % per_half] = att_out[d, ct]

            pl.when(jnp.logical_not(is_mine(d, ct)))(lambda ct=ct: attended_copy(d, ct).start())

    for d in range(nz):
        attend_plane(d)
        advance(1 if d + 2 < nz else len(tasks), 0)

    for dy, dc in labels:
        sy, sc = (y + n_y - dy) % n_y, (c + dc) % 2
        for p in range(per_half):
            arrived(att_in.at[sy * 2 + sc, p], a_send.at[0, 0], a_recv.at[sy * 2 + sc, p])

    for at in (5,) + tuple(range(11, 16)):
        loads[at].wait()
    o_hi, o_lo = split(wo_ref[...])
    wide = n_rows * opm
    left_hi, left_lo = split(left_w[...])
    left_both = jnp.concatenate([left_hi, left_lo], axis=0)
    right_hi, right_lo = split(right_w[...])
    right_both = jnp.concatenate([right_hi, right_lo], axis=0)
    lefts = []
    count = jnp.zeros((sub, cols), jnp.float32)
    for s in range(n_rows):
        at = slice(s * group_width, (s + 1) * group_width)
        whole = jnp.concatenate(
            [
                jnp.concatenate([att_in[g, p][:, at] for p in range(per_half)], axis=0)
                for g in range(2 * n_y)
            ],
            axis=1,
        ) * gate_ref[s]
        hi, lo = split(whole)
        out = x_ref[s] + (mm(hi, o_hi) + mm(lo, o_hi) + mm(hi, o_lo))
        msa_ref[s] = out
        f_hi, f_lo = split(ln(out, tensor_gain[...]))
        live = row_mask[s].astype(jnp.float32)
        both = mm(right_both, f_hi, NT)
        right_buf[z, x * 2 + c, s * opm:(s + 1) * opm, :] = (both[:opm] + both[opm:] + mm(right_hi, f_lo, NT)) * live
        both = mm(f_hi, left_both, NT)
        lefts.append((both[:, :opm] + both[:, opm:] + mm(f_lo, left_hi, NT)) * live)
        count = count + live
    right_buf[z, x * 2 + c, wide:, :] = count

    left = jnp.concatenate(lefts, axis=1)
    blocks = per_half * 4
    tall = left.shape[0] // blocks // 2
    left = left.reshape(blocks, 2, tall, wide)
    left_loc[...] = jnp.concatenate([left[:, 0], left[:, 1]], axis=2)

    def left_copy(p):
        return remote(left_loc.at[pl.ds(p * 4, 4)], left_own.at[z], l1_send.at[p], l1_recv.at[z],
                      place(y * per_half + p, x, c), y)

    for p in range(per_half):
        here = y * per_half + p == z

        @pl.when(here)
        def _(p=p):
            left_own[z] = left_loc[p * 4:(p + 1) * 4]

        pl.when(jnp.logical_not(here))(lambda p=p: left_copy(p).start())

    def right_core(zz, far):
        block = right_buf.at[zz, (x if far == 0 else 1 - x) * 2 + c]
        return remote(block, block, rc_send.at[zz, far], rc_recv.at[zz, far], place(z, x, 1 - c), y)

    def right_direct(d):
        block = right_buf.at[z, x * 2 + c]
        return remote(block, block, rz_send.at[d], rz_recv.at[z], place(across(d), x, c), y)

    def right_cross(zz):
        block = right_buf.at[zz, x * 2 + c]
        return remote(block, block, rx_send.at[zz], rx_recv.at[zz], place(z, 1 - x, c), y)

    right_cross(z).start()
    right_core(z, 0).start()
    for d in range(1, nz):
        right_direct(d).start()

    owner = half == y
    finals = [(dx, dc, dy) for dx in range(2) for dc in range(2) for dy in range(n_y) if dx or dc or dy]

    def final_copy(at, zz):
        dx, dc, dy = finals[at]
        tx, tc, ty = (x + dx) % 2, (c + dc) % 2, (y + dy) % n_y
        return remote(left_own.at[zz, tx * 2 + tc], left_in.at[zz, x * 2 + c], l2_send.at[zz, at],
                      l2_recv.at[zz, x * 2 + c], place(z, tx, tc), ty)

    def left_pass(zz):
        @pl.when(owner)
        def _():
            pl.when(zz != z)(lambda: arrived(left_own.at[zz], l1_send.at[0], l1_recv.at[zz]))
            for at in range(len(finals)):
                final_copy(at, zz).start()
            left_in[zz, x * 2 + c] = left_own[zz, x * 2 + c]

    def left_wait(zz):
        for xx in range(2):
            for cc in range(2):
                mine_too = jnp.logical_and(owner, jnp.logical_and(xx == x, cc == c))

                @pl.when(jnp.logical_not(mine_too))
                def _(xx=xx, cc=cc):
                    arrived(left_in.at[zz, xx * 2 + cc], l2_send.at[0, 0], l2_recv.at[zz, xx * 2 + cc])

    def right_pass(zz):
        arrived(right_buf.at[zz, x * 2 + c], rz_send.at[0], rz_recv.at[zz])
        right_cross(zz).start()
        right_core(zz, 0).start()

    def right_far(zz):
        arrived(right_buf.at[zz, (1 - x) * 2 + c], rx_send.at[0], rx_recv.at[zz])
        right_core(zz, 1).start()

    def ordered(p):
        late = jnp.where(z < nz // 2, p, nz - 1 - p)
        return jnp.where(p == 0, z, jnp.where(p == 1, across(1), late))

    tall = pair_ref.shape[0] // 2
    t_hi, t_lo = (t_hi_0, t_hi_1), (t_lo_0, t_lo_1)
    slots = 4 * n_rows
    group = 4

    def left_rows(zz):
        for i in range(2 * tall):
            block = left_in[zz, :, i % tall, :]
            base = (i // tall) * wide
            rows_ref[i * slots:(i + 1) * slots, :] = jnp.concatenate(
                [block[:, base + s * opm:base + (s + 1) * opm] for s in range(n_rows)], axis=0
            )
        hi, lo = split(rows_ref[...])
        return jnp.concatenate([hi, hi, lo], axis=1)

    def weigh(rows, to, d0, d1):
        for d in range(d0, d1, 2):
            t = mm(rows, w_ref[:, d * pair_width:(d + 2) * pair_width])
            for i in range(2 * tall):
                piece = t[i * slots:(i + 1) * slots]
                hi, lo = split(jnp.concatenate([piece[:, :pair_width], piece[:, pair_width:]], axis=0))
                rows_at, cols_at = slice(d * slots, (d + 2) * slots), slice(i * pair_width, (i + 1) * pair_width)
                t_hi[to][rows_at, cols_at] = hi
                t_lo[to][rows_at, cols_at] = lo

    def right_ready(zz):
        for far in range(2):
            block = right_buf.at[zz, (x if far == 0 else 1 - x) * 2 + 1 - c]
            arrived(block, rc_send.at[0, 0], rc_recv.at[zz, far])

    def right_rows(zz):
        for d in range(opm):
            for s in range(n_rows):
                spot = (d * n_rows + s) * 4
                rt_ref[spot:spot + 4, :] = right_buf[zz, :, s * opm + d, :]
        hi, lo = split(rt_ref[...].T)
        r_hi[...] = hi
        r_lo[...] = lo

    def update_of(at, i):
        cols_at = slice(i * pair_width, (i + group) * pair_width)
        high = t_hi[at][:, cols_at]
        return mm(r_hi[...], high) + mm(r_lo[...], high) + mm(r_hi[...], t_lo[at][:, cols_at])

    left_pass(z)
    left_wait(z)
    left_pass(ordered(1))
    rows = left_rows(z)
    weigh(rows, 0, 0, opm // 4)
    right_far(z)
    right_pass(ordered(1))
    weigh(rows, 0, opm // 4, opm)

    def outer_plane(p):
        zz, after = ordered(p), ordered(p + 1)
        now, later = p % 2, (p + 1) % 2
        right_ready(zz)
        left_wait(after)
        rows = left_rows(after)
        right_rows(zz)
        share = opm // (2 * tall // group)
        for i in range(0, 2 * tall, group):
            update = update_of(now, i)
            for e in range(group):
                acc_ref[i + e] += update[:, e * pair_width:(e + 1) * pair_width]
            weigh(rows, later, i // group * share, (i // group + 1) * share)
            if i + group == tall:
                if p + 2 < nz:
                    left_pass(ordered(p + 2))
                    right_pass(ordered(p + 2))
                right_far(after)

    for p in range(nz - 1):
        outer_plane(p)

    last = ordered(nz - 1)
    right_ready(last)
    total = jnp.zeros((sub, pair_width), jnp.float32)
    for zz in range(nz):
        for at in range(4):
            total = total + right_buf[zz, at, wide:, :pair_width]
    live_ref[...] = live_ref[...] * (1.0 / (total[0:1, :] + 0.001))
    right_rows(last)
    for i in range(0, 2 * tall, group):
        update = update_of((nz - 1) % 2, i)
        for e in range(group):
            live = mask_ref[me * 2 * tall + i + e].astype(jnp.float32)
            whole = acc_ref[i + e] + update[:, e * pair_width:(e + 1) * pair_width]
            acc_ref[i + e] = pair_ref[i + e] + whole * (live_ref[...] * live)

    for zz in range(nz):
        block = bias_ref.at[zz, x, pl.ds(0, last_chunk)]
        remote(block, block, x_send.at[zz], x_recv.at[zz, 0], place(z, 1 - x, c), y).wait_send()
        pl.when(zz == z)(lambda zz=zz: cross_copy(zz, last_chunk).wait_send())
        pl.when(zz != z)(lambda zz=zz: cross_copy(zz, last_chunk, True).wait_send())
        for up in range(2):
            far = zz <= z if up else zz >= z
            @pl.when(jnp.logical_and(far, reaches(up, 1)))
            def _(up=up, zz=zz):
                relay_copy(up, zz, None).wait_send()
                twin_copy(up, zz).wait_send()

        right_cross(zz).wait_send()
        for far in range(2):
            right_core(zz, far).wait_send()
    for d in range(1, nz):
        right_direct(d).wait_send()
    for d in range(nz):
        for ct in range(2):
            pl.when(jnp.logical_not(is_mine(d, ct)))(lambda d=d, ct=ct: attended_copy(d, ct).wait_send())
    for p in range(per_half):
        pl.when(y * per_half + p != z)(lambda p=p: left_copy(p).wait_send())

    @pl.when(owner)
    def _():
        for zz in range(nz):
            for at in range(len(finals)):
                final_copy(at, zz).wait_send()


def front(n_row, n_y, x, pair, row_mask, residue_mask, gain, wq, wk, wv, wg, wo,
          pair_gain, bias_w, tensor_gain, left_w, right_w, weight):
    n_rows, cols, feat = x.shape
    pair_rows, _, pair_width = pair.shape
    heads = bias_w.shape[1]
    width = feat // heads
    group_heads = heads // n_y // 2
    nz, sub = n_row // 4, 8
    chunks = pair_rows // sub
    keys = n_y * cols
    per_half = nz // n_y
    plane = cols // per_half
    opm = left_w.shape[1]
    wide = n_rows * opm
    f32, b16 = jnp.float32, jnp.bfloat16
    hbm, vmem = pl.BlockSpec(memory_space=pltpu.HBM), pl.BlockSpec(memory_space=pltpu.VMEM)
    dma = pltpu.SemaphoreType.DMA
    labels = 2 * n_y - 1
    return pl.pallas_call(
        front_kernel,
        out_shape=(
            jax.ShapeDtypeStruct(x.shape, f32),
            jax.ShapeDtypeStruct(pair.shape, f32),
        ),
        in_specs=[hbm] * 17,
        out_specs=(vmem, vmem),
        scratch_shapes=[
            pltpu.VMEM(x.shape, f32),
            pltpu.VMEM(pair.shape, f32),
        ]
        + [pltpu.VMEM((feat, feat), f32)] * 5
        + [
            pltpu.VMEM((sub // 2, 2 * sub * heads, 2 * pair_width), b16),
            pltpu.VMEM((chunks, 2 * n_y, group_heads, sub, cols), f32),
            pltpu.VMEM((nz, 2, chunks, 2, n_y, group_heads, sub, cols), f32),
            pltpu.VMEM((n_y, 2, n_rows, cols, feat), f32),
            pltpu.VMEM((2 * n_rows, group_heads, keys, 4 * width), b16),
            pltpu.VMEM((2 * n_rows, group_heads, keys, 4 * width), b16),
            pltpu.VMEM((2 * n_rows, group_heads, keys, 2 * n_rows * group_heads * width), b16),
            pltpu.VMEM((n_y, cols, width), b16),
            pltpu.VMEM((2, n_rows * group_heads, plane, keys), f32),
            pltpu.VMEM((2, n_rows * group_heads, 2 * plane, keys), b16),
            pltpu.VMEM(x.shape, f32),
            pltpu.VMEM((nz, 2, plane, n_rows * group_heads * width), f32),
            pltpu.VMEM((2 * n_y, per_half, plane, n_rows * group_heads * width), f32),
            pltpu.VMEM((nz, 4, wide + sub, cols), f32),
            pltpu.VMEM((4 * per_half, pair_rows // 2, 2 * wide), f32),
            pltpu.VMEM((nz, 4, pair_rows // 2, 2 * wide), f32),
            pltpu.VMEM((nz, 4, pair_rows // 2, 2 * wide), f32),
            pltpu.SMEM(row_mask.shape, jnp.int32),
            pltpu.SMEM(residue_mask.shape, jnp.int32),
            pltpu.VMEM((1, keys), jnp.int32),
            pltpu.VMEM((1, feat), f32),
            pltpu.VMEM((1, pair_width), f32),
            pltpu.VMEM((heads, pair_width), f32),
            pltpu.VMEM((1, feat), f32),
            pltpu.VMEM((opm, feat), f32),
            pltpu.VMEM((opm, feat), f32),
            pltpu.VMEM(weight.shape, f32),
            pltpu.VMEM((3 * opm, opm * pair_width), b16),
            pltpu.VMEM((pair_rows * 4 * n_rows, opm), f32),
            pltpu.VMEM((opm * 4 * n_rows, cols), f32),
            pltpu.VMEM((cols, opm * 4 * n_rows), b16),
            pltpu.VMEM((cols, opm * 4 * n_rows), b16),
            pltpu.VMEM((opm * 4 * n_rows, pair_rows * pair_width), b16),
            pltpu.VMEM((opm * 4 * n_rows, pair_rows * pair_width), b16),
            pltpu.VMEM((opm * 4 * n_rows, pair_rows * pair_width), b16),
            pltpu.VMEM((opm * 4 * n_rows, pair_rows * pair_width), b16),
            pltpu.VMEM((cols, pair_width), f32),
            dma((16,)), dma((chunks,)),
            dma((chunks, labels)), dma((chunks, labels)),
            dma((2 * n_y, n_rows)), dma((2 * n_y, n_rows)),
            dma((2, nz)), dma((nz, chunks)),
            dma((nz,)), dma((nz, chunks)), dma((nz,)), dma((2, nz)), dma((nz,)),
            dma((nz, 2)), dma((2 * n_y, per_half)),
            dma((nz,)), dma((nz,)), dma((nz,)), dma((nz,)),
            dma((nz, 2)), dma((nz, 2)),
            dma((per_half,)), dma((nz,)),
            dma((nz, 4 * n_y - 1)), dma((nz, 4)),
        ],
        compiler_params=pltpu.CompilerParams(
            collective_id=0, has_side_effects=True, vmem_limit_bytes=VMEM_GRANT
        ),
    )(*[
        pltpu.with_memory_space_constraint(a, pltpu.HBM)
        for a in (x, pair, row_mask, residue_mask[None, :], gain[None, :], wq, wk, wv, wg, wo,
                  pair_gain[None, :], bias_w.T, tensor_gain[None, :], left_w.T, right_w.T,
                  weight, residue_mask)
    ])


def fused_body(
    sequence_matrix, pair_representation, alignment_row_mask, residue_mask, attention_scale_vector,
    asking_factor_matrix, lookup_factor_matrix, content_factor_matrix, sigmoid_factor_matrix,
    final_factor_matrix, pair_norm_gain, bias_weight, tensor_scale_vector, first_factor_matrix,
    second_factor_matrix, outer_weight,
):
    return front(
        lax.axis_size("row"), lax.axis_size("head"), sequence_matrix, pair_representation,
        alignment_row_mask, residue_mask, attention_scale_vector, asking_factor_matrix,
        lookup_factor_matrix, content_factor_matrix, sigmoid_factor_matrix, final_factor_matrix,
        pair_norm_gain, bias_weight, tensor_scale_vector, first_factor_matrix, second_factor_matrix,
        outer_weight,
    )


def fits(n_row, n_y, sequence_matrix, pair_representation, bias_weight, first_factor_matrix):
    rows, residues, feat = sequence_matrix.shape
    heads, opm = bias_weight.shape[1], first_factor_matrix.shape[1]
    n_rows, cols, pair_rows, nz = rows // n_row, residues // n_y, residues // n_row, n_row // 4
    if n_row % 4 or nz & (nz - 1) or nz % n_y or heads % (2 * n_y):
        return False
    group_width = heads // n_y // 2 * (feat // heads)
    return (
        n_rows * group_width == 128 and group_width == 64 and 2 * n_rows * opm == 128
        and cols % 128 == 0 and pair_rows % 16 == 0 and pair_representation.shape[2] == 128
        and n_row % 8 == 0
    )


def solution(mesh):
    placed = (P("row", "head", None), P("row", "head", None), P("row")) + (P(),) * 13
    n_row, n_y = mesh.shape["row"], mesh.shape["head"]

    def step(*args):
        chosen = fused_body if fits(n_row, n_y, args[0], args[1], args[11], args[13]) else body
        return jax.shard_map(
            chosen,
            mesh=mesh,
            in_specs=placed,
            out_specs=(P("row", "head", None), P("row", "head", None)),
            check_vma=False,
        )(*args)

    return step
```

```python
import functools
import math

import jax
import jax.numpy as jnp
from jax import lax
from jax.experimental import pallas as pl
from jax.experimental.pallas import tpu as pltpu
from jax.sharding import PartitionSpec as P


HIGH = lax.Precision.HIGHEST
VMEM_GRANT = 40 * 2**20
LOG2E = math.log2(math.e)


def apply_layer_norm(values, gains):
    center = values - jnp.mean(values, axis=-1, keepdims=True)
    spread = jnp.mean(center * center, axis=-1, keepdims=True)
    return center * lax.rsqrt(spread + 1e-05) * gains


def split(x):
    hi = x.astype(jnp.bfloat16)
    lo = (x - hi.astype(jnp.float32)).astype(jnp.bfloat16)
    return hi, lo


def mm(a, b, dims=(((1,), (0,)), ((), ()))):
    return lax.dot_general(a, b, dims, preferred_element_type=jnp.float32)


def split_outside(x):
    hi = lax.reduce_precision(x, 8, 7)
    return hi.astype(jnp.bfloat16), lax.reduce_precision(x - hi, 8, 7).astype(jnp.bfloat16)


NT = (((1,), (1,)), ((), ()))


def bias_kernel(pair_ref, gain_ref, weight_ref, out_ref):
    rows, cols, width = pair_ref.shape
    w_hi, w_lo = split(weight_ref[...])
    heads = w_hi.shape[0]
    w_both = jnp.concatenate([w_hi, w_lo], axis=0)
    for r in range(rows):
        x = apply_layer_norm(pair_ref[r], gain_ref[...])
        x_hi, x_lo = split(x)
        both = mm(w_both, x_hi, NT)
        out_ref[r] = both[:heads] + both[heads:] + mm(w_hi, x_lo, NT)


def pair_bias(pair, gain, weight):
    rows, cols, width = pair.shape
    heads = weight.shape[1]
    step = 4
    return pl.pallas_call(
        bias_kernel,
        grid=(rows // step,),
        in_specs=[
            pl.BlockSpec((step, cols, width), lambda i: (i, 0, 0)),
            pl.BlockSpec((1, width), lambda i: (0, 0)),
            pl.BlockSpec((heads, width), lambda i: (0, 0)),
        ],
        out_specs=pl.BlockSpec((step, heads, cols), lambda i: (i, 0, 0)),
        out_shape=jax.ShapeDtypeStruct((rows, heads, cols), jnp.float32),
        cost_estimate=pl.CostEstimate(flops=10**9, bytes_accessed=5 * 10**6, transcendentals=0),
    )(pair, gain[None, :], weight.T)


def attend_kernel(x_ref, gain_ref, w_ref, bias_ref, key_ref, out_ref, q_ref, k_ref, v_ref):
    blocks, heads, depth, keys = bias_ref.shape
    n_rows = x_ref.shape[0]
    width = v_ref.shape[3] // 2
    local = heads * width
    rows = blocks * depth
    step = pl.program_id(0)

    @pl.when(step == 0)
    def _():
        w_hi, w_lo = split(w_ref[...])
        for s in range(n_rows):
            x_hi, x_lo = split(apply_layer_norm(x_ref[s], gain_ref[...]))
            made = mm(x_hi, w_hi) + mm(x_lo, w_hi) + mm(x_hi, w_lo)
            q_hi, q_lo = split(made[:, :local] * (1.0 / math.sqrt(width)))
            k_hi, k_lo = split(made[:, local:2 * local])
            v_hi, v_lo = split(made[:, 2 * local:])
            for h in range(heads):
                at = slice(h * width, (h + 1) * width)
                q_ref[s, h] = jnp.concatenate([q_hi[:, at], q_hi[:, at], q_lo[:, at]], axis=-1)
                k_ref[s, h] = jnp.concatenate([k_hi[:, at], k_lo[:, at], k_hi[:, at]], axis=-1)
                v_ref[s, h] = jnp.concatenate([v_hi[:, at], v_lo[:, at]], axis=-1)

    key_bias = key_ref[...]
    mine = pl.ds(pl.multiple_of(step * rows, rows), rows)
    for s in range(n_rows):
        pieces = []
        for h in range(heads):
            logits = mm(q_ref[s, h, mine, :], k_ref[s, h], NT)
            logits = logits + bias_ref[:, h].reshape(rows, keys) + key_bias
            largest = jnp.max(logits, axis=-1, keepdims=True)
            e = jnp.exp(logits - largest)
            total = jnp.sum(e, axis=-1, keepdims=True)
            e_hi, e_lo = split(e)
            v = v_ref[s, h]
            both = mm(e_hi, v)
            got = both[:, :width] + both[:, width:] + mm(e_lo, v[:, :width])
            pieces.append(got / total)
        out_ref[s] = jnp.concatenate(pieces, axis=-1)


def attend(x, gain, weight, bias, key_bias):
    n_rows, residues, features = x.shape
    groups, heads, depth, keys = bias.shape
    local = weight.shape[1] // 3
    width = local // heads
    blocks = max(1, 128 // depth)
    rows = blocks * depth
    return pl.pallas_call(
        attend_kernel,
        grid=(groups // blocks,),
        in_specs=[
            pl.BlockSpec(x.shape, lambda i: (0, 0, 0)),
            pl.BlockSpec((1, features), lambda i: (0, 0)),
            pl.BlockSpec(weight.shape, lambda i: (0, 0)),
            pl.BlockSpec((blocks, heads, depth, keys), lambda i: (i, 0, 0, 0)),
            pl.BlockSpec((1, keys), lambda i: (0, 0)),
        ],
        out_specs=pl.BlockSpec((n_rows, rows, local), lambda i: (0, i, 0)),
        out_shape=jax.ShapeDtypeStruct((n_rows, residues, local), jnp.float32),
        scratch_shapes=[
            pltpu.VMEM((n_rows, heads, residues, 3 * width), jnp.bfloat16),
            pltpu.VMEM((n_rows, heads, residues, 3 * width), jnp.bfloat16),
            pltpu.VMEM((n_rows, heads, residues, 2 * width), jnp.bfloat16),
        ],
        cost_estimate=pl.CostEstimate(flops=4 * 10**9, bytes_accessed=6 * 10**6, transcendentals=2 * 10**6),
    )(x, gain[None, :], weight, bias, key_bias)


def outer_kernel(scale_ref, left_ref, weight_ref, right_ref, live_ref, pair_ref, out_ref,
                 r_hi, r_lo, t_hi, t_lo):
    step, cols, depth = pair_ref.shape
    rows_all = r_hi.shape[1]
    n_rows = left_ref.shape[0] // step
    width = rows_all // n_rows
    me = pl.program_id(0)

    @pl.when(me == 0)
    def _():
        hi, lo = split(right_ref[...].T)
        r_hi[...] = hi
        r_lo[...] = lo

    left = left_ref[...]
    group = 2
    for d0 in range(0, width, group):
        t = mm(left, weight_ref[:, d0 * depth:(d0 + group) * depth])
        hi, lo = split(t)
        for g in range(group):
            d = d0 + g
            for i in range(step):
                src = (slice(i * n_rows, (i + 1) * n_rows), slice(g * depth, (g + 1) * depth))
                dst = (slice(d * n_rows, (d + 1) * n_rows), slice(i * depth, (i + 1) * depth))
                t_hi[dst] = hi[src]
                t_lo[dst] = lo[src]
    update = mm(r_hi[...], t_hi[...]) + mm(r_lo[...], t_hi[...]) + mm(r_hi[...], t_lo[...])
    for i in range(step):
        norm = scale_ref[me * step + i] * live_ref[...] + 0.001
        out_ref[i] = pair_ref[i] + update[:, i * depth:(i + 1) * depth] / norm


def outer_mean(scale, left, weight, right, live, pair):
    rows, cols, depth = pair.shape
    total = right.shape[0]
    n_rows = left.shape[0] // rows
    packed = left.shape[1]
    step = 4
    return pl.pallas_call(
        outer_kernel,
        grid=(rows // step,),
        in_specs=[
            pl.BlockSpec(memory_space=pltpu.SMEM),
            pl.BlockSpec((step * n_rows, packed), lambda i: (i, 0)),
            pl.BlockSpec(weight.shape, lambda i: (0, 0)),
            pl.BlockSpec(right.shape, lambda i: (0, 0)),
            pl.BlockSpec((cols, 1), lambda i: (0, 0)),
            pl.BlockSpec((step, cols, depth), lambda i: (i, 0, 0)),
        ],
        out_specs=pl.BlockSpec((step, cols, depth), lambda i: (i, 0, 0)),
        out_shape=jax.ShapeDtypeStruct(pair.shape, jnp.float32),
        scratch_shapes=[
            pltpu.VMEM((cols, total), jnp.bfloat16),
            pltpu.VMEM((cols, total), jnp.bfloat16),
            pltpu.VMEM((total, step * depth), jnp.bfloat16),
            pltpu.VMEM((total, step * depth), jnp.bfloat16),
        ],
        cost_estimate=pl.CostEstimate(flops=9 * 10**9, bytes_accessed=10**7, transcendentals=0),
    )(scale, left, weight, right, live, pair)


def gather_kernel(n, block_ref, out_ref, own_sem, send_sem, recv_sem):
    me = lax.axis_index("row")
    core = me % 2
    x = (me // 2) % 2
    nz = n // 4
    z = me // 4

    def place(zz, xx, cc):
        return (zz * 2 + xx) * 2 + cc

    barrier = pltpu.get_barrier_semaphore()
    up_ok, down_ok = z + 1 < nz, z >= 1

    def greet(target):
        pl.semaphore_signal(barrier, inc=1, device_id={"row": target},
                            device_id_type=pl.DeviceIdType.MESH)

    greet(place(z, x, 1 - core))
    greet(place(z, 1 - x, core))
    pl.when(up_ok)(lambda: greet(place(z + 1, x, core)))
    pl.when(down_ok)(lambda: greet(place(z - 1, x, core)))
    peers = 2 + jnp.where(up_ok, 1, 0) + jnp.where(down_ok, 1, 0)
    pl.semaphore_wait(barrier, peers)

    own = pltpu.make_async_copy(block_ref, out_ref.at[me], own_sem)
    own.start()

    def sends(d, other):
        found = []
        first = core == 0
        if other == 0:
            cross = (z >= 0) if d == 0 else jnp.logical_not(first)
            run = z >= 0
        else:
            cross = None
            run = first
        if d <= 0:
            found.append((jnp.logical_and(run, up_ok), 0, lambda: place(z + 1, x, core)))
        if d >= 0:
            found.append((jnp.logical_and(run, down_ok), 1, lambda: place(z - 1, x, core)))
        if cross is not None:
            found.append((cross, 2, lambda: place(z, 1 - x, core)))
        found.append((z >= 0, 3, lambda: place(z, x, 1 - core)))
        return found

    def copy(source, kind, target, mine):
        return pltpu.make_async_remote_copy(
            src_ref=block_ref if mine else out_ref.at[source],
            dst_ref=out_ref.at[source],
            send_sem=send_sem.at[kind, source],
            recv_sem=recv_sem.at[source],
            device_id={"row": target},
            device_id_type=pl.DeviceIdType.MESH,
        )

    hops = [(0, 0), (0, 1)]
    for far in range(1, nz):
        hops += [(-far, 0), (far, 0), (-far, 1), (far, 1)]

    def each(action):
        for d, other in hops:
            source = place(z + d, (x + other) % 2, core)
            mine = d == 0 and other == 0
            there = jnp.logical_and(z + d >= 0, z + d < nz)

            @pl.when(there)
            def _(d=d, other=other, source=source, mine=mine):
                action(d, other, source, mine)

    def forward(d, other, source, mine):
        if not mine:
            copy(source, 3, place(z, x, 1 - core), False).wait_recv()
        for ok, kind, target in sends(d, other):
            pl.when(ok)(lambda kind=kind, target=target: copy(source, kind, target(), mine).start())

    def finish(d, other, source, mine):
        for ok, kind, target in sends(d, other):
            pl.when(ok)(lambda kind=kind, target=target: copy(source, kind, target(), mine).wait_send())

    each(forward)
    for k in range(n // 2):
        copy(2 * k + 1 - core, 3, place(z, x, 1 - core), False).wait_recv()
    each(finish)
    own.wait()


def gather_rows(block, n, ident):
    return pl.pallas_call(
        functools.partial(gather_kernel, n),
        out_shape=jax.ShapeDtypeStruct((n,) + block.shape, block.dtype),
        in_specs=[pl.BlockSpec(memory_space=pltpu.VMEM)],
        out_specs=pl.BlockSpec(memory_space=pl.ANY),
        scratch_shapes=[
            pltpu.SemaphoreType.DMA,
            pltpu.SemaphoreType.DMA((4, n)),
            pltpu.SemaphoreType.DMA((n,)),
        ],
        compiler_params=pltpu.CompilerParams(collective_id=ident, has_side_effects=True),
    )(block)


def around(n):
    return [[(src, (src + k) % n) for src in range(n)] for k in range(n)]


def gather_heads(block, n, index, axis):
    size = block.shape[axis]
    shape = list(block.shape)
    shape[axis] = size * n
    whole = jnp.zeros(shape, block.dtype)
    for k in range(n):
        part = block if k == 0 else lax.ppermute(block, "head", around(n)[k])
        whole = lax.dynamic_update_slice_in_dim(whole, part, ((index - k) % n) * size, axis)
    return whole


def exchange_heads(block, n, index, split_axis, concat_axis):
    size = block.shape[split_axis] // n
    shape = list(block.shape)
    shape[split_axis] = size
    length = shape[concat_axis]
    shape[concat_axis] = length * n
    whole = jnp.zeros(shape, block.dtype)
    for k in range(n):
        part = lax.dynamic_slice_in_dim(block, ((index + k) % n) * size, size, split_axis)
        if k:
            part = lax.ppermute(part, "head", around(n)[k])
        whole = lax.dynamic_update_slice_in_dim(whole, part, ((index - k) % n) * length, concat_axis)
    return whole


def body(
    sequence_matrix,
    pair_representation,
    alignment_row_mask,
    residue_mask,
    attention_scale_vector,
    asking_factor_matrix,
    lookup_factor_matrix,
    content_factor_matrix,
    sigmoid_factor_matrix,
    final_factor_matrix,
    pair_norm_gain,
    bias_weight,
    tensor_scale_vector,
    first_factor_matrix,
    second_factor_matrix,
    outer_weight,
):
    head_count = lax.axis_size("head")
    head_index = lax.axis_index("head")
    row_index = lax.axis_index("row")
    row_count = lax.axis_size("row")
    n_rows, col_count, width = sequence_matrix.shape
    residues = col_count * head_count
    pair_rows = pair_representation.shape[0]
    pair_depth = pair_representation.shape[2]
    heads_all = bias_weight.shape[1]
    head_width = width // heads_all
    local_heads = heads_all // head_count
    local_width = local_heads * head_width
    opm_width = first_factor_matrix.shape[1]

    sequence_all = gather_heads(sequence_matrix, head_count, head_index, 1)

    bias_all = pair_bias(pair_representation, pair_norm_gain, bias_weight)
    bias_part = exchange_heads(
        bias_all.transpose(1, 0, 2), head_count, head_index, 0, 2
    )
    bias = gather_rows(bias_part, row_count, 0)
    key_bias = ((residue_mask.astype(jnp.float32) - 1.0) * 1000000000.0)[None, :]

    weights = jnp.concatenate(
        [
            lax.dynamic_slice_in_dim(w, head_index * local_width, local_width, 1)
            for w in (asking_factor_matrix, lookup_factor_matrix, content_factor_matrix)
        ],
        axis=1,
    )
    attended = attend(sequence_all, attention_scale_vector, weights, bias, key_bias)
    norm_mine = apply_layer_norm(sequence_matrix, attention_scale_vector)
    gate = jax.nn.sigmoid(
        jnp.einsum("sic,ce->sie", norm_mine, sigmoid_factor_matrix, precision=HIGH)
    )
    returned_values = exchange_heads(attended, head_count, head_index, 1, 2) * gate
    alignment_updated = sequence_matrix + jnp.einsum(
        "jna,ab->jnb", returned_values, final_factor_matrix, precision=HIGH
    )

    outer_product_norm = apply_layer_norm(alignment_updated, tensor_scale_vector)
    live_cols = lax.dynamic_slice_in_dim(residue_mask, head_index * col_count, col_count).astype(
        jnp.float32
    )
    row_live = alignment_row_mask.astype(jnp.float32)
    live = row_live[:, None] * live_cols[None, :]
    left_side = (
        jnp.einsum("sic,co->soi", outer_product_norm, first_factor_matrix, precision=HIGH)
        * live[:, None, :]
    )
    right = (
        jnp.einsum("sic,co->soi", outer_product_norm, second_factor_matrix, precision=HIGH)
        * live[:, None, :]
    )
    left_all = gather_heads(left_side, head_count, head_index, 1)
    carried = jnp.broadcast_to(row_live[:, None, None], (n_rows, 8, col_count))
    sides = gather_rows(jnp.concatenate([left_all, right, carried], axis=1), row_count, 1)
    sides = sides.reshape(row_count * n_rows, -1, col_count)
    left_width = head_count * opm_width
    first_row = row_index * pair_rows
    left_mine = lax.dynamic_slice(
        sides,
        (0, (first_row // col_count) * opm_width, first_row % col_count),
        (row_count * n_rows, opm_width, pair_rows),
    )
    right_all = sides[:, left_width:]
    total_rows = row_count * n_rows
    count = jnp.sum(right_all[:, opm_width, 0])
    right_rows = right_all[:, :opm_width].transpose(1, 0, 2).reshape(
        opm_width * total_rows, col_count
    )
    left_rows = left_mine.transpose(2, 0, 1).reshape(pair_rows * total_rows, opm_width)
    l_hi, l_lo = split_outside(left_rows)
    w_hi, w_lo = split_outside(outer_weight.reshape(opm_width, opm_width * pair_depth))
    rows_live = lax.dynamic_slice_in_dim(residue_mask, row_index * pair_rows, pair_rows).astype(
        jnp.float32
    )
    pair_out = outer_mean(
        count * rows_live,
        jnp.concatenate([l_hi, l_hi, l_lo], axis=1),
        jnp.concatenate([w_hi, w_lo, w_hi], axis=0),
        right_rows,
        live_cols[:, None],
        pair_representation,
    )
    return alignment_updated, pair_out


def ln(values, gains):
    return apply_layer_norm(values, gains)


def front_kernel(
    x_hbm, pair_hbm, row_mask_hbm, key_hbm, gain_hbm, wq_hbm, wk_hbm, wv_hbm, wg_hbm, wo_hbm,
    pair_gain_hbm, bias_hbm, tensor_gain_hbm, left_hbm, right_hbm, weight_hbm, mask_hbm,
    msa_ref, acc_ref,
    x_ref, pair_ref, wq_ref, wk_ref, wv_ref, wg_ref, wo_ref, wpair_ref, group_ref,
    bias_ref, xn_ref, q_ref, k_ref, v_ref, absent_ref, logit_ref, e_ref, gate_ref, att_out, att_in, right_buf, left_loc, left_own,
    left_in, row_mask, mask_ref, key_ref, gain_ref, pair_gain, bias_w, tensor_gain, left_w, right_w,
    weight_ref, w_ref, rows_ref, rt_ref, r_hi, r_lo, t_hi_0, t_hi_1, t_lo_0, t_lo_1, live_ref,
    load_sem, pair_sem, s1_send, s1_recv, n_send, n_recv, z_send, z_recv, x_send, x_recv, xl_send, t_send, t_recv,
    a_send, a_recv, rz_send, rz_recv, rx_send, rx_recv, rc_send, rc_recv,
    l1_send, l1_recv, l2_send, l2_recv,
):
    nz, _, chunks, _, n_y, group_heads, sub, cols = bias_ref.shape
    n_rows, _, feat = x_ref.shape
    heads = bias_w.shape[0]
    keys = n_y * cols
    width = k_ref.shape[3] // 4
    group_width = group_heads * width
    local_width = 2 * group_width
    per_half = nz // n_y
    plane = cols // per_half
    pair_width = pair_ref.shape[2]
    opm = left_w.shape[0]

    me, y = lax.axis_index("row"), lax.axis_index("head")
    c, x, z = me % 2, (me // 2) % 2, me // 4
    half = z // per_half

    def place(zz, xx, cc):
        return (zz * 2 + xx) * 2 + cc

    def across(d):
        out, bit = z, 1
        while bit <= d:
            if d & bit:
                out = out + bit * (1 - 2 * ((out // bit) % 2))
            bit *= 2
        return out

    def plane_at(p):
        if p == 0:
            return z
        late = jnp.where(z < nz // 2, max(p, 2), nz - 1 - max(p, 2))
        return jnp.where((half == y) == (p == 1), late, across(1)) if p < 3 else late

    def remote(src, dst, send, recv, row, head):
        return pltpu.make_async_remote_copy(
            src_ref=src, dst_ref=dst, send_sem=send, recv_sem=recv,
            device_id={"row": row, "head": head}, device_id_type=pl.DeviceIdType.MESH,
        )

    def arrived(dst, send, recv):
        remote(dst, dst, send, recv, place(z, x, 1 - c), y).wait_recv()

    pending = []

    def go(copy):
        copy.start()
        pending.append(copy)

    loads = {}
    for at, (src, dst) in enumerate(
        [(x_hbm, x_ref), (wq_hbm, wq_ref), (wk_hbm, wk_ref), (wv_hbm, wv_ref), (wg_hbm, wg_ref), (wo_hbm, wo_ref),
         (weight_hbm, weight_ref), (pair_gain_hbm, pair_gain), (bias_hbm, bias_w), (gain_hbm, gain_ref),
         (key_hbm, key_ref), (row_mask_hbm, row_mask), (mask_hbm, mask_ref), (tensor_gain_hbm, tensor_gain),
         (left_hbm, left_w), (right_hbm, right_w)]
    ):
        loads[at] = pltpu.make_async_copy(src, dst, load_sem.at[at])
    pair_loads = [
        pltpu.make_async_copy(
            pair_hbm.at[pl.ds(k * sub, sub)], pair_ref.at[pl.ds(k * sub, sub)], pair_sem.at[k]
        )
        for k in range(chunks)
    ]
    for at in (7, 8):
        loads[at].start()
    for copy in pair_loads:
        copy.start()
    for at in [0, 9, 10] + list(range(1, 7)) + list(range(11, 16)):
        loads[at].start()

    barrier = pltpu.get_barrier_semaphore()
    peers = []
    for dx in range(2):
        for dc in range(2):
            for dy in range(n_y):
                if dx or dc or dy:
                    peers.append((place(z, (x + dx) % 2, (c + dc) % 2), (y + dy) % n_y))
    for d in range(1, nz):
        peers.append((place(across(d), x, c), y))
    for row, head in peers:
        pl.semaphore_signal(barrier, inc=1, device_id={"row": row, "head": head},
                            device_id_type=pl.DeviceIdType.MESH)

    for at in (7, 8):
        loads[at].wait()
    w_hi, w_lo = split(bias_w[...] * LOG2E)
    spread = sub * heads
    at_row = lax.broadcasted_iota(jnp.int32, (heads, sub, pair_width), 1).reshape(spread, pair_width)
    zero = jnp.zeros((spread, pair_width), jnp.float32)

    def rows_of(part):
        part = part.astype(jnp.float32)
        return jnp.broadcast_to(part[:, None, :], (heads, sub, pair_width)).reshape(spread, pair_width)

    rep_hi, rep_lo = rows_of(w_hi), rows_of(w_lo)
    for t in range(sub // 2):
        first, second = at_row == 2 * t, at_row == 2 * t + 1
        both = [
            jnp.concatenate([jnp.where(first, rep, zero), jnp.where(second, rep, zero)], axis=1)
            for rep in (rep_hi, rep_lo)
        ]
        wpair_ref[t] = jnp.concatenate(both, axis=0).astype(jnp.bfloat16)

    def bias_chunk(k):
        pair_loads[k].wait()
        total = None
        for t in range(sub // 2):
            at = k * sub + 2 * t
            pieces = [split(ln(pair_ref[at + e], pair_gain[...])) for e in range(2)]
            hi = jnp.concatenate([pieces[0][0], pieces[1][0]], axis=1)
            lo = jnp.concatenate([pieces[0][1], pieces[1][1]], axis=1)
            both = mm(wpair_ref[t], hi, NT)
            part = both[:spread] + both[spread:] + mm(wpair_ref[t, :spread], lo, NT)
            total = part if total is None else total + part
        group_ref[k] = total.reshape(2 * n_y, group_heads, sub, cols)
        bias_ref[z, x, k, c, y] = group_ref[k, y * 2 + c]

    labels = [(dy, dc) for dy in range(n_y) for dc in range(2) if dy or dc]

    def stage_one(k):
        for at, (dy, dc) in enumerate(labels):
            ty, tc = (y + dy) % n_y, (c + dc) % 2
            go(remote(group_ref.at[k, ty * 2 + tc], bias_ref.at[z, x, k, c, y],
                      s1_send.at[k, at], s1_recv.at[k, at], place(z, x, tc), ty))

    def stage_two(k):
        for at, (dy, dc) in enumerate(labels):
            sy, sc = (y + n_y - dy) % n_y, (c + dc) % 2
            arrived(bias_ref.at[z, x, k, sc, sy], s1_send.at[k, at], s1_recv.at[k, at])
        own = bias_ref.at[z, x, k]
        for up in range(2):
            pl.when(reaches(up, 1))(lambda up=up: relay_copy(up, z, k).start())
        cross_copy(z, k).start()

    def relay_copy(up, zz, k):
        block = bias_ref.at[zz, x] if k is None else bias_ref.at[zz, x, k]
        return remote(block, block, z_send.at[up, zz], z_recv.at[zz, 0 if k is None else k],
                      place(z + 1 if up else z - 1, x, c), y)

    def reaches(up, j):
        return z + j < nz if up else z >= j

    def source(up, j):
        return (z - j, z >= j) if up else (z + j, z + j < nz)

    def pass_on(j, k):
        for up in range(2):
            zz, there = source(up, j)

            @pl.when(there)
            def _(up=up, zz=zz):
                block = bias_ref.at[zz, x, k]
                arrived(block, z_send.at[0, 0], z_recv.at[zz, k])
                if j < nz - 1:
                    pl.when(reaches(up, 1))(lambda: relay_copy(up, zz, k).start())
                cross_copy(zz, k, True).start()

    def pass_twin(j):
        for up in range(2):
            zz, there = source(up, j)

            @pl.when(there)
            def _(up=up, zz=zz):
                arrived(bias_ref.at[zz, 1 - x, last_chunk, 0], t_send.at[0, 0], t_recv.at[zz])
                if j < nz - 1:
                    pl.when(reaches(up, 1))(lambda: twin_copy(up, zz).start())

    last_chunk = chunks - 1

    def cross_copy(zz, k, beyond=False):
        block = bias_ref.at[zz, x, k, 1] if beyond and k == last_chunk else bias_ref.at[zz, x, k]
        return remote(block, block, (xl_send if k == last_chunk else x_send).at[zz], x_recv.at[zz, k],
                      place(z, 1 - x, c), y)

    def twin_copy(up, zz):
        block = bias_ref.at[zz, 1 - x, last_chunk, 0]
        return remote(block, block, t_send.at[up, zz], t_recv.at[zz], place(z + 1 if up else z - 1, x, c), y)

    def start_twins():
        arrived(bias_ref.at[z, 1 - x, last_chunk], xl_send.at[0], x_recv.at[z, last_chunk])
        for up in range(2):
            pl.when(reaches(up, 1))(lambda up=up: twin_copy(up, z).start())

    bias_chunk(0)
    pl.semaphore_wait(barrier, len(peers))
    stage_one(0)
    for k in range(1, chunks):
        bias_chunk(k)
        stage_one(k)
        if k >= 2:
            stage_two(k - 2)

    for at in (0, 9, 10):
        loads[at].wait()
    for s in range(n_rows):
        xn_ref[y, c, s] = ln(x_ref[s], gain_ref[...])
        own_x = xn_ref.at[y, c, s]
        for dy in range(1, n_y):
            go(remote(own_x, own_x, n_send.at[dy, s], n_recv.at[dy, s], place(z, x, c), (y + dy) % n_y))
        go(remote(own_x, own_x, n_send.at[0, s], n_recv.at[0, s], place(z, x, 1 - c), y))
    stage_two(chunks - 2)

    for at in (1, 2, 3):
        loads[at].wait()
    mine = pl.ds(pl.multiple_of(y * local_width, local_width), local_width)
    picked = []
    for ref in (wq_ref, wk_ref, wv_ref):
        whole = ref[:, mine]
        picked.append(jnp.where(c == 0, whole[:, :group_width], whole[:, group_width:]))
    wa_hi, wa_lo = split(jnp.concatenate(picked, axis=1))

    lane = lax.broadcasted_iota(jnp.int32, (cols, width), 1)
    pick = jnp.where(lane < 2, 1.0, 0.0).astype(jnp.bfloat16)
    one, none = jnp.ones((cols, width), jnp.bfloat16), jnp.zeros((cols, width), jnp.bfloat16)
    for yy in range(n_y):
        keep = jnp.broadcast_to(
            key_ref[:, yy * cols:(yy + 1) * cols].astype(jnp.float32), (pair_width, cols)
        ).T[:, :width]
        hi, lo = split((keep - 1.0) * (1000000000.0 * LOG2E))
        absent_ref[yy] = jnp.where(
            lane == 0, hi.astype(jnp.float32), jnp.where(lane == 1, lo.astype(jnp.float32), 0.0)
        ).astype(jnp.bfloat16)

    def project(yy, cc, rows=range(n_rows)):
        spot = pl.ds(pl.multiple_of(yy * cols, cols), cols)
        absent = absent_ref[yy]
        for s in rows:
            hi, lo = split(xn_ref[yy, cc, s])
            made = mm(hi, wa_hi) + mm(lo, wa_hi) + mm(hi, wa_lo)
            q_hi, q_lo = split(made[:, :group_width] * (LOG2E / math.sqrt(width)))
            k_hi, k_lo = split(made[:, group_width:2 * group_width])
            v_hi, v_lo = split(made[:, 2 * group_width:])
            for h in range(group_heads):
                at = slice(h * width, (h + 1) * width)
                to = cc * n_rows + s
                q_ref[to, h, spot, :] = jnp.concatenate([q_hi[:, at], q_hi[:, at], q_lo[:, at], pick], axis=-1)
                k_ref[to, h, spot, :] = jnp.concatenate([k_hi[:, at], k_lo[:, at], k_hi[:, at], absent], axis=-1)
                mine_at, count_at = s * group_heads + h, (s * group_heads + h + 1) % (n_rows * group_heads)
                parts = [none] * (2 * n_rows * group_heads)
                parts[mine_at], parts[count_at], parts[n_rows * group_heads + mine_at] = v_hi[:, at], one, v_lo[:, at]
                v_ref[to, h, spot, :] = jnp.concatenate(parts, axis=-1)

    project(y, c)
    stage_two(chunks - 1)

    def gate_rows(s):
        hi, lo = split(xn_ref[y, c, s])
        gate_ref[s] = jax.nn.sigmoid(mm(hi, g_hi) + mm(lo, g_hi) + mm(hi, g_lo))

    def own_rows(s):
        arrived(xn_ref.at[y, 1 - c, s], n_send.at[0, s], n_recv.at[0, s])
        project(y, 1 - c, [s])

    def spread_weight(d0, d1):
        for d in range(d0, d1):
            hi, lo = split(weight_ref[pl.ds(d, opm, stride=opm), :])
            w_ref[:, d * pair_width:(d + 1) * pair_width] = jnp.concatenate([hi, lo, hi], axis=0)

    def clear(i0, i1):
        acc_ref[i0:i1] = jnp.zeros((i1 - i0, cols, pair_width), jnp.float32)

    loads[4].wait()
    g_hi, g_lo = split(wg_ref[...])
    loads[6].wait()
    pair_rows = pair_ref.shape[0]
    fillers = [functools.partial(gate_rows, s) for s in range(n_rows)]
    fillers += [functools.partial(own_rows, s) for s in range(n_rows)]
    quarter = opm // 4
    fillers += [functools.partial(spread_weight, i * quarter, (i + 1) * quarter) for i in range(4)]
    part = pair_rows // 4
    fillers += [functools.partial(clear, i * part, (i + 1) * part) for i in range(4)]
    tasks = [functools.partial(pass_on, j, k) for j in range(1, nz) for k in range(chunks)]
    for j in range(nz - 1, 0, -1):
        tasks.insert(min(chunks * (j + 1) - 1, len(tasks)), functools.partial(pass_twin, j))
    tasks.insert(chunks, start_twins)

    def advance(n_tasks, n_fillers):
        for _ in range(n_tasks):
            if tasks:
                tasks.pop(0)()
            if n_fillers and fillers:
                fillers.pop(0)()

    advance(chunks + 3, chunks + 3)
    while fillers:
        fillers.pop(0)()
    for dy in range(1, n_y):
        sy = (y + n_y - dy) % n_y
        for s in range(n_rows):
            block = xn_ref.at[sy, c, s]
            arrived(block, n_send.at[dy, s], n_recv.at[dy, s])
            go(remote(block, block, n_send.at[n_y + dy, s], n_recv.at[n_y + dy, s], place(z, x, 1 - c), y))
            advance(2 if s + 1 < n_rows else 1, 0)
            project(sy, c, [s])
            advance(1 if s + 1 < n_rows else 0, 0)
    for dy in range(1, n_y):
        sy = (y + n_y - dy) % n_y
        for s in range(n_rows):
            arrived(xn_ref.at[sy, 1 - c, s], n_send.at[n_y + dy, s], n_recv.at[n_y + dy, s])
            project(sy, 1 - c, [s])
    advance(max(0, len(tasks) - 4), 0)
    for copy in pending:
        copy.wait_send()
    pending.clear()

    own = pl.ds(pl.multiple_of(y * cols, cols), cols)
    live_ref[...] = jnp.broadcast_to(key_ref[:, own].astype(jnp.float32), (pair_width, cols)).T

    lanes = n_rows * group_width
    block = lax.broadcasted_iota(jnp.int32, (plane, lanes), 1) // width

    def attended_copy(d, ct):
        zz = plane_at(d)
        return remote(att_out.at[d, ct], att_in.at[y * 2 + c, zz % per_half],
                      a_send.at[d, ct], a_recv.at[y * 2 + c, zz % per_half],
                      place(z, x, ct), zz // per_half)

    def is_mine(d, ct):
        return jnp.logical_and(plane_at(d) // per_half == y, ct == c)

    def attend_plane(d):
        zz = plane_at(d)
        for k in range(last_chunk):
            arrived(bias_ref.at[zz, 1 - x, k], x_send.at[0], x_recv.at[zz, k])
        if d:
            arrived(bias_ref.at[zz, 1 - x, last_chunk, 1], xl_send.at[0], x_recv.at[zz, last_chunk])
        queries = pl.ds(pl.multiple_of(zz * plane, plane), plane)

        tiles = [
            jnp.concatenate(
                [
                    jnp.concatenate(
                        [bias_ref[zz, xx, :, cc, yy, h].reshape(chunks * sub, cols) for yy in range(n_y)],
                        axis=1,
                    )
                    for xx in range(2)
                    for cc in range(2)
                ],
                axis=0,
            )
            for h in range(group_heads)
        ]
        units = [(s, h) for s in range(n_rows) for h in range(group_heads)]

        def compare(ct):
            for at, (s, h) in enumerate(units):
                row = ct * n_rows + s
                logit_ref[ct, at] = mm(q_ref[row, h, queries, :], k_ref[row, h], NT) + tiles[h]

        def soften(ct):
            for at in range(len(units)):
                logits = logit_ref[ct, at]
                e_hi, e_lo = split(jnp.exp2(logits - jnp.max(logits, axis=-1, keepdims=True)))
                e_ref[ct, at, :plane] = e_hi
                e_ref[ct, at, plane:] = e_lo

        def gather(ct):
            upper = lower = None
            for at, (s, h) in enumerate(units):
                row = ct * n_rows + s
                both = mm(e_ref[ct, at, :plane], v_ref[row, h])
                whole = both[:, :lanes] + both[:, lanes:] + mm(e_ref[ct, at, plane:], v_ref[row, h, :, :lanes])
                upper = whole if upper is None else jnp.where(block == at, whole, upper)
                lower = whole if lower is None else jnp.where(block == (at + 1) % len(units), whole, lower)
            return upper / pltpu.roll(lower, lanes - width, 1)

        def hand_over(ct):
            @pl.when(is_mine(d, ct))
            def _():
                att_in[y * 2 + c, zz % per_half] = att_out[d, ct]

            pl.when(jnp.logical_not(is_mine(d, ct)))(lambda: attended_copy(d, ct).start())

        compare(0)
        soften(0)
        compare(1)
        att_out[d, 0] = gather(0)
        if d + 1 == nz:
            hand_over(0)
        soften(1)
        att_out[d, 1] = gather(1)
        if d + 1 < nz:
            hand_over(0)
        hand_over(1)

    for d in range(nz):
        attend_plane(d)
        advance(2 if d + 2 < nz else len(tasks), 0)

    for at in (5,) + tuple(range(11, 16)):
        loads[at].wait()
    o_hi, o_lo = split(wo_ref[...])
    wide = n_rows * opm
    left_hi, left_lo = split(left_w[...])
    left_both = jnp.concatenate([left_hi, left_lo], axis=0)
    right_hi, right_lo = split(right_w[...])
    right_both = jnp.concatenate([right_hi, right_lo], axis=0)
    tall = pair_rows // 2

    def left_copy(p):
        return remote(left_loc.at[pl.ds(p * 4, 4)], left_own.at[z], l1_send.at[p], l1_recv.at[z],
                      place(y * per_half + p, x, c), y)

    def finish(p):
        for dy, dc in labels:
            sy, sc = (y + n_y - dy) % n_y, (c + dc) % 2
            arrived(att_in.at[sy * 2 + sc, p], a_send.at[0, 0], a_recv.at[sy * 2 + sc, p])
        part = slice(p * plane, (p + 1) * plane)
        lefts = []
        count = jnp.zeros((sub, plane), jnp.float32)
        for s in range(n_rows):
            at = slice(s * group_width, (s + 1) * group_width)
            whole = jnp.concatenate([att_in[g, p][:, at] for g in range(2 * n_y)], axis=1) * gate_ref[s, part]
            hi, lo = split(whole)
            out = x_ref[s, part] + (mm(hi, o_hi) + mm(lo, o_hi) + mm(hi, o_lo))
            msa_ref[s, part] = out
            f_hi, f_lo = split(ln(out, tensor_gain[...]))
            live = row_mask[s].astype(jnp.float32)
            both = mm(right_both, f_hi, NT)
            right_buf[z, x * 2 + c, s * opm:(s + 1) * opm, part] = (
                both[:opm] + both[opm:] + mm(right_hi, f_lo, NT)
            ) * live
            both = mm(f_hi, left_both, NT)
            lefts.append((both[:, :opm] + both[:, opm:] + mm(f_lo, left_hi, NT)) * live)
            count = count + live
        right_buf[z, x * 2 + c, wide:, part] = count
        left = jnp.concatenate(lefts, axis=1).reshape(4, 2, tall, wide)
        left_loc[p * 4:(p + 1) * 4] = jnp.concatenate([left[:, 0], left[:, 1]], axis=2)
        here = y * per_half + p == z

        @pl.when(here)
        def _():
            left_own[z] = left_loc[p * 4:(p + 1) * 4]

        pl.when(jnp.logical_not(here))(lambda: left_copy(p).start())

    for p in range(per_half):
        finish(p)

    def right_core(zz, far):
        block = right_buf.at[zz, (x if far == 0 else 1 - x) * 2 + c]
        return remote(block, block, rc_send.at[zz, far], rc_recv.at[zz, far], place(z, x, 1 - c), y)

    def right_direct(d):
        block = right_buf.at[z, x * 2 + c]
        return remote(block, block, rz_send.at[d], rz_recv.at[z], place(across(d), x, c), y)

    def right_cross(zz):
        block = right_buf.at[zz, x * 2 + c]
        return remote(block, block, rx_send.at[zz], rx_recv.at[zz], place(z, 1 - x, c), y)

    right_cross(z).start()
    right_core(z, 0).start()
    for d in range(1, nz):
        right_direct(d).start()

    owner = half == y
    finals = [(dx, dc, dy) for dx in range(2) for dc in range(2) for dy in range(n_y) if dx or dc or dy]

    def final_copy(at, zz):
        dx, dc, dy = finals[at]
        tx, tc, ty = (x + dx) % 2, (c + dc) % 2, (y + dy) % n_y
        return remote(left_own.at[zz, tx * 2 + tc], left_in.at[zz, x * 2 + c], l2_send.at[zz, at],
                      l2_recv.at[zz, x * 2 + c], place(z, tx, tc), ty)

    def left_pass(zz):
        @pl.when(owner)
        def _():
            pl.when(zz != z)(lambda: arrived(left_own.at[zz], l1_send.at[0], l1_recv.at[zz]))
            for at in range(len(finals)):
                final_copy(at, zz).start()
            left_in[zz, x * 2 + c] = left_own[zz, x * 2 + c]

    def left_wait(zz):
        for xx in range(2):
            for cc in range(2):
                mine_too = jnp.logical_and(owner, jnp.logical_and(xx == x, cc == c))

                @pl.when(jnp.logical_not(mine_too))
                def _(xx=xx, cc=cc):
                    arrived(left_in.at[zz, xx * 2 + cc], l2_send.at[0, 0], l2_recv.at[zz, xx * 2 + cc])

    def right_pass(zz):
        arrived(right_buf.at[zz, x * 2 + c], rz_send.at[0], rz_recv.at[zz])
        right_cross(zz).start()
        right_core(zz, 0).start()

    def right_far(zz):
        arrived(right_buf.at[zz, (1 - x) * 2 + c], rx_send.at[0], rx_recv.at[zz])
        right_core(zz, 1).start()

    def ordered(p):
        late = jnp.where(z < nz // 2, p, nz - 1 - p)
        return jnp.where(p == 0, z, jnp.where(p == 1, across(1), late))

    t_hi, t_lo = (t_hi_0, t_hi_1), (t_lo_0, t_lo_1)
    slots = 4 * n_rows
    group = 4

    def left_rows(zz):
        for i in range(2 * tall):
            block = left_in[zz, :, i % tall, :]
            base = (i // tall) * wide
            rows_ref[i * slots:(i + 1) * slots, :] = jnp.concatenate(
                [block[:, base + s * opm:base + (s + 1) * opm] for s in range(n_rows)], axis=0
            )
        hi, lo = split(rows_ref[...])
        return jnp.concatenate([hi, hi, lo], axis=1)

    def weigh(rows, to, d0, d1):
        for d in range(d0, d1, 2):
            t = mm(rows, w_ref[:, d * pair_width:(d + 2) * pair_width])
            for i in range(2 * tall):
                piece = t[i * slots:(i + 1) * slots]
                hi, lo = split(jnp.concatenate([piece[:, :pair_width], piece[:, pair_width:]], axis=0))
                rows_at, cols_at = slice(d * slots, (d + 2) * slots), slice(i * pair_width, (i + 1) * pair_width)
                t_hi[to][rows_at, cols_at] = hi
                t_lo[to][rows_at, cols_at] = lo

    def right_ready(zz):
        for far in range(2):
            block = right_buf.at[zz, (x if far == 0 else 1 - x) * 2 + 1 - c]
            arrived(block, rc_send.at[0, 0], rc_recv.at[zz, far])

    def right_rows(zz):
        for d in range(opm):
            for s in range(n_rows):
                spot = (d * n_rows + s) * 4
                rt_ref[spot:spot + 4, :] = right_buf[zz, :, s * opm + d, :]
        hi, lo = split(rt_ref[...].T)
        r_hi[...] = hi
        r_lo[...] = lo

    def update_of(at, i):
        cols_at = slice(i * pair_width, (i + group) * pair_width)
        high = t_hi[at][:, cols_at]
        return mm(r_hi[...], high) + mm(r_lo[...], high) + mm(r_hi[...], t_lo[at][:, cols_at])

    left_pass(z)
    left_wait(z)
    left_pass(ordered(1))
    rows = left_rows(z)
    weigh(rows, 0, 0, opm // 4)
    right_far(z)
    right_pass(ordered(1))
    weigh(rows, 0, opm // 4, opm)

    def outer_plane(p):
        zz, after = ordered(p), ordered(p + 1)
        now, later = p % 2, (p + 1) % 2
        right_ready(zz)
        left_wait(after)
        rows = left_rows(after)
        right_rows(zz)
        share = opm // (2 * tall // group)
        for i in range(0, 2 * tall, group):
            update = update_of(now, i)
            for e in range(group):
                acc_ref[i + e] += update[:, e * pair_width:(e + 1) * pair_width]
            weigh(rows, later, i // group * share, (i // group + 1) * share)
            if i + group == tall:
                for q in range(2, nz if p == 0 else 0):
                    left_pass(ordered(q))
                if p + 2 < nz:
                    right_pass(ordered(p + 2))
                right_far(after)

    for p in range(nz - 1):
        outer_plane(p)

    last = ordered(nz - 1)
    right_ready(last)
    total = jnp.zeros((sub, pair_width), jnp.float32)
    for zz in range(nz):
        for at in range(4):
            total = total + right_buf[zz, at, wide:, :pair_width]
    live_ref[...] = live_ref[...] * (1.0 / (total[0:1, :] + 0.001))
    right_rows(last)
    for i in range(0, 2 * tall, group):
        update = update_of((nz - 1) % 2, i)
        for e in range(group):
            live = mask_ref[me * 2 * tall + i + e].astype(jnp.float32)
            whole = acc_ref[i + e] + update[:, e * pair_width:(e + 1) * pair_width]
            acc_ref[i + e] = pair_ref[i + e] + whole * (live_ref[...] * live)

    for zz in range(nz):
        block = bias_ref.at[zz, x, pl.ds(0, last_chunk)]
        remote(block, block, x_send.at[zz], x_recv.at[zz, 0], place(z, 1 - x, c), y).wait_send()
        pl.when(zz == z)(lambda zz=zz: cross_copy(zz, last_chunk).wait_send())
        pl.when(zz != z)(lambda zz=zz: cross_copy(zz, last_chunk, True).wait_send())
        for up in range(2):
            far = zz <= z if up else zz >= z
            @pl.when(jnp.logical_and(far, reaches(up, 1)))
            def _(up=up, zz=zz):
                relay_copy(up, zz, None).wait_send()
                twin_copy(up, zz).wait_send()

        right_cross(zz).wait_send()
        for far in range(2):
            right_core(zz, far).wait_send()
    for d in range(1, nz):
        right_direct(d).wait_send()
    for d in range(nz):
        for ct in range(2):
            pl.when(jnp.logical_not(is_mine(d, ct)))(lambda d=d, ct=ct: attended_copy(d, ct).wait_send())
    for p in range(per_half):
        pl.when(y * per_half + p != z)(lambda p=p: left_copy(p).wait_send())

    @pl.when(owner)
    def _():
        for zz in range(nz):
            for at in range(len(finals)):
                final_copy(at, zz).wait_send()


def front(n_row, n_y, x, pair, row_mask, residue_mask, gain, wq, wk, wv, wg, wo,
          pair_gain, bias_w, tensor_gain, left_w, right_w, weight):
    n_rows, cols, feat = x.shape
    pair_rows, _, pair_width = pair.shape
    heads = bias_w.shape[1]
    width = feat // heads
    group_heads = heads // n_y // 2
    nz, sub = n_row // 4, 8
    chunks = pair_rows // sub
    keys = n_y * cols
    per_half = nz // n_y
    plane = cols // per_half
    opm = left_w.shape[1]
    wide = n_rows * opm
    f32, b16 = jnp.float32, jnp.bfloat16
    hbm, vmem = pl.BlockSpec(memory_space=pltpu.HBM), pl.BlockSpec(memory_space=pltpu.VMEM)
    dma = pltpu.SemaphoreType.DMA
    labels = 2 * n_y - 1
    return pl.pallas_call(
        front_kernel,
        out_shape=(
            jax.ShapeDtypeStruct(x.shape, f32),
            jax.ShapeDtypeStruct(pair.shape, f32),
        ),
        in_specs=[hbm] * 17,
        out_specs=(vmem, vmem),
        scratch_shapes=[
            pltpu.VMEM(x.shape, f32),
            pltpu.VMEM(pair.shape, f32),
        ]
        + [pltpu.VMEM((feat, feat), f32)] * 5
        + [
            pltpu.VMEM((sub // 2, 2 * sub * heads, 2 * pair_width), b16),
            pltpu.VMEM((chunks, 2 * n_y, group_heads, sub, cols), f32),
            pltpu.VMEM((nz, 2, chunks, 2, n_y, group_heads, sub, cols), f32),
            pltpu.VMEM((n_y, 2, n_rows, cols, feat), f32),
            pltpu.VMEM((2 * n_rows, group_heads, keys, 4 * width), b16),
            pltpu.VMEM((2 * n_rows, group_heads, keys, 4 * width), b16),
            pltpu.VMEM((2 * n_rows, group_heads, keys, 2 * n_rows * group_heads * width), b16),
            pltpu.VMEM((n_y, cols, width), b16),
            pltpu.VMEM((2, n_rows * group_heads, plane, keys), f32),
            pltpu.VMEM((2, n_rows * group_heads, 2 * plane, keys), b16),
            pltpu.VMEM(x.shape, f32),
            pltpu.VMEM((nz, 2, plane, n_rows * group_heads * width), f32),
            pltpu.VMEM((2 * n_y, per_half, plane, n_rows * group_heads * width), f32),
            pltpu.VMEM((nz, 4, wide + sub, cols), f32),
            pltpu.VMEM((4 * per_half, pair_rows // 2, 2 * wide), f32),
            pltpu.VMEM((nz, 4, pair_rows // 2, 2 * wide), f32),
            pltpu.VMEM((nz, 4, pair_rows // 2, 2 * wide), f32),
            pltpu.SMEM(row_mask.shape, jnp.int32),
            pltpu.SMEM(residue_mask.shape, jnp.int32),
            pltpu.VMEM((1, keys), jnp.int32),
            pltpu.VMEM((1, feat), f32),
            pltpu.VMEM((1, pair_width), f32),
            pltpu.VMEM((heads, pair_width), f32),
            pltpu.VMEM((1, feat), f32),
            pltpu.VMEM((opm, feat), f32),
            pltpu.VMEM((opm, feat), f32),
            pltpu.VMEM(weight.shape, f32),
            pltpu.VMEM((3 * opm, opm * pair_width), b16),
            pltpu.VMEM((pair_rows * 4 * n_rows, opm), f32),
            pltpu.VMEM((opm * 4 * n_rows, cols), f32),
            pltpu.VMEM((cols, opm * 4 * n_rows), b16),
            pltpu.VMEM((cols, opm * 4 * n_rows), b16),
            pltpu.VMEM((opm * 4 * n_rows, pair_rows * pair_width), b16),
            pltpu.VMEM((opm * 4 * n_rows, pair_rows * pair_width), b16),
            pltpu.VMEM((opm * 4 * n_rows, pair_rows * pair_width), b16),
            pltpu.VMEM((opm * 4 * n_rows, pair_rows * pair_width), b16),
            pltpu.VMEM((cols, pair_width), f32),
            dma((16,)), dma((chunks,)),
            dma((chunks, labels)), dma((chunks, labels)),
            dma((2 * n_y, n_rows)), dma((2 * n_y, n_rows)),
            dma((2, nz)), dma((nz, chunks)),
            dma((nz,)), dma((nz, chunks)), dma((nz,)), dma((2, nz)), dma((nz,)),
            dma((nz, 2)), dma((2 * n_y, per_half)),
            dma((nz,)), dma((nz,)), dma((nz,)), dma((nz,)),
            dma((nz, 2)), dma((nz, 2)),
            dma((per_half,)), dma((nz,)),
            dma((nz, 4 * n_y - 1)), dma((nz, 4)),
        ],
        compiler_params=pltpu.CompilerParams(
            collective_id=0, has_side_effects=True, vmem_limit_bytes=VMEM_GRANT
        ),
    )(*[
        pltpu.with_memory_space_constraint(a, pltpu.HBM)
        for a in (x, pair, row_mask, residue_mask[None, :], gain[None, :], wq, wk, wv, wg, wo,
                  pair_gain[None, :], bias_w.T, tensor_gain[None, :], left_w.T, right_w.T,
                  weight, residue_mask)
    ])


def fused_body(
    sequence_matrix, pair_representation, alignment_row_mask, residue_mask, attention_scale_vector,
    asking_factor_matrix, lookup_factor_matrix, content_factor_matrix, sigmoid_factor_matrix,
    final_factor_matrix, pair_norm_gain, bias_weight, tensor_scale_vector, first_factor_matrix,
    second_factor_matrix, outer_weight,
):
    return front(
        lax.axis_size("row"), lax.axis_size("head"), sequence_matrix, pair_representation,
        alignment_row_mask, residue_mask, attention_scale_vector, asking_factor_matrix,
        lookup_factor_matrix, content_factor_matrix, sigmoid_factor_matrix, final_factor_matrix,
        pair_norm_gain, bias_weight, tensor_scale_vector, first_factor_matrix, second_factor_matrix,
        outer_weight,
    )


def fits(n_row, n_y, sequence_matrix, pair_representation, bias_weight, first_factor_matrix):
    rows, residues, feat = sequence_matrix.shape
    heads, opm = bias_weight.shape[1], first_factor_matrix.shape[1]
    n_rows, cols, pair_rows, nz = rows // n_row, residues // n_y, residues // n_row, n_row // 4
    if n_row % 4 or nz & (nz - 1) or nz % n_y or heads % (2 * n_y):
        return False
    group_width = heads // n_y // 2 * (feat // heads)
    return (
        n_rows * group_width == 128 and group_width == 64 and 2 * n_rows * opm == 128
        and cols % 128 == 0 and pair_rows % 16 == 0 and pair_representation.shape[2] == 128
        and n_row % 8 == 0
    )


def solution(mesh):
    placed = (P("row", "head", None), P("row", "head", None), P("row")) + (P(),) * 13
    n_row, n_y = mesh.shape["row"], mesh.shape["head"]

    def step(*args):
        chosen = fused_body if fits(n_row, n_y, args[0], args[1], args[11], args[13]) else body
        return jax.shard_map(
            chosen,
            mesh=mesh,
            in_specs=placed,
            out_specs=(P("row", "head", None), P("row", "head", None)),
            check_vma=False,
        )(*args)

    return step
```

```python
import functools
import math

import jax
import jax.numpy as jnp
from jax import lax
from jax.experimental import pallas as pl
from jax.experimental.pallas import tpu as pltpu
from jax.sharding import PartitionSpec as P


HIGH = lax.Precision.HIGHEST
VMEM_GRANT = 40 * 2**20
LOG2E = math.log2(math.e)


def apply_layer_norm(values, gains):
    center = values - jnp.mean(values, axis=-1, keepdims=True)
    spread = jnp.mean(center * center, axis=-1, keepdims=True)
    return center * lax.rsqrt(spread + 1e-05) * gains


def split(x):
    hi = x.astype(jnp.bfloat16)
    lo = (x - hi.astype(jnp.float32)).astype(jnp.bfloat16)
    return hi, lo


def mm(a, b, dims=(((1,), (0,)), ((), ()))):
    return lax.dot_general(a, b, dims, preferred_element_type=jnp.float32)


def split_outside(x):
    hi = lax.reduce_precision(x, 8, 7)
    return hi.astype(jnp.bfloat16), lax.reduce_precision(x - hi, 8, 7).astype(jnp.bfloat16)


NT = (((1,), (1,)), ((), ()))


def bias_kernel(pair_ref, gain_ref, weight_ref, out_ref):
    rows, cols, width = pair_ref.shape
    w_hi, w_lo = split(weight_ref[...])
    heads = w_hi.shape[0]
    w_both = jnp.concatenate([w_hi, w_lo], axis=0)
    for r in range(rows):
        x = apply_layer_norm(pair_ref[r], gain_ref[...])
        x_hi, x_lo = split(x)
        both = mm(w_both, x_hi, NT)
        out_ref[r] = both[:heads] + both[heads:] + mm(w_hi, x_lo, NT)


def pair_bias(pair, gain, weight):
    rows, cols, width = pair.shape
    heads = weight.shape[1]
    step = 4
    return pl.pallas_call(
        bias_kernel,
        grid=(rows // step,),
        in_specs=[
            pl.BlockSpec((step, cols, width), lambda i: (i, 0, 0)),
            pl.BlockSpec((1, width), lambda i: (0, 0)),
            pl.BlockSpec((heads, width), lambda i: (0, 0)),
        ],
        out_specs=pl.BlockSpec((step, heads, cols), lambda i: (i, 0, 0)),
        out_shape=jax.ShapeDtypeStruct((rows, heads, cols), jnp.float32),
        cost_estimate=pl.CostEstimate(flops=10**9, bytes_accessed=5 * 10**6, transcendentals=0),
    )(pair, gain[None, :], weight.T)


def attend_kernel(x_ref, gain_ref, w_ref, bias_ref, key_ref, out_ref, q_ref, k_ref, v_ref):
    blocks, heads, depth, keys = bias_ref.shape
    n_rows = x_ref.shape[0]
    width = v_ref.shape[3] // 2
    local = heads * width
    rows = blocks * depth
    step = pl.program_id(0)

    @pl.when(step == 0)
    def _():
        w_hi, w_lo = split(w_ref[...])
        for s in range(n_rows):
            x_hi, x_lo = split(apply_layer_norm(x_ref[s], gain_ref[...]))
            made = mm(x_hi, w_hi) + mm(x_lo, w_hi) + mm(x_hi, w_lo)
            q_hi, q_lo = split(made[:, :local] * (1.0 / math.sqrt(width)))
            k_hi, k_lo = split(made[:, local:2 * local])
            v_hi, v_lo = split(made[:, 2 * local:])
            for h in range(heads):
                at = slice(h * width, (h + 1) * width)
                q_ref[s, h] = jnp.concatenate([q_hi[:, at], q_hi[:, at], q_lo[:, at]], axis=-1)
                k_ref[s, h] = jnp.concatenate([k_hi[:, at], k_lo[:, at], k_hi[:, at]], axis=-1)
                v_ref[s, h] = jnp.concatenate([v_hi[:, at], v_lo[:, at]], axis=-1)

    key_bias = key_ref[...]
    mine = pl.ds(pl.multiple_of(step * rows, rows), rows)
    for s in range(n_rows):
        pieces = []
        for h in range(heads):
            logits = mm(q_ref[s, h, mine, :], k_ref[s, h], NT)
            logits = logits + bias_ref[:, h].reshape(rows, keys) + key_bias
            largest = jnp.max(logits, axis=-1, keepdims=True)
            e = jnp.exp(logits - largest)
            total = jnp.sum(e, axis=-1, keepdims=True)
            e_hi, e_lo = split(e)
            v = v_ref[s, h]
            both = mm(e_hi, v)
            got = both[:, :width] + both[:, width:] + mm(e_lo, v[:, :width])
            pieces.append(got / total)
        out_ref[s] = jnp.concatenate(pieces, axis=-1)


def attend(x, gain, weight, bias, key_bias):
    n_rows, residues, features = x.shape
    groups, heads, depth, keys = bias.shape
    local = weight.shape[1] // 3
    width = local // heads
    blocks = max(1, 128 // depth)
    rows = blocks * depth
    return pl.pallas_call(
        attend_kernel,
        grid=(groups // blocks,),
        in_specs=[
            pl.BlockSpec(x.shape, lambda i: (0, 0, 0)),
            pl.BlockSpec((1, features), lambda i: (0, 0)),
            pl.BlockSpec(weight.shape, lambda i: (0, 0)),
            pl.BlockSpec((blocks, heads, depth, keys), lambda i: (i, 0, 0, 0)),
            pl.BlockSpec((1, keys), lambda i: (0, 0)),
        ],
        out_specs=pl.BlockSpec((n_rows, rows, local), lambda i: (0, i, 0)),
        out_shape=jax.ShapeDtypeStruct((n_rows, residues, local), jnp.float32),
        scratch_shapes=[
            pltpu.VMEM((n_rows, heads, residues, 3 * width), jnp.bfloat16),
            pltpu.VMEM((n_rows, heads, residues, 3 * width), jnp.bfloat16),
            pltpu.VMEM((n_rows, heads, residues, 2 * width), jnp.bfloat16),
        ],
        cost_estimate=pl.CostEstimate(flops=4 * 10**9, bytes_accessed=6 * 10**6, transcendentals=2 * 10**6),
    )(x, gain[None, :], weight, bias, key_bias)


def outer_kernel(scale_ref, left_ref, weight_ref, right_ref, live_ref, pair_ref, out_ref,
                 r_hi, r_lo, t_hi, t_lo):
    step, cols, depth = pair_ref.shape
    rows_all = r_hi.shape[1]
    n_rows = left_ref.shape[0] // step
    width = rows_all // n_rows
    me = pl.program_id(0)

    @pl.when(me == 0)
    def _():
        hi, lo = split(right_ref[...].T)
        r_hi[...] = hi
        r_lo[...] = lo

    left = left_ref[...]
    group = 2
    for d0 in range(0, width, group):
        t = mm(left, weight_ref[:, d0 * depth:(d0 + group) * depth])
        hi, lo = split(t)
        for g in range(group):
            d = d0 + g
            for i in range(step):
                src = (slice(i * n_rows, (i + 1) * n_rows), slice(g * depth, (g + 1) * depth))
                dst = (slice(d * n_rows, (d + 1) * n_rows), slice(i * depth, (i + 1) * depth))
                t_hi[dst] = hi[src]
                t_lo[dst] = lo[src]
    update = mm(r_hi[...], t_hi[...]) + mm(r_lo[...], t_hi[...]) + mm(r_hi[...], t_lo[...])
    for i in range(step):
        norm = scale_ref[me * step + i] * live_ref[...] + 0.001
        out_ref[i] = pair_ref[i] + update[:, i * depth:(i + 1) * depth] / norm


def outer_mean(scale, left, weight, right, live, pair):
    rows, cols, depth = pair.shape
    total = right.shape[0]
    n_rows = left.shape[0] // rows
    packed = left.shape[1]
    step = 4
    return pl.pallas_call(
        outer_kernel,
        grid=(rows // step,),
        in_specs=[
            pl.BlockSpec(memory_space=pltpu.SMEM),
            pl.BlockSpec((step * n_rows, packed), lambda i: (i, 0)),
            pl.BlockSpec(weight.shape, lambda i: (0, 0)),
            pl.BlockSpec(right.shape, lambda i: (0, 0)),
            pl.BlockSpec((cols, 1), lambda i: (0, 0)),
            pl.BlockSpec((step, cols, depth), lambda i: (i, 0, 0)),
        ],
        out_specs=pl.BlockSpec((step, cols, depth), lambda i: (i, 0, 0)),
        out_shape=jax.ShapeDtypeStruct(pair.shape, jnp.float32),
        scratch_shapes=[
            pltpu.VMEM((cols, total), jnp.bfloat16),
            pltpu.VMEM((cols, total), jnp.bfloat16),
            pltpu.VMEM((total, step * depth), jnp.bfloat16),
            pltpu.VMEM((total, step * depth), jnp.bfloat16),
        ],
        cost_estimate=pl.CostEstimate(flops=9 * 10**9, bytes_accessed=10**7, transcendentals=0),
    )(scale, left, weight, right, live, pair)


def gather_kernel(n, block_ref, out_ref, own_sem, send_sem, recv_sem):
    me = lax.axis_index("row")
    core = me % 2
    x = (me // 2) % 2
    nz = n // 4
    z = me // 4

    def place(zz, xx, cc):
        return (zz * 2 + xx) * 2 + cc

    barrier = pltpu.get_barrier_semaphore()
    up_ok, down_ok = z + 1 < nz, z >= 1

    def greet(target):
        pl.semaphore_signal(barrier, inc=1, device_id={"row": target},
                            device_id_type=pl.DeviceIdType.MESH)

    greet(place(z, x, 1 - core))
    greet(place(z, 1 - x, core))
    pl.when(up_ok)(lambda: greet(place(z + 1, x, core)))
    pl.when(down_ok)(lambda: greet(place(z - 1, x, core)))
    peers = 2 + jnp.where(up_ok, 1, 0) + jnp.where(down_ok, 1, 0)
    pl.semaphore_wait(barrier, peers)

    own = pltpu.make_async_copy(block_ref, out_ref.at[me], own_sem)
    own.start()

    def sends(d, other):
        found = []
        first = core == 0
        if other == 0:
            cross = (z >= 0) if d == 0 else jnp.logical_not(first)
            run = z >= 0
        else:
            cross = None
            run = first
        if d <= 0:
            found.append((jnp.logical_and(run, up_ok), 0, lambda: place(z + 1, x, core)))
        if d >= 0:
            found.append((jnp.logical_and(run, down_ok), 1, lambda: place(z - 1, x, core)))
        if cross is not None:
            found.append((cross, 2, lambda: place(z, 1 - x, core)))
        found.append((z >= 0, 3, lambda: place(z, x, 1 - core)))
        return found

    def copy(source, kind, target, mine):
        return pltpu.make_async_remote_copy(
            src_ref=block_ref if mine else out_ref.at[source],
            dst_ref=out_ref.at[source],
            send_sem=send_sem.at[kind, source],
            recv_sem=recv_sem.at[source],
            device_id={"row": target},
            device_id_type=pl.DeviceIdType.MESH,
        )

    hops = [(0, 0), (0, 1)]
    for far in range(1, nz):
        hops += [(-far, 0), (far, 0), (-far, 1), (far, 1)]

    def each(action):
        for d, other in hops:
            source = place(z + d, (x + other) % 2, core)
            mine = d == 0 and other == 0
            there = jnp.logical_and(z + d >= 0, z + d < nz)

            @pl.when(there)
            def _(d=d, other=other, source=source, mine=mine):
                action(d, other, source, mine)

    def forward(d, other, source, mine):
        if not mine:
            copy(source, 3, place(z, x, 1 - core), False).wait_recv()
        for ok, kind, target in sends(d, other):
            pl.when(ok)(lambda kind=kind, target=target: copy(source, kind, target(), mine).start())

    def finish(d, other, source, mine):
        for ok, kind, target in sends(d, other):
            pl.when(ok)(lambda kind=kind, target=target: copy(source, kind, target(), mine).wait_send())

    each(forward)
    for k in range(n // 2):
        copy(2 * k + 1 - core, 3, place(z, x, 1 - core), False).wait_recv()
    each(finish)
    own.wait()


def gather_rows(block, n, ident):
    return pl.pallas_call(
        functools.partial(gather_kernel, n),
        out_shape=jax.ShapeDtypeStruct((n,) + block.shape, block.dtype),
        in_specs=[pl.BlockSpec(memory_space=pltpu.VMEM)],
        out_specs=pl.BlockSpec(memory_space=pl.ANY),
        scratch_shapes=[
            pltpu.SemaphoreType.DMA,
            pltpu.SemaphoreType.DMA((4, n)),
            pltpu.SemaphoreType.DMA((n,)),
        ],
        compiler_params=pltpu.CompilerParams(collective_id=ident, has_side_effects=True),
    )(block)


def around(n):
    return [[(src, (src + k) % n) for src in range(n)] for k in range(n)]


def gather_heads(block, n, index, axis):
    size = block.shape[axis]
    shape = list(block.shape)
    shape[axis] = size * n
    whole = jnp.zeros(shape, block.dtype)
    for k in range(n):
        part = block if k == 0 else lax.ppermute(block, "head", around(n)[k])
        whole = lax.dynamic_update_slice_in_dim(whole, part, ((index - k) % n) * size, axis)
    return whole


def exchange_heads(block, n, index, split_axis, concat_axis):
    size = block.shape[split_axis] // n
    shape = list(block.shape)
    shape[split_axis] = size
    length = shape[concat_axis]
    shape[concat_axis] = length * n
    whole = jnp.zeros(shape, block.dtype)
    for k in range(n):
        part = lax.dynamic_slice_in_dim(block, ((index + k) % n) * size, size, split_axis)
        if k:
            part = lax.ppermute(part, "head", around(n)[k])
        whole = lax.dynamic_update_slice_in_dim(whole, part, ((index - k) % n) * length, concat_axis)
    return whole


def body(
    sequence_matrix,
    pair_representation,
    alignment_row_mask,
    residue_mask,
    attention_scale_vector,
    asking_factor_matrix,
    lookup_factor_matrix,
    content_factor_matrix,
    sigmoid_factor_matrix,
    final_factor_matrix,
    pair_norm_gain,
    bias_weight,
    tensor_scale_vector,
    first_factor_matrix,
    second_factor_matrix,
    outer_weight,
):
    head_count = lax.axis_size("head")
    head_index = lax.axis_index("head")
    row_index = lax.axis_index("row")
    row_count = lax.axis_size("row")
    n_rows, col_count, width = sequence_matrix.shape
    residues = col_count * head_count
    pair_rows = pair_representation.shape[0]
    pair_depth = pair_representation.shape[2]
    heads_all = bias_weight.shape[1]
    head_width = width // heads_all
    local_heads = heads_all // head_count
    local_width = local_heads * head_width
    opm_width = first_factor_matrix.shape[1]

    sequence_all = gather_heads(sequence_matrix, head_count, head_index, 1)

    bias_all = pair_bias(pair_representation, pair_norm_gain, bias_weight)
    bias_part = exchange_heads(
        bias_all.transpose(1, 0, 2), head_count, head_index, 0, 2
    )
    bias = gather_rows(bias_part, row_count, 0)
    key_bias = ((residue_mask.astype(jnp.float32) - 1.0) * 1000000000.0)[None, :]

    weights = jnp.concatenate(
        [
            lax.dynamic_slice_in_dim(w, head_index * local_width, local_width, 1)
            for w in (asking_factor_matrix, lookup_factor_matrix, content_factor_matrix)
        ],
        axis=1,
    )
    attended = attend(sequence_all, attention_scale_vector, weights, bias, key_bias)
    norm_mine = apply_layer_norm(sequence_matrix, attention_scale_vector)
    gate = jax.nn.sigmoid(
        jnp.einsum("sic,ce->sie", norm_mine, sigmoid_factor_matrix, precision=HIGH)
    )
    returned_values = exchange_heads(attended, head_count, head_index, 1, 2) * gate
    alignment_updated = sequence_matrix + jnp.einsum(
        "jna,ab->jnb", returned_values, final_factor_matrix, precision=HIGH
    )

    outer_product_norm = apply_layer_norm(alignment_updated, tensor_scale_vector)
    live_cols = lax.dynamic_slice_in_dim(residue_mask, head_index * col_count, col_count).astype(
        jnp.float32
    )
    row_live = alignment_row_mask.astype(jnp.float32)
    live = row_live[:, None] * live_cols[None, :]
    left_side = (
        jnp.einsum("sic,co->soi", outer_product_norm, first_factor_matrix, precision=HIGH)
        * live[:, None, :]
    )
    right = (
        jnp.einsum("sic,co->soi", outer_product_norm, second_factor_matrix, precision=HIGH)
        * live[:, None, :]
    )
    left_all = gather_heads(left_side, head_count, head_index, 1)
    carried = jnp.broadcast_to(row_live[:, None, None], (n_rows, 8, col_count))
    sides = gather_rows(jnp.concatenate([left_all, right, carried], axis=1), row_count, 1)
    sides = sides.reshape(row_count * n_rows, -1, col_count)
    left_width = head_count * opm_width
    first_row = row_index * pair_rows
    left_mine = lax.dynamic_slice(
        sides,
        (0, (first_row // col_count) * opm_width, first_row % col_count),
        (row_count * n_rows, opm_width, pair_rows),
    )
    right_all = sides[:, left_width:]
    total_rows = row_count * n_rows
    count = jnp.sum(right_all[:, opm_width, 0])
    right_rows = right_all[:, :opm_width].transpose(1, 0, 2).reshape(
        opm_width * total_rows, col_count
    )
    left_rows = left_mine.transpose(2, 0, 1).reshape(pair_rows * total_rows, opm_width)
    l_hi, l_lo = split_outside(left_rows)
    w_hi, w_lo = split_outside(outer_weight.reshape(opm_width, opm_width * pair_depth))
    rows_live = lax.dynamic_slice_in_dim(residue_mask, row_index * pair_rows, pair_rows).astype(
        jnp.float32
    )
    pair_out = outer_mean(
        count * rows_live,
        jnp.concatenate([l_hi, l_hi, l_lo], axis=1),
        jnp.concatenate([w_hi, w_lo, w_hi], axis=0),
        right_rows,
        live_cols[:, None],
        pair_representation,
    )
    return alignment_updated, pair_out


def ln(values, gains):
    return apply_layer_norm(values, gains)


def front_kernel(
    x_hbm, pair_hbm, row_mask_hbm, key_hbm, gain_hbm, wq_hbm, wk_hbm, wv_hbm, wg_hbm, wo_hbm,
    pair_gain_hbm, bias_hbm, tensor_gain_hbm, left_hbm, right_hbm, weight_hbm, mask_hbm,
    msa_ref, acc_ref,
    x_ref, pair_ref, wq_ref, wk_ref, wv_ref, wg_ref, wo_ref, wpair_ref, group_ref,
    bias_ref, xn_ref, q_ref, k_ref, v_ref, absent_ref, logit_ref, e_ref, gate_ref, att_out, att_in, right_buf, left_loc, left_own,
    left_in, row_mask, mask_ref, key_ref, gain_ref, pair_gain, bias_w, tensor_gain, left_w, right_w,
    weight_ref, w_ref, rows_ref, rt_ref, r_hi, r_lo, t_hi_0, t_hi_1, t_lo_0, t_lo_1, live_ref,
    load_sem, pair_sem, s1_send, s1_recv, n_send, n_recv, z_send, z_recv, x_send, x_recv, xl_send, t_send, t_recv,
    a_send, a_recv, rz_send, rz_recv, rx_send, rx_recv, rc_send, rc_recv,
    l1_send, l1_recv, l2_send, l2_recv,
):
    nz, _, chunks, _, n_y, group_heads, sub, cols = bias_ref.shape
    n_rows, _, feat = x_ref.shape
    heads = bias_w.shape[0]
    keys = n_y * cols
    width = k_ref.shape[3] // 4
    group_width = group_heads * width
    local_width = 2 * group_width
    per_half = nz // n_y
    plane = cols // per_half
    pair_width = pair_ref.shape[2]
    opm = left_w.shape[0]

    me, y = lax.axis_index("row"), lax.axis_index("head")
    c, x, z = me % 2, (me // 2) % 2, me // 4
    half = z // per_half

    def place(zz, xx, cc):
        return (zz * 2 + xx) * 2 + cc

    def across(d):
        out, bit = z, 1
        while bit <= d:
            if d & bit:
                out = out + bit * (1 - 2 * ((out // bit) % 2))
            bit *= 2
        return out

    def plane_at(p):
        if p == 0:
            return z
        late = jnp.where(z < nz // 2, max(p, 2), nz - 1 - max(p, 2))
        return jnp.where((half == y) == (p == 1), late, across(1)) if p < 3 else late

    def remote(src, dst, send, recv, row, head):
        return pltpu.make_async_remote_copy(
            src_ref=src, dst_ref=dst, send_sem=send, recv_sem=recv,
            device_id={"row": row, "head": head}, device_id_type=pl.DeviceIdType.MESH,
        )

    def arrived(dst, send, recv):
        remote(dst, dst, send, recv, place(z, x, 1 - c), y).wait_recv()

    pending = []

    def go(copy):
        copy.start()
        pending.append(copy)

    loads = {}
    for at, (src, dst) in enumerate(
        [(x_hbm, x_ref), (wq_hbm, wq_ref), (wk_hbm, wk_ref), (wv_hbm, wv_ref), (wg_hbm, wg_ref), (wo_hbm, wo_ref),
         (weight_hbm, weight_ref), (pair_gain_hbm, pair_gain), (bias_hbm, bias_w), (gain_hbm, gain_ref),
         (key_hbm, key_ref), (row_mask_hbm, row_mask), (mask_hbm, mask_ref), (tensor_gain_hbm, tensor_gain),
         (left_hbm, left_w), (right_hbm, right_w)]
    ):
        loads[at] = pltpu.make_async_copy(src, dst, load_sem.at[at])
    pair_loads = [
        pltpu.make_async_copy(
            pair_hbm.at[pl.ds(k * sub, sub)], pair_ref.at[pl.ds(k * sub, sub)], pair_sem.at[k]
        )
        for k in range(chunks)
    ]
    for at in (7, 8):
        loads[at].start()
    for copy in pair_loads:
        copy.start()
    for at in [0, 9, 10] + list(range(1, 7)) + list(range(11, 16)):
        loads[at].start()

    barrier = pltpu.get_barrier_semaphore()
    peers = []
    for dx in range(2):
        for dc in range(2):
            for dy in range(n_y):
                if dx or dc or dy:
                    peers.append((place(z, (x + dx) % 2, (c + dc) % 2), (y + dy) % n_y))
    for d in range(1, nz):
        peers.append((place(across(d), x, c), y))
    for row, head in peers:
        pl.semaphore_signal(barrier, inc=1, device_id={"row": row, "head": head},
                            device_id_type=pl.DeviceIdType.MESH)

    for at in (7, 8):
        loads[at].wait()
    w_hi, w_lo = split(bias_w[...] * LOG2E)
    spread = sub * heads
    at_row = lax.broadcasted_iota(jnp.int32, (heads, sub, pair_width), 1).reshape(spread, pair_width)
    zero = jnp.zeros((spread, pair_width), jnp.float32)

    def rows_of(part):
        part = part.astype(jnp.float32)
        return jnp.broadcast_to(part[:, None, :], (heads, sub, pair_width)).reshape(spread, pair_width)

    rep_hi, rep_lo = rows_of(w_hi), rows_of(w_lo)
    for t in range(sub // 2):
        first, second = at_row == 2 * t, at_row == 2 * t + 1
        both = [
            jnp.concatenate([jnp.where(first, rep, zero), jnp.where(second, rep, zero)], axis=1)
            for rep in (rep_hi, rep_lo)
        ]
        wpair_ref[t] = jnp.concatenate(both, axis=0).astype(jnp.bfloat16)

    def bias_chunk(k):
        pair_loads[k].wait()
        total = None
        for t in range(sub // 2):
            at = k * sub + 2 * t
            pieces = [split(ln(pair_ref[at + e], pair_gain[...])) for e in range(2)]
            hi = jnp.concatenate([pieces[0][0], pieces[1][0]], axis=1)
            lo = jnp.concatenate([pieces[0][1], pieces[1][1]], axis=1)
            both = mm(wpair_ref[t], hi, NT)
            part = both[:spread] + both[spread:] + mm(wpair_ref[t, :spread], lo, NT)
            total = part if total is None else total + part
        group_ref[k] = total.reshape(2 * n_y, group_heads, sub, cols)
        bias_ref[z, x, k, c, y] = group_ref[k, y * 2 + c]

    labels = [(dy, dc) for dy in range(n_y) for dc in range(2) if dy or dc]

    def stage_one(k):
        for at, (dy, dc) in enumerate(labels):
            ty, tc = (y + dy) % n_y, (c + dc) % 2
            go(remote(group_ref.at[k, ty * 2 + tc], bias_ref.at[z, x, k, c, y],
                      s1_send.at[k, at], s1_recv.at[k, at], place(z, x, tc), ty))

    def stage_two(k):
        for at, (dy, dc) in enumerate(labels):
            sy, sc = (y + n_y - dy) % n_y, (c + dc) % 2
            arrived(bias_ref.at[z, x, k, sc, sy], s1_send.at[k, at], s1_recv.at[k, at])
        own = bias_ref.at[z, x, k]
        for up in range(2):
            pl.when(reaches(up, 1))(lambda up=up: relay_copy(up, z, k).start())
        cross_copy(z, k).start()

    def relay_copy(up, zz, k):
        block = bias_ref.at[zz, x] if k is None else bias_ref.at[zz, x, k]
        return remote(block, block, z_send.at[up, zz], z_recv.at[zz, 0 if k is None else k],
                      place(z + 1 if up else z - 1, x, c), y)

    def reaches(up, j):
        return z + j < nz if up else z >= j

    def source(up, j):
        return (z - j, z >= j) if up else (z + j, z + j < nz)

    def pass_on(j, k):
        for up in range(2):
            zz, there = source(up, j)

            @pl.when(there)
            def _(up=up, zz=zz):
                block = bias_ref.at[zz, x, k]
                arrived(block, z_send.at[0, 0], z_recv.at[zz, k])
                if j < nz - 1:
                    pl.when(reaches(up, 1))(lambda: relay_copy(up, zz, k).start())
                cross_copy(zz, k, True).start()

    def pass_twin(j):
        for up in range(2):
            zz, there = source(up, j)

            @pl.when(there)
            def _(up=up, zz=zz):
                arrived(bias_ref.at[zz, 1 - x, last_chunk, 0], t_send.at[0, 0], t_recv.at[zz])
                if j < nz - 1:
                    pl.when(reaches(up, 1))(lambda: twin_copy(up, zz).start())

    last_chunk = chunks - 1

    def cross_copy(zz, k, beyond=False):
        block = bias_ref.at[zz, x, k, 1] if beyond and k == last_chunk else bias_ref.at[zz, x, k]
        return remote(block, block, (xl_send if k == last_chunk else x_send).at[zz], x_recv.at[zz, k],
                      place(z, 1 - x, c), y)

    def twin_copy(up, zz):
        block = bias_ref.at[zz, 1 - x, last_chunk, 0]
        return remote(block, block, t_send.at[up, zz], t_recv.at[zz], place(z + 1 if up else z - 1, x, c), y)

    def start_twins():
        arrived(bias_ref.at[z, 1 - x, last_chunk], xl_send.at[0], x_recv.at[z, last_chunk])
        for up in range(2):
            pl.when(reaches(up, 1))(lambda up=up: twin_copy(up, z).start())

    bias_chunk(0)
    pl.semaphore_wait(barrier, len(peers))
    stage_one(0)
    for k in range(1, chunks):
        bias_chunk(k)
        stage_one(k)
        if k >= 2:
            stage_two(k - 2)

    for at in (0, 9, 10):
        loads[at].wait()
    for s in range(n_rows):
        xn_ref[y, c, s] = ln(x_ref[s], gain_ref[...])
        own_x = xn_ref.at[y, c, s]
        for dy in range(1, n_y):
            go(remote(own_x, own_x, n_send.at[dy, s], n_recv.at[dy, s], place(z, x, c), (y + dy) % n_y))
        go(remote(own_x, own_x, n_send.at[0, s], n_recv.at[0, s], place(z, x, 1 - c), y))
    stage_two(chunks - 2)

    for at in (1, 2, 3):
        loads[at].wait()
    mine = pl.ds(pl.multiple_of(y * local_width, local_width), local_width)
    picked = []
    for ref in (wq_ref, wk_ref, wv_ref):
        whole = ref[:, mine]
        picked.append(jnp.where(c == 0, whole[:, :group_width], whole[:, group_width:]))
    wa_hi, wa_lo = split(jnp.concatenate(picked, axis=1))

    lane = lax.broadcasted_iota(jnp.int32, (cols, width), 1)
    pick = jnp.where(lane < 2, 1.0, 0.0).astype(jnp.bfloat16)
    one, none = jnp.ones((cols, width), jnp.bfloat16), jnp.zeros((cols, width), jnp.bfloat16)
    for yy in range(n_y):
        keep = jnp.broadcast_to(
            key_ref[:, yy * cols:(yy + 1) * cols].astype(jnp.float32), (pair_width, cols)
        ).T[:, :width]
        hi, lo = split((keep - 1.0) * (1000000000.0 * LOG2E))
        absent_ref[yy] = jnp.where(
            lane == 0, hi.astype(jnp.float32), jnp.where(lane == 1, lo.astype(jnp.float32), 0.0)
        ).astype(jnp.bfloat16)

    def project(yy, cc, rows=range(n_rows)):
        spot = pl.ds(pl.multiple_of(yy * cols, cols), cols)
        absent = absent_ref[yy]
        for s in rows:
            hi, lo = split(xn_ref[yy, cc, s])
            made = mm(hi, wa_hi) + mm(lo, wa_hi) + mm(hi, wa_lo)
            q_hi, q_lo = split(made[:, :group_width] * (LOG2E / math.sqrt(width)))
            k_hi, k_lo = split(made[:, group_width:2 * group_width])
            v_hi, v_lo = split(made[:, 2 * group_width:])
            for h in range(group_heads):
                at = slice(h * width, (h + 1) * width)
                to = cc * n_rows + s
                q_ref[to, h, spot, :] = jnp.concatenate([q_hi[:, at], q_hi[:, at], q_lo[:, at], pick], axis=-1)
                k_ref[to, h, spot, :] = jnp.concatenate([k_hi[:, at], k_lo[:, at], k_hi[:, at], absent], axis=-1)
                mine_at, count_at = s * group_heads + h, (s * group_heads + h + 1) % (n_rows * group_heads)
                parts = [none] * (2 * n_rows * group_heads)
                parts[mine_at], parts[count_at], parts[n_rows * group_heads + mine_at] = v_hi[:, at], one, v_lo[:, at]
                v_ref[to, h, spot, :] = jnp.concatenate(parts, axis=-1)

    project(y, c)
    stage_two(chunks - 1)

    def gate_rows(s):
        hi, lo = split(xn_ref[y, c, s])
        gate_ref[s] = jax.nn.sigmoid(mm(hi, g_hi) + mm(lo, g_hi) + mm(hi, g_lo))

    def own_rows(s):
        arrived(xn_ref.at[y, 1 - c, s], n_send.at[0, s], n_recv.at[0, s])
        project(y, 1 - c, [s])

    def spread_weight(d0, d1):
        for d in range(d0, d1):
            hi, lo = split(weight_ref[pl.ds(d, opm, stride=opm), :])
            w_ref[:, d * pair_width:(d + 1) * pair_width] = jnp.concatenate([hi, lo, hi], axis=0)

    def clear(i0, i1):
        acc_ref[i0:i1] = jnp.zeros((i1 - i0, cols, pair_width), jnp.float32)

    loads[4].wait()
    g_hi, g_lo = split(wg_ref[...])
    loads[6].wait()
    pair_rows = pair_ref.shape[0]
    fillers = [functools.partial(gate_rows, s) for s in range(n_rows)]
    fillers += [functools.partial(own_rows, s) for s in range(n_rows)]
    quarter = opm // 4
    fillers += [functools.partial(spread_weight, i * quarter, (i + 1) * quarter) for i in range(4)]
    part = pair_rows // 4
    fillers += [functools.partial(clear, i * part, (i + 1) * part) for i in range(4)]
    tasks = [functools.partial(pass_on, j, k) for j in range(1, nz) for k in range(chunks)]
    for j in range(nz - 1, 0, -1):
        tasks.insert(min(chunks * (j + 1) - 1, len(tasks)), functools.partial(pass_twin, j))
    tasks.insert(chunks, start_twins)

    def advance(n_tasks, n_fillers):
        for _ in range(n_tasks):
            if tasks:
                tasks.pop(0)()
            if n_fillers and fillers:
                fillers.pop(0)()

    advance(chunks + 3, chunks + 3)
    while fillers:
        fillers.pop(0)()
    for dy in range(1, n_y):
        sy = (y + n_y - dy) % n_y
        for s in range(n_rows):
            block = xn_ref.at[sy, c, s]
            arrived(block, n_send.at[dy, s], n_recv.at[dy, s])
            go(remote(block, block, n_send.at[n_y + dy, s], n_recv.at[n_y + dy, s], place(z, x, 1 - c), y))
            advance(2 if s + 1 < n_rows else 1, 0)
            project(sy, c, [s])
            advance(1 if s + 1 < n_rows else 0, 0)
    for dy in range(1, n_y):
        sy = (y + n_y - dy) % n_y
        for s in range(n_rows):
            arrived(xn_ref.at[sy, 1 - c, s], n_send.at[n_y + dy, s], n_recv.at[n_y + dy, s])
            project(sy, 1 - c, [s])
    advance(max(0, len(tasks) - 4), 0)
    for copy in pending:
        copy.wait_send()
    pending.clear()

    own = pl.ds(pl.multiple_of(y * cols, cols), cols)
    live_ref[...] = jnp.broadcast_to(key_ref[:, own].astype(jnp.float32), (pair_width, cols)).T

    lanes = n_rows * group_width
    block = lax.broadcasted_iota(jnp.int32, (plane, lanes), 1) // width

    def attended_copy(d, ct):
        zz = plane_at(d)
        return remote(att_out.at[d, ct], att_in.at[y * 2 + c, zz % per_half],
                      a_send.at[d, ct], a_recv.at[y * 2 + c, zz % per_half],
                      place(z, x, ct), zz // per_half)

    def is_mine(d, ct):
        return jnp.logical_and(plane_at(d) // per_half == y, ct == c)

    def attend_plane(d):
        zz = plane_at(d)
        for k in range(last_chunk):
            arrived(bias_ref.at[zz, 1 - x, k], x_send.at[0], x_recv.at[zz, k])
        if d:
            arrived(bias_ref.at[zz, 1 - x, last_chunk, 1], xl_send.at[0], x_recv.at[zz, last_chunk])
        queries = pl.ds(pl.multiple_of(zz * plane, plane), plane)

        tiles = [
            jnp.concatenate(
                [
                    jnp.concatenate(
                        [bias_ref[zz, xx, :, cc, yy, h].reshape(chunks * sub, cols) for yy in range(n_y)],
                        axis=1,
                    )
                    for xx in range(2)
                    for cc in range(2)
                ],
                axis=0,
            )
            for h in range(group_heads)
        ]
        units = [(s, h) for s in range(n_rows) for h in range(group_heads)]

        def compare(ct):
            for at, (s, h) in enumerate(units):
                row = ct * n_rows + s
                logit_ref[ct, at] = mm(q_ref[row, h, queries, :], k_ref[row, h], NT) + tiles[h]

        def soften(ct):
            for at in range(len(units)):
                logits = logit_ref[ct, at]
                e_hi, e_lo = split(jnp.exp2(logits - jnp.max(logits, axis=-1, keepdims=True)))
                e_ref[ct, at, :plane] = e_hi
                e_ref[ct, at, plane:] = e_lo

        def gather(ct):
            upper = lower = None
            for at, (s, h) in enumerate(units):
                row = ct * n_rows + s
                both = mm(e_ref[ct, at, :plane], v_ref[row, h])
                whole = both[:, :lanes] + both[:, lanes:] + mm(e_ref[ct, at, plane:], v_ref[row, h, :, :lanes])
                upper = whole if upper is None else jnp.where(block == at, whole, upper)
                lower = whole if lower is None else jnp.where(block == (at + 1) % len(units), whole, lower)
            return upper / pltpu.roll(lower, lanes - width, 1)

        def hand_over(ct):
            @pl.when(is_mine(d, ct))
            def _():
                att_in[y * 2 + c, zz % per_half] = att_out[d, ct]

            pl.when(jnp.logical_not(is_mine(d, ct)))(lambda: attended_copy(d, ct).start())

        compare(0)
        soften(0)
        compare(1)
        att_out[d, 0] = gather(0)
        hand_over(0)
        soften(1)
        att_out[d, 1] = gather(1)
        hand_over(1)

    for d in range(nz):
        attend_plane(d)
        advance(2 if d + 2 < nz else len(tasks), 0)

    for at in (5,) + tuple(range(11, 16)):
        loads[at].wait()
    o_hi, o_lo = split(wo_ref[...])
    wide = n_rows * opm
    left_hi, left_lo = split(left_w[...])
    left_both = jnp.concatenate([left_hi, left_lo], axis=0)
    right_hi, right_lo = split(right_w[...])
    right_both = jnp.concatenate([right_hi, right_lo], axis=0)
    tall = pair_rows // 2

    def left_copy(p):
        return remote(left_loc.at[pl.ds(p * 4, 4)], left_own.at[z], l1_send.at[p], l1_recv.at[z],
                      place(y * per_half + p, x, c), y)

    def finish(p):
        for dy, dc in labels:
            sy, sc = (y + n_y - dy) % n_y, (c + dc) % 2
            arrived(att_in.at[sy * 2 + sc, p], a_send.at[0, 0], a_recv.at[sy * 2 + sc, p])
        part = slice(p * plane, (p + 1) * plane)
        lefts = []
        count = jnp.zeros((sub, plane), jnp.float32)
        for s in range(n_rows):
            at = slice(s * group_width, (s + 1) * group_width)
            whole = jnp.concatenate([att_in[g, p][:, at] for g in range(2 * n_y)], axis=1) * gate_ref[s, part]
            hi, lo = split(whole)
            out = x_ref[s, part] + (mm(hi, o_hi) + mm(lo, o_hi) + mm(hi, o_lo))
            msa_ref[s, part] = out
            f_hi, f_lo = split(ln(out, tensor_gain[...]))
            live = row_mask[s].astype(jnp.float32)
            both = mm(right_both, f_hi, NT)
            right_buf[z, x * 2 + c, s * opm:(s + 1) * opm, part] = (
                both[:opm] + both[opm:] + mm(right_hi, f_lo, NT)
            ) * live
            both = mm(f_hi, left_both, NT)
            lefts.append((both[:, :opm] + both[:, opm:] + mm(f_lo, left_hi, NT)) * live)
            count = count + live
        right_buf[z, x * 2 + c, wide:, part] = count
        left = jnp.concatenate(lefts, axis=1).reshape(4, 2, tall, wide)
        left_loc[p * 4:(p + 1) * 4] = jnp.concatenate([left[:, 0], left[:, 1]], axis=2)
        here = y * per_half + p == z

        @pl.when(here)
        def _():
            left_own[z] = left_loc[p * 4:(p + 1) * 4]

        pl.when(jnp.logical_not(here))(lambda: left_copy(p).start())

    for p in range(per_half):
        finish(p)

    def right_core(zz, far):
        block = right_buf.at[zz, (x if far == 0 else 1 - x) * 2 + c]
        return remote(block, block, rc_send.at[zz, far], rc_recv.at[zz, far], place(z, x, 1 - c), y)

    def right_direct(d):
        block = right_buf.at[z, x * 2 + c]
        return remote(block, block, rz_send.at[d], rz_recv.at[z], place(across(d), x, c), y)

    def right_cross(zz):
        block = right_buf.at[zz, x * 2 + c]
        return remote(block, block, rx_send.at[zz], rx_recv.at[zz], place(z, 1 - x, c), y)

    right_cross(z).start()
    right_core(z, 0).start()
    for d in range(1, nz):
        right_direct(d).start()

    owner = half == y
    finals = [(dx, dc, dy) for dx in range(2) for dc in range(2) for dy in range(n_y) if dx or dc or dy]

    def final_copy(at, zz):
        dx, dc, dy = finals[at]
        tx, tc, ty = (x + dx) % 2, (c + dc) % 2, (y + dy) % n_y
        return remote(left_own.at[zz, tx * 2 + tc], left_in.at[zz, x * 2 + c], l2_send.at[zz, at],
                      l2_recv.at[zz, x * 2 + c], place(z, tx, tc), ty)

    def left_pass(zz):
        @pl.when(owner)
        def _():
            pl.when(zz != z)(lambda: arrived(left_own.at[zz], l1_send.at[0], l1_recv.at[zz]))
            for at in range(len(finals)):
                final_copy(at, zz).start()
            left_in[zz, x * 2 + c] = left_own[zz, x * 2 + c]

    def left_wait(zz):
        for xx in range(2):
            for cc in range(2):
                mine_too = jnp.logical_and(owner, jnp.logical_and(xx == x, cc == c))

                @pl.when(jnp.logical_not(mine_too))
                def _(xx=xx, cc=cc):
                    arrived(left_in.at[zz, xx * 2 + cc], l2_send.at[0, 0], l2_recv.at[zz, xx * 2 + cc])

    def right_pass(zz):
        arrived(right_buf.at[zz, x * 2 + c], rz_send.at[0], rz_recv.at[zz])
        right_cross(zz).start()
        right_core(zz, 0).start()

    def right_far(zz):
        arrived(right_buf.at[zz, (1 - x) * 2 + c], rx_send.at[0], rx_recv.at[zz])
        right_core(zz, 1).start()

    ordered = across

    t_hi, t_lo = (t_hi_0, t_hi_1), (t_lo_0, t_lo_1)
    slots = 4 * n_rows
    group = 4

    def left_rows(zz):
        for i in range(2 * tall):
            block = left_in[zz, :, i % tall, :]
            base = (i // tall) * wide
            rows_ref[i * slots:(i + 1) * slots, :] = jnp.concatenate(
                [block[:, base + s * opm:base + (s + 1) * opm] for s in range(n_rows)], axis=0
            )
        hi, lo = split(rows_ref[...])
        return jnp.concatenate([hi, hi, lo], axis=1)

    def weigh(rows, to, d0, d1):
        for d in range(d0, d1, 2):
            t = mm(rows, w_ref[:, d * pair_width:(d + 2) * pair_width])
            for i in range(2 * tall):
                piece = t[i * slots:(i + 1) * slots]
                hi, lo = split(jnp.concatenate([piece[:, :pair_width], piece[:, pair_width:]], axis=0))
                rows_at, cols_at = slice(d * slots, (d + 2) * slots), slice(i * pair_width, (i + 1) * pair_width)
                t_hi[to][rows_at, cols_at] = hi
                t_lo[to][rows_at, cols_at] = lo

    def right_ready(zz):
        for far in range(2):
            block = right_buf.at[zz, (x if far == 0 else 1 - x) * 2 + 1 - c]
            arrived(block, rc_send.at[0, 0], rc_recv.at[zz, far])

    def right_rows(zz):
        for d in range(opm):
            for s in range(n_rows):
                spot = (d * n_rows + s) * 4
                rt_ref[spot:spot + 4, :] = right_buf[zz, :, s * opm + d, :]
        hi, lo = split(rt_ref[...].T)
        r_hi[...] = hi
        r_lo[...] = lo

    def update_of(at, i):
        cols_at = slice(i * pair_width, (i + group) * pair_width)
        high = t_hi[at][:, cols_at]
        return mm(r_hi[...], high) + mm(r_lo[...], high) + mm(r_hi[...], t_lo[at][:, cols_at])

    left_pass(z)
    for zz in range(nz):
        block = bias_ref.at[zz, x, pl.ds(0, last_chunk)]
        remote(block, block, x_send.at[zz], x_recv.at[zz, 0], place(z, 1 - x, c), y).wait_send()
        pl.when(zz == z)(lambda zz=zz: cross_copy(zz, last_chunk).wait_send())
        pl.when(zz != z)(lambda zz=zz: cross_copy(zz, last_chunk, True).wait_send())
        for up in range(2):
            far = zz <= z if up else zz >= z
            @pl.when(jnp.logical_and(far, reaches(up, 1)))
            def _(up=up, zz=zz):
                relay_copy(up, zz, None).wait_send()
                twin_copy(up, zz).wait_send()

    for d in range(nz):
        for ct in range(2):
            pl.when(jnp.logical_not(is_mine(d, ct)))(lambda d=d, ct=ct: attended_copy(d, ct).wait_send())

    left_wait(z)
    left_pass(ordered(1))
    rows = left_rows(z)
    weigh(rows, 0, 0, opm // 4)
    right_far(z)
    right_pass(ordered(1))
    weigh(rows, 0, opm // 4, opm)

    def outer_plane(p):
        zz, after = ordered(p), ordered(p + 1)
        now, later = p % 2, (p + 1) % 2
        right_ready(zz)
        left_wait(after)
        rows = left_rows(after)
        right_rows(zz)
        share = opm // (2 * tall // group)
        for i in range(0, 2 * tall, group):
            update = update_of(now, i)
            for e in range(group):
                acc_ref[i + e] += update[:, e * pair_width:(e + 1) * pair_width]
            weigh(rows, later, i // group * share, (i // group + 1) * share)
            if i + group == tall:
                for q in range(2, nz if p == 0 else 0):
                    left_pass(ordered(q))
                if p + 2 < nz:
                    right_pass(ordered(p + 2))
                right_far(after)

    for p in range(nz - 1):
        outer_plane(p)

    last = ordered(nz - 1)
    right_ready(last)
    total = jnp.zeros((sub, pair_width), jnp.float32)
    for zz in range(nz):
        for at in range(4):
            total = total + right_buf[zz, at, wide:, :pair_width]
    live_ref[...] = live_ref[...] * (1.0 / (total[0:1, :] + 0.001))
    right_rows(last)
    for i in range(0, 2 * tall, group):
        update = update_of((nz - 1) % 2, i)
        for e in range(group):
            live = mask_ref[me * 2 * tall + i + e].astype(jnp.float32)
            whole = acc_ref[i + e] + update[:, e * pair_width:(e + 1) * pair_width]
            acc_ref[i + e] = pair_ref[i + e] + whole * (live_ref[...] * live)

    for zz in range(nz):
        right_cross(zz).wait_send()
        for far in range(2):
            right_core(zz, far).wait_send()
    for d in range(1, nz):
        right_direct(d).wait_send()
    for p in range(per_half):
        pl.when(y * per_half + p != z)(lambda p=p: left_copy(p).wait_send())

    @pl.when(owner)
    def _():
        for zz in range(nz):
            for at in range(len(finals)):
                final_copy(at, zz).wait_send()


def front(n_row, n_y, x, pair, row_mask, residue_mask, gain, wq, wk, wv, wg, wo,
          pair_gain, bias_w, tensor_gain, left_w, right_w, weight):
    n_rows, cols, feat = x.shape
    pair_rows, _, pair_width = pair.shape
    heads = bias_w.shape[1]
    width = feat // heads
    group_heads = heads // n_y // 2
    nz, sub = n_row // 4, 8
    chunks = pair_rows // sub
    keys = n_y * cols
    per_half = nz // n_y
    plane = cols // per_half
    opm = left_w.shape[1]
    wide = n_rows * opm
    f32, b16 = jnp.float32, jnp.bfloat16
    hbm, vmem = pl.BlockSpec(memory_space=pltpu.HBM), pl.BlockSpec(memory_space=pltpu.VMEM)
    dma = pltpu.SemaphoreType.DMA
    labels = 2 * n_y - 1
    return pl.pallas_call(
        front_kernel,
        out_shape=(
            jax.ShapeDtypeStruct(x.shape, f32),
            jax.ShapeDtypeStruct(pair.shape, f32),
        ),
        in_specs=[hbm] * 17,
        out_specs=(vmem, vmem),
        scratch_shapes=[
            pltpu.VMEM(x.shape, f32),
            pltpu.VMEM(pair.shape, f32),
        ]
        + [pltpu.VMEM((feat, feat), f32)] * 5
        + [
            pltpu.VMEM((sub // 2, 2 * sub * heads, 2 * pair_width), b16),
            pltpu.VMEM((chunks, 2 * n_y, group_heads, sub, cols), f32),
            pltpu.VMEM((nz, 2, chunks, 2, n_y, group_heads, sub, cols), f32),
            pltpu.VMEM((n_y, 2, n_rows, cols, feat), f32),
            pltpu.VMEM((2 * n_rows, group_heads, keys, 4 * width), b16),
            pltpu.VMEM((2 * n_rows, group_heads, keys, 4 * width), b16),
            pltpu.VMEM((2 * n_rows, group_heads, keys, 2 * n_rows * group_heads * width), b16),
            pltpu.VMEM((n_y, cols, width), b16),
            pltpu.VMEM((2, n_rows * group_heads, plane, keys), f32),
            pltpu.VMEM((2, n_rows * group_heads, 2 * plane, keys), b16),
            pltpu.VMEM(x.shape, f32),
            pltpu.VMEM((nz, 2, plane, n_rows * group_heads * width), f32),
            pltpu.VMEM((2 * n_y, per_half, plane, n_rows * group_heads * width), f32),
            pltpu.VMEM((nz, 4, wide + sub, cols), f32),
            pltpu.VMEM((4 * per_half, pair_rows // 2, 2 * wide), f32),
            pltpu.VMEM((nz, 4, pair_rows // 2, 2 * wide), f32),
            pltpu.VMEM((nz, 4, pair_rows // 2, 2 * wide), f32),
            pltpu.SMEM(row_mask.shape, jnp.int32),
            pltpu.SMEM(residue_mask.shape, jnp.int32),
            pltpu.VMEM((1, keys), jnp.int32),
            pltpu.VMEM((1, feat), f32),
            pltpu.VMEM((1, pair_width), f32),
            pltpu.VMEM((heads, pair_width), f32),
            pltpu.VMEM((1, feat), f32),
            pltpu.VMEM((opm, feat), f32),
            pltpu.VMEM((opm, feat), f32),
            pltpu.VMEM(weight.shape, f32),
            pltpu.VMEM((3 * opm, opm * pair_width), b16),
            pltpu.VMEM((pair_rows * 4 * n_rows, opm), f32),
            pltpu.VMEM((opm * 4 * n_rows, cols), f32),
            pltpu.VMEM((cols, opm * 4 * n_rows), b16),
            pltpu.VMEM((cols, opm * 4 * n_rows), b16),
            pltpu.VMEM((opm * 4 * n_rows, pair_rows * pair_width), b16),
            pltpu.VMEM((opm * 4 * n_rows, pair_rows * pair_width), b16),
            pltpu.VMEM((opm * 4 * n_rows, pair_rows * pair_width), b16),
            pltpu.VMEM((opm * 4 * n_rows, pair_rows * pair_width), b16),
            pltpu.VMEM((cols, pair_width), f32),
            dma((16,)), dma((chunks,)),
            dma((chunks, labels)), dma((chunks, labels)),
            dma((2 * n_y, n_rows)), dma((2 * n_y, n_rows)),
            dma((2, nz)), dma((nz, chunks)),
            dma((nz,)), dma((nz, chunks)), dma((nz,)), dma((2, nz)), dma((nz,)),
            dma((nz, 2)), dma((2 * n_y, per_half)),
            dma((nz,)), dma((nz,)), dma((nz,)), dma((nz,)),
            dma((nz, 2)), dma((nz, 2)),
            dma((per_half,)), dma((nz,)),
            dma((nz, 4 * n_y - 1)), dma((nz, 4)),
        ],
        compiler_params=pltpu.CompilerParams(
            collective_id=0, has_side_effects=True, vmem_limit_bytes=VMEM_GRANT
        ),
    )(*[
        pltpu.with_memory_space_constraint(a, pltpu.HBM)
        for a in (x, pair, row_mask, residue_mask[None, :], gain[None, :], wq, wk, wv, wg, wo,
                  pair_gain[None, :], bias_w.T, tensor_gain[None, :], left_w.T, right_w.T,
                  weight, residue_mask)
    ])


def fused_body(
    sequence_matrix, pair_representation, alignment_row_mask, residue_mask, attention_scale_vector,
    asking_factor_matrix, lookup_factor_matrix, content_factor_matrix, sigmoid_factor_matrix,
    final_factor_matrix, pair_norm_gain, bias_weight, tensor_scale_vector, first_factor_matrix,
    second_factor_matrix, outer_weight,
):
    return front(
        lax.axis_size("row"), lax.axis_size("head"), sequence_matrix, pair_representation,
        alignment_row_mask, residue_mask, attention_scale_vector, asking_factor_matrix,
        lookup_factor_matrix, content_factor_matrix, sigmoid_factor_matrix, final_factor_matrix,
        pair_norm_gain, bias_weight, tensor_scale_vector, first_factor_matrix, second_factor_matrix,
        outer_weight,
    )


def fits(n_row, n_y, sequence_matrix, pair_representation, bias_weight, first_factor_matrix):
    rows, residues, feat = sequence_matrix.shape
    heads, opm = bias_weight.shape[1], first_factor_matrix.shape[1]
    n_rows, cols, pair_rows, nz = rows // n_row, residues // n_y, residues // n_row, n_row // 4
    if n_row % 4 or nz & (nz - 1) or nz % n_y or heads % (2 * n_y):
        return False
    group_width = heads // n_y // 2 * (feat // heads)
    return (
        n_rows * group_width == 128 and group_width == 64 and 2 * n_rows * opm == 128
        and cols % 128 == 0 and pair_rows % 16 == 0 and pair_representation.shape[2] == 128
        and n_row % 8 == 0
    )


def solution(mesh):
    placed = (P("row", "head", None), P("row", "head", None), P("row")) + (P(),) * 13
    n_row, n_y = mesh.shape["row"], mesh.shape["head"]

    def step(*args):
        chosen = fused_body if fits(n_row, n_y, args[0], args[1], args[11], args[13]) else body
        return jax.shard_map(
            chosen,
            mesh=mesh,
            in_specs=placed,
            out_specs=(P("row", "head", None), P("row", "head", None)),
            check_vma=False,
        )(*args)

    return step
```
